8 devices in a mesh: dp: 2 (over z, y), tp: 4 (over x, core).
Axes of the slice: x: 2, y: 2, z: 1, core: 2. Of those that a mesh axis runs over, the one named last changes fastest.
Arguments:
- hidden: bfloat16 [512, 2048], P('dp'), parts along dimension 0
- positions: int32 [512], P('dp'), parts along dimension 0
- k_cache: bfloat16 [2, 512, 64, 8, 128], P(None, 'dp', None, 'tp'), parts along dimension 1
- v_cache: bfloat16 [2, 512, 64, 8, 128], P(None, 'dp', None, 'tp'), parts along dimension 1
- attn_norm: bfloat16 [2, 2048], replicated
- w_query: bfloat16 [2, 2048, 2048], P(None, None, 'tp')
- w_key: bfloat16 [2, 2048, 1024], P(None, None, 'tp')
- w_value: bfloat16 [2, 2048, 1024], P(None, None, 'tp')
- w_out: bfloat16 [2, 2048, 2048], P(None, 'tp')
- mlp_norm: bfloat16 [2, 2048], replicated
- w_gate: bfloat16 [2, 2048, 8192], P(None, None, 'tp')
- w_up: bfloat16 [2, 2048, 8192], P(None, None, 'tp')
- w_down: bfloat16 [2, 8192, 2048], P(None, 'tp')
Outputs:
- output 1: bfloat16 [512, 2048], P('dp'), parts along dimension 0
- output 2: bfloat16 [2, 512, 64, 8, 128], P(None, 'dp', None, 'tp'), parts along dimension 1
- output 3: bfloat16 [2, 512, 64, 8, 128], P(None, 'dp', None, 'tp'), parts along dimension 1
There are 2 independent parts. The reference program is written for one: setup_inputs(seed, part) draws one part's arguments, and reference() takes and returns one part's arrays. A program takes and returns all parts, laid end to end along the dimension named above; an argument that names none is the same for every part.
All inputs are finite; a program needn't handle non-finite values.
Results may differ from the reference program's by a relative error of at most 0.02.
Values are sent between devices in bfloat16 or wider.
A program may use at most 1 GiB of HBM per device.

```python
import math
import jax
import jax.numpy as jnp
from jax import lax

LAYERS = 2
BATCH = 256
SEQ = 64
D = 2048
HEADS = 16
KV_HEADS = 8
HEAD = 128
FF = 8192


def normal_weight(rng_key, shape, scale):
    return (jax.random.normal(rng_key, shape, jnp.float32) * scale).astype(jnp.bfloat16)


def setup_inputs(seed: int = 0, part: int = 0) -> dict:
    base_key = jax.random.key(seed)
    shared_keys = jax.random.split(base_key, 9)
    part_keys = jax.random.split(jax.random.fold_in(base_key, part), 5)
    cache_shape = (LAYERS, BATCH, SEQ, KV_HEADS, HEAD)
    drawn_pos = jax.random.randint(part_keys[1], (BATCH,), SEQ // 8, SEQ, dtype=jnp.int32)
    drawn_pos = drawn_pos.at[0].set(SEQ - 1).at[1].set(SEQ // 8)
    return dict(
        hidden=normal_weight(part_keys[0], (BATCH, D), 1.0),
        positions=jax.random.permutation(part_keys[2], drawn_pos),
        k_cache=normal_weight(part_keys[3], cache_shape, 1.0),
        v_cache=normal_weight(part_keys[4], cache_shape, 1.0),
        attn_norm=(1.0 + 0.3 * jax.random.normal(shared_keys[0], (LAYERS, D), jnp.float32)).astype(jnp.bfloat16),
        w_query=normal_weight(shared_keys[1], (LAYERS, D, HEADS * HEAD), D ** -0.5),
        w_key=normal_weight(shared_keys[2], (LAYERS, D, KV_HEADS * HEAD), 1.5 * D ** -0.5),
        w_value=normal_weight(shared_keys[3], (LAYERS, D, KV_HEADS * HEAD), 1.5 * D ** -0.5),
        w_out=normal_weight(shared_keys[4], (LAYERS, HEADS * HEAD, D), 0.5 * (SEQ / (HEADS * HEAD)) ** 0.5),
        mlp_norm=(1.0 + 0.3 * jax.random.normal(shared_keys[5], (LAYERS, D), jnp.float32)).astype(jnp.bfloat16),
        w_gate=normal_weight(shared_keys[6], (LAYERS, D, FF), D ** -0.5),
        w_up=normal_weight(shared_keys[7], (LAYERS, D, FF), D ** -0.5),
        w_down=normal_weight(shared_keys[8], (LAYERS, FF, D), 1.5 * FF ** -0.5),
    )


def rms_norm(hidden, weight):
    hidden_f32 = hidden.astype(jnp.float32)
    mean_sq = jnp.mean(hidden_f32 * hidden_f32, axis=-1, keepdims=True)
    return (hidden_f32 * lax.rsqrt(mean_sq + 1e-5) * weight.astype(jnp.float32)).astype(jnp.bfloat16)


def rope_tables(positions, head_dim):
    half_dim = head_dim // 2
    inv_freq = jnp.power(500000.0, -jnp.arange(half_dim, dtype=jnp.float32) * (2.0 / head_dim))
    wavelen = (2.0 * math.pi) / inv_freq
    smooth = (8192.0 / wavelen - 1.0) / 3.0
    blended = (1.0 - smooth) * inv_freq / 8.0 + smooth * inv_freq
    scaled = jnp.where(wavelen < 2048.0, inv_freq, jnp.where(wavelen > 8192.0, inv_freq / 8.0, blended))
    angles = positions.astype(jnp.float32)[:, None] * scaled[None, :]
    return jnp.cos(angles), jnp.sin(angles)


def apply_rope(vectors, cos_tab, sin_tab):
    half_dim = vectors.shape[-1] // 2
    vec_f32 = vectors.astype(jnp.float32)
    first = vec_f32[..., :half_dim]
    second = vec_f32[..., half_dim:]
    cos_b = cos_tab[:, None, :]
    sin_b = sin_tab[:, None, :]
    return jnp.concatenate([first * cos_b - second * sin_b, second * cos_b + first * sin_b], axis=-1).astype(jnp.bfloat16)


def attend(query, k_all, v_all, visible):
    scores = jnp.einsum('bkgd,bskd->bkgs', query.astype(jnp.float32), k_all.astype(jnp.float32)) * (query.shape[-1] ** -0.5)
    scores = jnp.where(visible, scores, -jnp.inf)
    prob_rows = jax.nn.softmax(scores, axis=-1).astype(jnp.bfloat16)
    attn_out = jnp.einsum('bkgs,bskd->bkgd', prob_rows.astype(jnp.float32), v_all.astype(jnp.float32))
    return attn_out.astype(jnp.bfloat16)


def reference(hidden, positions, k_cache, v_cache, attn_norm, w_query, w_key, w_value, w_out, mlp_norm, w_gate, w_up, w_down):
    group = HEADS // KV_HEADS
    cos_tab, sin_tab = rope_tables(positions, HEAD)
    seq_ids = jnp.arange(SEQ)
    at_pos = (seq_ids[None, :] == positions[:, None])[:, :, None, None]
    visible = (seq_ids[None, :] <= positions[:, None])[:, None, None, :]

    def layer_step(state, layer_args):
        norm_attn, wq_layer, wk_layer, wv_layer, wo_layer, norm_mlp, wg_layer, wu_layer, wd_layer, k_layer, v_layer = layer_args
        normed = rms_norm(state, norm_attn)
        query = jnp.dot(normed, wq_layer, preferred_element_type=jnp.float32).astype(jnp.bfloat16)
        key_new = jnp.dot(normed, wk_layer, preferred_element_type=jnp.float32).astype(jnp.bfloat16)
        value_new = jnp.dot(normed, wv_layer, preferred_element_type=jnp.float32).astype(jnp.bfloat16)
        query = apply_rope(query.reshape(BATCH, HEADS, HEAD), cos_tab, sin_tab)
        key_new = apply_rope(key_new.reshape(BATCH, KV_HEADS, HEAD), cos_tab, sin_tab)
        value_new = value_new.reshape(BATCH, KV_HEADS, HEAD)
        k_layer = jnp.where(at_pos, key_new[:, None], k_layer)
        v_layer = jnp.where(at_pos, value_new[:, None], v_layer)
        attended = attend(query.reshape(BATCH, KV_HEADS, group, HEAD), k_layer, v_layer, visible)
        mixed = jnp.dot(attended.reshape(BATCH, HEADS * HEAD), wo_layer, preferred_element_type=jnp.float32)
        state = state + mixed.astype(jnp.bfloat16)
        normed = rms_norm(state, norm_mlp)
        gate_proj = jnp.dot(normed, wg_layer, preferred_element_type=jnp.float32).astype(jnp.bfloat16)
        up_proj = jnp.dot(normed, wu_layer, preferred_element_type=jnp.float32).astype(jnp.bfloat16)
        activated = (jax.nn.silu(gate_proj.astype(jnp.float32)) * up_proj.astype(jnp.float32)).astype(jnp.bfloat16)
        state = state + jnp.dot(activated, wd_layer, preferred_element_type=jnp.float32).astype(jnp.bfloat16)
        return state, (k_layer, v_layer)

    stacked = (attn_norm, w_query, w_key, w_value, w_out, mlp_norm, w_gate, w_up, w_down, k_cache, v_cache)
    final, (k_out, v_out) = lax.scan(layer_step, hidden, stacked)
    return final, k_out, v_out
```

```python
import functools
import math

import jax
import jax.numpy as jnp
import numpy as np
from jax import lax
from jax.experimental import pallas as pl
from jax.experimental.pallas import tpu as pltpu
from jax.sharding import PartitionSpec as P

MESH = pl.DeviceIdType.MESH
BF16 = jnp.bfloat16
F32 = jnp.float32
ANY = pl.BlockSpec(memory_space=pl.ANY)
VMEM = pl.BlockSpec(memory_space=pltpu.VMEM)
SMEM = pl.BlockSpec(memory_space=pltpu.SMEM)


def rope_by_position(seq_len, head_dim):
    half = head_dim // 2
    inv_freq = np.power(np.float32(500000.0), -np.arange(half, dtype=np.float32) * np.float32(2.0 / head_dim)).astype(np.float32)
    wavelen = np.float32(2.0 * math.pi) / inv_freq
    smooth = (np.float32(8192.0) / wavelen - np.float32(1.0)) / np.float32(3.0)
    blended = (np.float32(1.0) - smooth) * inv_freq / np.float32(8.0) + smooth * inv_freq
    scaled = np.where(wavelen < 2048.0, inv_freq, np.where(wavelen > 8192.0, inv_freq / np.float32(8.0), blended)).astype(np.float32)
    angles = np.arange(seq_len, dtype=np.float32)[:, None] * scaled[None, :]
    cos = np.cos(angles.astype(np.float64)).astype(np.float32)
    sin = np.sin(angles.astype(np.float64)).astype(np.float32)
    return np.concatenate([cos, cos], axis=1), np.concatenate([-sin, sin], axis=1)


def rms(rows_f32, weight_f32):
    mean_sq = jnp.mean(rows_f32 * rows_f32, axis=-1, keepdims=True)
    return (rows_f32 * lax.rsqrt(mean_sq + 1e-5) * weight_f32).astype(BF16)


def attention_kernel(layer, first, chunk, *refs):
    refs = list(refs)
    pos_ref = refs.pop(0)
    x_ref = refs.pop(0)
    norm_ref = refs.pop(0) if first else None
    cos_tab, sin_tab, wq_hbm, wk_hbm, wv_hbm, wo_hbm, kc_hbm, vc_hbm = refs[:8]
    refs = refs[8:]
    if not first:
        refs = refs[2:]
    part_ref, ko_hbm, vo_hbm = refs[:3]
    (wq, wk, wv, wo, kbuf, vbuf, h_scr, cos_scr, sin_scr, lim_scr, q_scr, k_scr, v_scr, kb_scr, vb_scr, s_scr, p_scr, o_scr,
     w_sem, in_sem, out_sem) = refs[3:]
    batch = x_ref.shape[0]
    n_q = wq.shape[1] // 128
    n_kv = wk.shape[1] // 128
    group = n_q // n_kv
    seq = kbuf.shape[1]
    n_chunks = batch // chunk

    loads = []
    for i, (src, dst) in enumerate(((wq_hbm, wq), (wk_hbm, wk), (wv_hbm, wv))):
        loads.append(pltpu.make_async_copy(src.at[layer], dst, w_sem.at[i]))
    for c in loads:
        c.start()
    kv_loads = []
    for c in range(n_chunks):
        rows = pl.ds(c * chunk, chunk)
        a = pltpu.make_async_copy(kc_hbm.at[layer, rows], kbuf.at[rows], in_sem.at[0, c])
        b = pltpu.make_async_copy(vc_hbm.at[layer, rows], vbuf.at[rows], in_sem.at[1, c])
        a.start()
        b.start()
        kv_loads.append((a, b))
    wo_load = pltpu.make_async_copy(wo_hbm.at[layer], wo, w_sem.at[3])
    wo_load.start()

    if first:
        weight = norm_ref[layer:layer + 1, :].astype(F32)

        def norm_body(i, carry):
            rows = pl.ds(pl.multiple_of(i * 16, 16), 16)
            h_scr[rows, :] = rms(x_ref[rows, :].astype(F32), weight)
            return carry

        lax.fori_loop(0, batch // 16, norm_body, 0)
        h_src = h_scr
    else:
        h_src = x_ref

    lane_head = lax.broadcasted_iota(jnp.int32, (n_q, 128), 1) % n_kv
    row_head = lax.broadcasted_iota(jnp.int32, (n_q, 128), 0) // group
    same_head = lane_head == row_head

    def table_body(i, carry):
        for u in range(8):
            b = i * 8 + u
            pos = pos_ref[b]
            cos_scr[pl.ds(b, 1), :] = cos_tab[pl.ds(pos, 1), :]
            sin_scr[pl.ds(b, 1), :] = sin_tab[pl.ds(pos, 1), :]
            lim_scr[pl.ds(b * n_q, n_q), :] = jnp.where(same_head, pos * n_kv + n_kv - 1, -1)
        return carry

    lax.fori_loop(0, batch // 8, table_body, 0)

    def rope(v):
        v = v.astype(BF16).astype(F32)
        return v * cos_scr[...] + pltpu.roll(v, 64, 1) * sin_scr[...]

    h = h_src[...]
    loads[0].wait()
    q = jnp.dot(h, wq[...], preferred_element_type=F32)
    for j in range(n_q):
        q_scr[pl.ds(j, batch, n_q), :] = rope(q[:, j * 128:(j + 1) * 128])
    loads[1].wait()
    k = jnp.dot(h, wk[...], preferred_element_type=F32)
    for j in range(n_kv):
        k_scr[pl.ds(j, batch, n_kv), :] = rope(k[:, j * 128:(j + 1) * 128])
    loads[2].wait()
    v = jnp.dot(h, wv[...], preferred_element_type=F32)
    for j in range(n_kv):
        v_scr[pl.ds(j, batch, n_kv), :] = v[:, j * 128:(j + 1) * 128]
    kb_scr.reshape(batch * n_kv, 128)[...] = k_scr[...].astype(BF16)
    vb_scr.reshape(batch * n_kv, 128)[...] = v_scr[...].astype(BF16)

    rows_kv = seq * n_kv
    kmat = kbuf.reshape(batch * rows_kv, 128)
    vmat = vbuf.reshape(batch * rows_kv, 128)
    scale = 128 ** -0.5
    row_id = lax.broadcasted_iota(jnp.int32, (4 * n_q, 128), 0)
    first_pair = row_id < 2 * n_q
    first_in_pair = (row_id % (2 * n_q)) < n_q
    zero = jnp.zeros((4 * n_q, 128), F32)
    quads = chunk // 4
    srows = chunk * n_q

    def square(mat, base):
        top = mat[pl.ds(base, 2 * rows_kv), :]
        bottom = mat[pl.ds(base + 2 * rows_kv, 2 * rows_kv), :]
        return jnp.concatenate([top, bottom], axis=1)

    stores = []
    for c in range(n_chunks):
        rows = pl.ds(c * chunk, chunk)
        stores.append((pltpu.make_async_copy(kbuf.at[rows], ko_hbm.at[layer, rows], out_sem.at[0, c]),
                       pltpu.make_async_copy(vbuf.at[rows], vo_hbm.at[layer, rows], out_sem.at[1, c])))

    for c in range(n_chunks):
        kv_loads[c][0].wait()
        kv_loads[c][1].wait()

        def insert_body(i, carry):
            for u in range(8):
                b = c * chunk + i * 8 + u
                pos = pos_ref[b]
                kbuf[b, pos] = kb_scr[b]
                vbuf[b, pos] = vb_scr[b]
            return carry

        lax.fori_loop(0, chunk // 8, insert_body, 0)

        for t in range(quads):
            b = c * chunk + t * 4
            q4 = q_scr[pl.ds(b * n_q, 4 * n_q), :]
            wide = jnp.concatenate([jnp.where(first_pair, q4, zero), jnp.where(first_pair, zero, q4)], axis=1).astype(BF16)
            s = lax.dot_general(wide, square(kmat, b * rows_kv), (((1,), (1,)), ((), ())), preferred_element_type=F32)
            s_scr[pl.ds(t * 4 * n_q, 4 * n_q), :] = jnp.where(first_in_pair, s[:, :rows_kv], s[:, rows_kv:])
        lanes = lax.broadcasted_iota(jnp.int32, (srows, 128), 1)
        s = jnp.where(lanes <= lim_scr[pl.ds(c * srows, srows), :], s_scr[...] * scale, -jnp.inf)
        e = jnp.exp(s - jnp.max(s, axis=-1, keepdims=True))
        p_scr[...] = (e * (1.0 / jnp.sum(e, axis=-1, keepdims=True)))
        for t in range(quads):
            b = c * chunk + t * 4
            p4 = p_scr[pl.ds(t * 4 * n_q, 4 * n_q), :]
            wide = jnp.concatenate([jnp.where(first_in_pair, p4, zero), jnp.where(first_in_pair, zero, p4)], axis=1).astype(BF16)
            o = jnp.dot(wide, square(vmat, b * rows_kv), preferred_element_type=F32)
            o_scr[pl.ds(b * n_q, 4 * n_q), :] = jnp.where(first_pair, o[:, :128], o[:, 128:])
        stores[c][0].start()
        stores[c][1].start()

    att = jnp.concatenate([o_scr[pl.ds(j, batch, n_q), :].astype(BF16) for j in range(n_q)], axis=1)
    wo_load.wait()
    for n in range(wo.shape[1] // 512):
        cols = pl.ds(n * 512, 512)
        part_ref[:, cols] = jnp.dot(att, wo[:, cols], preferred_element_type=F32).astype(BF16)
    for a, b in stores:
        a.wait()
        b.wait()


def attention_call(layer, first, positions, x, norm, tables, wq, wk, wv, wo, kc, vc, k_out, v_out):
    batch, d = x.shape
    _, _, seq, n_kv, hd = kc.shape
    n_q = wq.shape[2] // hd
    chunk = 64
    n_chunks = batch // chunk
    ins = [positions, x] + ([norm] if first else []) + [tables[0], tables[1], wq, wk, wv, wo, kc, vc]
    specs = [SMEM, VMEM] + ([VMEM] if first else []) + [VMEM, VMEM] + [ANY] * 6
    aliases = {}
    if not first:
        aliases = {len(ins): 1, len(ins) + 1: 2}
        ins += [k_out, v_out]
        specs += [ANY, ANY]
    scratch = [
        pltpu.VMEM(wq.shape[1:], BF16), pltpu.VMEM(wk.shape[1:], BF16), pltpu.VMEM(wv.shape[1:], BF16), pltpu.VMEM(wo.shape[1:], BF16),
        pltpu.VMEM(kc.shape[1:], BF16), pltpu.VMEM(vc.shape[1:], BF16),
        pltpu.VMEM((batch if first else 16, d), BF16),
        pltpu.VMEM((batch, hd), F32), pltpu.VMEM((batch, hd), F32), pltpu.VMEM((batch * n_q, hd), jnp.int32),
        pltpu.VMEM((batch * n_q, hd), F32), pltpu.VMEM((batch * n_kv, hd), F32), pltpu.VMEM((batch * n_kv, hd), F32),
        pltpu.VMEM((batch, n_kv, hd), BF16), pltpu.VMEM((batch, n_kv, hd), BF16),
        pltpu.VMEM((chunk * n_q, hd), F32), pltpu.VMEM((chunk * n_q, hd), F32), pltpu.VMEM((batch * n_q, hd), F32),
        pltpu.SemaphoreType.DMA((4,)), pltpu.SemaphoreType.DMA((2, n_chunks)), pltpu.SemaphoreType.DMA((2, n_chunks)),
    ]
    return pl.pallas_call(
        functools.partial(attention_kernel, layer, first, chunk),
        out_shape=(jax.ShapeDtypeStruct((batch, d), BF16), jax.ShapeDtypeStruct(kc.shape, BF16), jax.ShapeDtypeStruct(vc.shape, BF16)),
        in_specs=specs,
        out_specs=(VMEM, ANY, ANY),
        scratch_shapes=scratch,
        input_output_aliases=aliases,
        compiler_params=pltpu.CompilerParams(vmem_limit_bytes=56 * 2**20),
        name=f"attention{layer}",
    )(*ins)


GROUPS = 2
SUB = 2
NCOL = 4


def mlp_kernel(layer, last, x_ref, part_ref, norm_ref, next_norm_ref, wg_hbm, wu_hbm, wd_hbm, *refs):
    if last:
        (xo_ref,), refs = refs[:1], refs[1:]
    else:
        (ho_ref, xo_ref), refs = refs[:2], refs[2:]
    (wg, wu, wd, d1, c1, x1, d2, c2, x2, x_own, hbuf, abuf, pbuf, obuf, w_sem, s_send, s_recv) = refs
    t = lax.axis_index("tp")
    core = lax.rem(t, 2)
    other = 1 - core
    partner = t + other - core
    across = lax.rem(t + 2, 4)
    d = x_ref.shape[1]
    half = d1.shape[0]
    rows_g = half // GROUPS
    rows_s = rows_g // SUB
    cols_n = d // NCOL

    barrier = pltpu.get_barrier_semaphore()
    for dev in (partner, across):
        pl.semaphore_signal(barrier, inc=1, device_id={"tp": dev}, device_id_type=MESH)
    w_loads = []
    for i, (src, dst) in enumerate(((wg_hbm, wg), (wu_hbm, wu), (wd_hbm, wd))):
        n = dst.shape[0] // 4
        for j in range(4):
            cp = pltpu.make_async_copy(src.at[layer, pl.ds(j * n, n)], dst.at[pl.ds(j * n, n)], w_sem.at[i, j])
            cp.start()
            w_loads.append(cp)
    pl.semaphore_wait(barrier, 2)

    def send(stage, idx, src, dst, dev):
        cp = pltpu.make_async_remote_copy(src_ref=src, dst_ref=dst, send_sem=s_send.at[stage, idx], recv_sem=s_recv.at[stage, idx],
                                          device_id={"tp": dev}, device_id_type=MESH)
        cp.start()
        return cp

    started = []

    subs = [(g, s, g * rows_g + s * rows_s) for g in range(GROUPS) for s in range(SUB)]
    near = []
    for i, (g, s, r0) in enumerate(subs):
        near.append(send(0, i, part_ref.at[pl.ds(other * half + r0, rows_s)], d1.at[pl.ds(r0, rows_s)], partner))
    far = []
    for i, (g, s, r0) in enumerate(subs):
        near[i].wait_recv()
        rows = pl.ds(r0, rows_s)
        c1[rows, :] = (part_ref[pl.ds(core * half + r0, rows_s), :].astype(F32) + d1[rows, :].astype(F32)).astype(BF16)
        far.append(send(1, i, c1.at[rows], x1.at[rows], across))
    started += near + far

    weight = norm_ref[layer:layer + 1, :].astype(F32)
    gathers1 = {}

    def finish1(g):
        for s in range(SUB):
            i = g * SUB + s
            far[i].wait_recv()
            for r in range(rows_s // 16):
                r0 = g * rows_g + s * rows_s + r * 16
                rows = pl.ds(r0, 16)
                total = (c1[rows, :].astype(F32) + x1[rows, :].astype(F32)).astype(BF16)
                res = x_ref[pl.ds(r0, 16), :] if last else x_ref[pl.ds(core * half + r0, 16), :]
                xn = (res.astype(F32) + total.astype(F32)).astype(BF16)
                x_own[rows, :] = xn
                hbuf[g, core, pl.ds(s * rows_s + r * 16, 16), :] = rms(xn.astype(F32), weight)
            part = hbuf.at[g, core, pl.ds(s * rows_s, rows_s)]
            cp = send(2, i, part, part, partner)
            gathers1[i] = cp
            started.append(cp)

    def wait1(g):
        for s in range(SUB):
            gathers1[g * SUB + s].wait_recv()

    def gate_up(g):
        hid = hbuf.at[g].reshape(2 * rows_g, d)

        def body(n, carry):
            cols = pl.ds(pl.multiple_of(n * 512, 512), 512)
            gate = jnp.dot(hid[...], wg[:, cols], preferred_element_type=F32).astype(BF16).astype(F32)
            up = jnp.dot(hid[...], wu[:, cols], preferred_element_type=F32).astype(BF16).astype(F32)
            abuf[:, cols] = (gate * (1.0 / (1.0 + jnp.exp(-gate))) * up).astype(BF16)
            return carry

        lax.fori_loop(0, wg.shape[1] // 512, body, 0)

    near2, far2 = {}, {}

    def relay2(g, n):
        i = g * NCOL + n
        near2[i].wait_recv()
        cols = pl.ds(n * cols_n, cols_n)
        rows = pl.ds(g * rows_g, rows_g)
        c2[rows, cols] = (pbuf[g, core, :, cols].astype(F32) + d2[rows, cols].astype(F32)).astype(BF16)
        far2[i] = send(4, i, c2.at[rows, cols], x2.at[rows, cols], across)
        started.append(far2[i])

    def down(g):
        for n in range(NCOL):
            cols = pl.ds(n * cols_n, cols_n)
            y = jnp.dot(abuf[...], wd[:, cols], preferred_element_type=F32).astype(BF16)
            pbuf[g, :, :, cols] = y.reshape(2, rows_g, cols_n)
            i = g * NCOL + n
            near2[i] = send(3, i, pbuf.at[g, other, :, cols], d2.at[pl.ds(g * rows_g, rows_g), cols], partner)
            started.append(near2[i])
            if n > 0:
                relay2(g, n - 1)
        relay2(g, NCOL - 1)

    gathers2 = {}

    def finish2(g):
        for n in range(NCOL):
            far2[g * NCOL + n].wait_recv()
        if not last:
            nweight = next_norm_ref[layer + 1:layer + 2, :].astype(F32)
        for s in range(SUB):
            for r in range(rows_s // 16):
                r0 = g * rows_g + s * rows_s + r * 16
                rows = pl.ds(r0, 16)
                total = (c2[rows, :].astype(F32) + x2[rows, :].astype(F32)).astype(BF16)
                xn = (x_own[rows, :].astype(F32) + total.astype(F32)).astype(BF16)
                if last:
                    obuf[g, core, pl.ds(s * rows_s + r * 16, 16), :] = xn
                else:
                    xo_ref[rows, :] = xn
                    obuf[g, core, pl.ds(s * rows_s + r * 16, 16), :] = rms(xn.astype(F32), nweight)
            part = obuf.at[g, core, pl.ds(s * rows_s, rows_s)]
            cp = send(5, g * SUB + s, part, part, partner)
            gathers2[g * SUB + s] = cp
            started.append(cp)

    def wait2(g):
        out = xo_ref if last else ho_ref
        for s in range(SUB):
            gathers2[g * SUB + s].wait_recv()
        for c in range(2):
            out[c * half + g * rows_g:c * half + (g + 1) * rows_g, :] = obuf[g, c]

    finish1(0)
    wait1(0)
    for cp in w_loads:
        cp.wait()
    gate_up(0)
    down(0)
    finish1(1)
    wait1(1)
    gate_up(1)
    down(1)
    finish2(0)
    wait2(0)
    finish2(1)
    wait2(1)
    for cp in started:
        cp.wait_send()


def mlp_call(layer, last, x, part, norm, next_norm, wg, wu, wd):
    batch, d = part.shape
    half = batch // 2
    rows_g = half // GROUPS
    ff = wg.shape[2]
    n_sem = max(GROUPS * NCOL, GROUPS * SUB)
    own = lambda: pltpu.VMEM((half, d), BF16)
    scratch = [
        pltpu.VMEM(wg.shape[1:], BF16), pltpu.VMEM(wu.shape[1:], BF16), pltpu.VMEM(wd.shape[1:], BF16),
        own(), own(), own(), own(), own(), own(), own(),
        pltpu.VMEM((GROUPS, 2, rows_g, d), BF16), pltpu.VMEM((2 * rows_g, ff), BF16),
        pltpu.VMEM((GROUPS, 2, rows_g, d), BF16), pltpu.VMEM((GROUPS, 2, rows_g, d), BF16),
        pltpu.SemaphoreType.DMA((3, 4)), pltpu.SemaphoreType.DMA((6, n_sem)), pltpu.SemaphoreType.DMA((6, n_sem)),
    ]
    full = jax.ShapeDtypeStruct((batch, d), BF16)
    mine = jax.ShapeDtypeStruct((half, d), BF16)
    return pl.pallas_call(
        functools.partial(mlp_kernel, layer, last),
        out_shape=full if last else (full, mine),
        in_specs=[VMEM] * 4 + [ANY] * 3,
        out_specs=VMEM if last else (VMEM, VMEM),
        scratch_shapes=scratch,
        compiler_params=pltpu.CompilerParams(collective_id=layer, has_side_effects=True, vmem_limit_bytes=48 * 2**20),
        name=f"mlp{layer}",
    )(x, part, norm, next_norm, wg, wu, wd)


def solution(mesh):
    row_spec = P('dp', None)
    pos_spec = P('dp')
    cache_spec = P(None, 'dp', None, 'tp', None)
    norm_spec = P(None, None)
    col_spec = P(None, None, 'tp')
    split_rows = P(None, 'tp', None)

    def local_step(hidden, positions, k_cache, v_cache, attn_norm, w_query, w_key, w_value, w_out, mlp_norm, w_gate, w_up, w_down):
        tables = [jnp.asarray(t) for t in rope_by_position(k_cache.shape[2], k_cache.shape[4])]
        part, k_out, v_out = attention_call(0, True, positions, hidden, attn_norm, tables, w_query, w_key, w_value, w_out, k_cache, v_cache, None, None)
        h, x_own = mlp_call(0, False, hidden, part, mlp_norm, attn_norm, w_gate, w_up, w_down)
        part, k_out, v_out = attention_call(1, False, positions, h, None, tables, w_query, w_key, w_value, w_out, k_cache, v_cache, k_out, v_out)
        hidden = mlp_call(1, True, x_own, part, mlp_norm, attn_norm, w_gate, w_up, w_down)
        return hidden, k_out, v_out

    return jax.shard_map(local_step, mesh=mesh, in_specs=(row_spec, pos_spec, cache_spec, cache_spec, norm_spec, col_spec, col_spec, col_spec, split_rows, norm_spec, col_spec, col_spec, split_rows), out_specs=(row_spec, cache_spec, cache_spec), check_vma=False)
```

```python
import functools
import math

import jax
import jax.numpy as jnp
import numpy as np
from jax import lax
from jax.experimental import pallas as pl
from jax.experimental.pallas import tpu as pltpu
from jax.sharding import PartitionSpec as P

MESH = pl.DeviceIdType.MESH
BF16 = jnp.bfloat16
F32 = jnp.float32
ANY = pl.BlockSpec(memory_space=pl.ANY)
HBM = pl.BlockSpec(memory_space=pltpu.HBM)
VMEM = pl.BlockSpec(memory_space=pltpu.VMEM)
SMEM = pl.BlockSpec(memory_space=pltpu.SMEM)


def rope_by_position(seq_len, head_dim):
    half = head_dim // 2
    inv_freq = np.power(np.float32(500000.0), -np.arange(half, dtype=np.float32) * np.float32(2.0 / head_dim)).astype(np.float32)
    wavelen = np.float32(2.0 * math.pi) / inv_freq
    smooth = (np.float32(8192.0) / wavelen - np.float32(1.0)) / np.float32(3.0)
    blended = (np.float32(1.0) - smooth) * inv_freq / np.float32(8.0) + smooth * inv_freq
    scaled = np.where(wavelen < 2048.0, inv_freq, np.where(wavelen > 8192.0, inv_freq / np.float32(8.0), blended)).astype(np.float32)
    angles = np.arange(seq_len, dtype=np.float32)[:, None] * scaled[None, :]
    cos = np.cos(angles.astype(np.float64)).astype(np.float32)
    sin = np.sin(angles.astype(np.float64)).astype(np.float32)
    return np.concatenate([cos, cos], axis=1), np.concatenate([-sin, sin], axis=1)


def rms(rows_f32, weight_f32):
    mean_sq = jnp.mean(rows_f32 * rows_f32, axis=-1, keepdims=True)
    return (rows_f32 * lax.rsqrt(mean_sq + 1e-5) * weight_f32).astype(BF16)


def in_hbm(arrays):
    return [pltpu.with_memory_space_constraint(a, pltpu.HBM) for a in arrays]


def attention_kernel(layer, first, chunk, *refs):
    refs = list(refs)
    pos_ref = refs.pop(0)
    x_in = refs.pop(0)
    norm_ref = refs.pop(0) if first else None
    cos_tab, sin_tab, wq_hbm, wk_hbm, wv_hbm, wo_hbm, kc_hbm, vc_hbm = refs[:8]
    refs = refs[8:]
    if first:
        part_ref, ko_hbm, vo_hbm = refs[:3]
        x_ref, wq, wk, wv, wo, kbuf, vbuf, h_scr = refs[3:11]
        refs = refs[11:]
    else:
        x_ref, wq, wk, wv, wo = x_in, wq_hbm, wk_hbm, wv_hbm, wo_hbm
        part_ref, ko_hbm, vo_hbm, kbuf, vbuf = refs[2:7]
        refs = refs[7:]
    (cos_scr, sin_scr, lim_scr, q_scr, k_scr, v_scr, kb_scr, vb_scr, p_scr, o_scr, w_sem, in_sem, out_sem) = refs
    batch = x_ref.shape[0]
    n_q = wq.shape[1] // 128
    n_kv = wk.shape[1] // 128
    group = n_q // n_kv
    seq = kbuf.shape[1]
    n_chunks = batch // chunk

    if first:
        x_load = pltpu.make_async_copy(x_in, x_ref, w_sem.at[4])
        x_load.start()
        loads = []
        for i, (src, dst) in enumerate(((wq_hbm, wq), (wk_hbm, wk), (wv_hbm, wv))):
            loads.append(pltpu.make_async_copy(src.at[layer], dst, w_sem.at[i]))
        for c in loads:
            c.start()
        kv_loads = []
        for c in range(n_chunks):
            rows = pl.ds(c * chunk, chunk)
            a = pltpu.make_async_copy(kc_hbm.at[layer, rows], kbuf.at[rows], in_sem.at[0, c])
            b = pltpu.make_async_copy(vc_hbm.at[layer, rows], vbuf.at[rows], in_sem.at[1, c])
            a.start()
            b.start()
            kv_loads.append((a, b))
        wo_load = pltpu.make_async_copy(wo_hbm.at[layer], wo, w_sem.at[3])
        wo_load.start()

    per_row = 128 // n_q
    lane_request = lax.broadcasted_iota(jnp.int32, (1, 128), 1) // n_q

    def table_body(i, carry):
        limit = jnp.zeros((1, 128), jnp.int32)
        for u in range(per_row):
            b = i * per_row + u
            pos = pos_ref[b]
            cos_scr[pl.ds(b, 1), :] = cos_tab[pl.ds(pos, 1), :]
            sin_scr[pl.ds(b, 1), :] = sin_tab[pl.ds(pos, 1), :]
            limit = jnp.where(lane_request == u, pos * n_kv + n_kv - 1, limit)
        lim_scr[pl.ds(i, 1), :] = limit
        return carry

    lax.fori_loop(0, batch // per_row, table_body, 0)

    if first:
        x_load.wait()
        weight = norm_ref[layer:layer + 1, :].astype(F32)

        def norm_body(i, carry):
            rows = pl.ds(pl.multiple_of(i * 16, 16), 16)
            h_scr[rows, :] = rms(x_ref[rows, :].astype(F32), weight)
            return carry

        lax.fori_loop(0, batch // 16, norm_body, 0)
        h_src = h_scr
    else:
        h_src = x_ref

    def rope(v):
        v = v.astype(BF16).astype(F32)
        return v * cos_scr[...] + pltpu.roll(v, 64, 1) * sin_scr[...]

    h = h_src[...]
    if first:
        loads[0].wait()
    q = jnp.dot(h, wq[...], preferred_element_type=F32)
    for j in range(n_q):
        q_scr[pl.ds(j, batch, n_q), :] = rope(q[:, j * 128:(j + 1) * 128])
    if first:
        loads[1].wait()
    k = jnp.dot(h, wk[...], preferred_element_type=F32)
    for j in range(n_kv):
        k_scr[pl.ds(j, batch, n_kv), :] = rope(k[:, j * 128:(j + 1) * 128])
    if first:
        loads[2].wait()
    v = jnp.dot(h, wv[...], preferred_element_type=F32)
    for j in range(n_kv):
        v_scr[pl.ds(j, batch, n_kv), :] = v[:, j * 128:(j + 1) * 128]
    kb_scr.reshape(batch * n_kv, 128)[...] = k_scr[...].astype(BF16)
    vb_scr.reshape(batch * n_kv, 128)[...] = v_scr[...].astype(BF16)

    rows_kv = seq * n_kv
    kmat = kbuf.reshape(batch * rows_kv, 128)
    vmat = vbuf.reshape(batch * rows_kv, 128)
    scale = 128 ** -0.5
    pair = 2 * n_q
    row_id = lax.broadcasted_iota(jnp.int32, (2 * pair, 128), 0)
    first_pair = row_id < pair
    first_in_pair = (row_id % pair) < n_q
    zero = jnp.zeros((2 * pair, 128), F32)
    quads = chunk // 4
    cols = chunk * n_q
    lane = lax.broadcasted_iota(jnp.int32, (rows_kv, cols), 1)
    row = lax.broadcasted_iota(jnp.int32, (rows_kv, cols), 0)
    same_head = (row % n_kv) == (lane % n_q) // group
    first_of_two = (lane // n_q) % 2 == 0
    lane_pair = lax.broadcasted_iota(jnp.int32, (128, 128), 1) // pair
    no_tile = jnp.zeros((128, 128), BF16)
    pairs_per_tile = 128 // pair

    def square(mat, base):
        top = mat[pl.ds(base, 2 * rows_kv), :]
        bottom = mat[pl.ds(base + 2 * rows_kv, 2 * rows_kv), :]
        return jnp.concatenate([top, bottom], axis=1)

    stores = []
    for c in range(n_chunks):
        rows = pl.ds(c * chunk, chunk)
        stores.append((pltpu.make_async_copy(kbuf.at[rows], ko_hbm.at[layer, rows], out_sem.at[0, c]),
                       pltpu.make_async_copy(vbuf.at[rows], vo_hbm.at[layer, rows], out_sem.at[1, c])))

    for c in range(n_chunks):
        if first:
            kv_loads[c][0].wait()
            kv_loads[c][1].wait()

        def insert_body(i, carry):
            for u in range(8):
                b = c * chunk + i * 8 + u
                pos = pos_ref[b]
                kbuf[b, pos] = kb_scr[b]
                vbuf[b, pos] = vb_scr[b]
            return carry

        lax.fori_loop(0, chunk // 8, insert_body, 0)

        q_t = q_scr[pl.ds(c * cols, cols), :].T
        acc = None
        for t in range(quads):
            halves = []
            for i in range(2):
                p = 2 * t + i
                tile = p // pairs_per_tile
                tiles = [no_tile] * (cols // 128)
                tiles[tile] = jnp.where(lane_pair == p % pairs_per_tile, q_t[:, tile * 128:(tile + 1) * 128], 0.0).astype(BF16)
                halves.append(jnp.concatenate(tiles, axis=1))
            d = jnp.dot(square(kmat, (c * chunk + t * 4) * rows_kv), jnp.concatenate(halves, axis=0), preferred_element_type=F32)
            acc = d if acc is None else acc + d
        stores[c][0].start()
        stores[c][1].start()
        s = jnp.where(first_of_two, acc[:rows_kv], acc[rows_kv:])
        limit = jnp.concatenate([lim_scr[pl.ds(c * (cols // 128) + j, 1), :] for j in range(cols // 128)], axis=1)
        s = jnp.where(same_head & (row <= limit), s * scale, -jnp.inf)
        e = jnp.exp(s - jnp.max(s, axis=0, keepdims=True))
        p_scr[...] = (e * (1.0 / jnp.sum(e, axis=0, keepdims=True))).T
        for t in range(quads):
            b = c * chunk + t * 4
            p4 = p_scr[pl.ds(t * 2 * pair, 2 * pair), :]
            wide = jnp.concatenate([jnp.where(first_in_pair, p4, zero), jnp.where(first_in_pair, zero, p4)], axis=1).astype(BF16)
            o = jnp.dot(wide, square(vmat, b * rows_kv), preferred_element_type=F32)
            o_scr[pl.ds(b * n_q, 2 * pair), :] = jnp.where(first_pair, o[:, :128], o[:, 128:])

    att = jnp.concatenate([o_scr[pl.ds(j, batch, n_q), :].astype(BF16) for j in range(n_q)], axis=1)
    if first:
        wo_load.wait()
    for n in range(wo.shape[1] // 512):
        cols_n = pl.ds(n * 512, 512)
        part_ref[:, cols_n] = jnp.dot(att, wo[:, cols_n], preferred_element_type=F32).astype(BF16)
    for a, b in stores:
        a.wait()
        b.wait()


def attention_call(layer, first, positions, x, norm, tables, wq, wk, wv, wo, kc, vc, k_out, v_out):
    batch, d = x.shape
    seq, n_kv, hd = kc.shape[-3:]
    n_q = wq.shape[-1] // hd
    chunk = 64
    n_chunks = batch // chunk
    if first:
        ins = [positions] + in_hbm([x]) + [norm, tables[0], tables[1]] + in_hbm([wq, wk, wv, wo, kc, vc])
    else:
        ins = [positions, x, tables[0], tables[1], wq, wk, wv, wo, kc, vc]
    part = pltpu.VMEM((batch, d), BF16)
    if first:
        specs = [SMEM, HBM, VMEM, VMEM, VMEM] + [HBM] * 6
        outs = (part, pltpu.HBM(kc.shape, BF16), pltpu.HBM(vc.shape, BF16))
        out_specs = (VMEM, HBM, HBM)
        aliases = {}
        big = [(batch, d), wq.shape[1:], wk.shape[1:], wv.shape[1:], wo.shape[1:], kc.shape[1:], vc.shape[1:], (batch, d)]
    else:
        specs = [SMEM, VMEM, VMEM, VMEM] + [VMEM] * 6 + [HBM] * 2
        aliases = {len(ins): 1, len(ins) + 1: 2, len(ins) - 2: 3, len(ins) - 1: 4}
        outs = (part, pltpu.HBM(k_out.shape, BF16), pltpu.HBM(v_out.shape, BF16), pltpu.VMEM(kc.shape, BF16), pltpu.VMEM(vc.shape, BF16))
        ins += in_hbm([k_out, v_out])
        out_specs = (VMEM, HBM, HBM, VMEM, VMEM)
        big = []
    scratch = [pltpu.VMEM(shape, BF16) for shape in big] + [
        pltpu.VMEM((batch, hd), F32), pltpu.VMEM((batch, hd), F32), pltpu.VMEM((batch * n_q // hd, hd), jnp.int32),
        pltpu.VMEM((batch * n_q, hd), F32), pltpu.VMEM((batch * n_kv, hd), F32), pltpu.VMEM((batch * n_kv, hd), F32),
        pltpu.VMEM((batch, n_kv, hd), BF16), pltpu.VMEM((batch, n_kv, hd), BF16),
        pltpu.VMEM((chunk * n_q, hd), F32), pltpu.VMEM((batch * n_q, hd), F32),
        pltpu.SemaphoreType.DMA((5,)), pltpu.SemaphoreType.DMA((2, n_chunks)), pltpu.SemaphoreType.DMA((2, n_chunks)),
    ]
    return pl.pallas_call(
        functools.partial(attention_kernel, layer, first, chunk),
        out_shape=outs,
        in_specs=specs,
        out_specs=out_specs,
        scratch_shapes=scratch,
        input_output_aliases=aliases,
        compiler_params=pltpu.CompilerParams(vmem_limit_bytes=(62 if first else 8) * 2**20),
        name=f"attention{layer}",
    )(*ins)


GROUPS = 2
SUB = 2
NCOL = 4


def mlp_kernel(layer, last, x_ref, part_ref, norm_ref, next_norm_ref, wg_hbm, wu_hbm, wd_hbm, *refs):
    if last:
        carry_in, carry_out = (), ()
        (xo_ref,), refs = refs[:1], refs[1:]
    else:
        carry_in, (ho_ref, xo_ref), carry_out, refs = refs[:6], refs[6:8], refs[8:14], refs[14:]
    (wg, wu, wd, d1, c1, x1, d2, c2, x2, x_own, hbuf, abuf, pbuf, obuf, w_sem, c_sem, s_send, s_recv) = refs
    t = lax.axis_index("tp")
    core = lax.rem(t, 2)
    other = 1 - core
    partner = t + other - core
    across = lax.rem(t + 2, 4)
    d = x_ref.shape[1]
    half = d1.shape[0]
    rows_g = half // GROUPS
    rows_s = rows_g // SUB
    cols_n = d // NCOL

    barrier = pltpu.get_barrier_semaphore()
    for dev in (partner, across):
        pl.semaphore_signal(barrier, inc=1, device_id={"tp": dev}, device_id_type=MESH)
    w_loads = []
    for i, (src, dst) in enumerate(((wg_hbm, wg), (wu_hbm, wu), (wd_hbm, wd))):
        n = dst.shape[0] // 4
        for j in range(4):
            cp = pltpu.make_async_copy(src.at[layer, pl.ds(j * n, n)], dst.at[pl.ds(j * n, n)], w_sem.at[i, j])
            cp.start()
            w_loads.append(cp)
    c_loads = []
    for i, (src, dst) in enumerate(zip(carry_in, carry_out)):
        n = dst.shape[0] // 4
        for j in range(4):
            cp = pltpu.make_async_copy(src.at[layer + 1, pl.ds(j * n, n)], dst.at[pl.ds(j * n, n)], c_sem.at[i, j])
            cp.start()
            c_loads.append(cp)
    pl.semaphore_wait(barrier, 2)

    def send(stage, idx, src, dst, dev):
        cp = pltpu.make_async_remote_copy(src_ref=src, dst_ref=dst, send_sem=s_send.at[stage, idx], recv_sem=s_recv.at[stage, idx],
                                          device_id={"tp": dev}, device_id_type=MESH)
        cp.start()
        return cp

    started = []

    subs = [(g, s, g * rows_g + s * rows_s) for g in range(GROUPS) for s in range(SUB)]
    near = []
    for i, (g, s, r0) in enumerate(subs):
        near.append(send(0, i, part_ref.at[pl.ds(other * half + r0, rows_s)], d1.at[pl.ds(r0, rows_s)], partner))
    far = []
    for i, (g, s, r0) in enumerate(subs):
        near[i].wait_recv()
        rows = pl.ds(r0, rows_s)
        c1[rows, :] = (part_ref[pl.ds(core * half + r0, rows_s), :].astype(F32) + d1[rows, :].astype(F32)).astype(BF16)
        far.append(send(1, i, c1.at[rows], x1.at[rows], across))
    started += near + far

    weight = norm_ref[layer:layer + 1, :].astype(F32)
    gathers1 = {}

    def finish1(g):
        for s in range(SUB):
            i = g * SUB + s
            far[i].wait_recv()
            for r in range(rows_s // 16):
                r0 = g * rows_g + s * rows_s + r * 16
                rows = pl.ds(r0, 16)
                total = (c1[rows, :].astype(F32) + x1[rows, :].astype(F32)).astype(BF16)
                res = x_ref[pl.ds(r0, 16), :] if last else x_ref[pl.ds(core * half + r0, 16), :]
                xn = (res.astype(F32) + total.astype(F32)).astype(BF16)
                x_own[rows, :] = xn
                hbuf[g, core, pl.ds(s * rows_s + r * 16, 16), :] = rms(xn.astype(F32), weight)
            part = hbuf.at[g, core, pl.ds(s * rows_s, rows_s)]
            cp = send(2, i, part, part, partner)
            gathers1[i] = cp
            started.append(cp)

    def wait1(g):
        for s in range(SUB):
            gathers1[g * SUB + s].wait_recv()

    def gate_up(g):
        hid = hbuf.at[g].reshape(2 * rows_g, d)

        def body(n, carry):
            cols = pl.ds(pl.multiple_of(n * 512, 512), 512)
            gate = jnp.dot(hid[...], wg[:, cols], preferred_element_type=F32).astype(BF16).astype(F32)
            up = jnp.dot(hid[...], wu[:, cols], preferred_element_type=F32).astype(BF16).astype(F32)
            abuf[:, cols] = (gate * (1.0 / (1.0 + jnp.exp(-gate))) * up).astype(BF16)
            return carry

        lax.fori_loop(0, wg.shape[1] // 512, body, 0)

    near2, far2 = {}, {}

    def relay2(g, n):
        i = g * NCOL + n
        near2[i].wait_recv()
        cols = pl.ds(n * cols_n, cols_n)
        rows = pl.ds(g * rows_g, rows_g)
        c2[rows, cols] = (pbuf[g, core, :, cols].astype(F32) + d2[rows, cols].astype(F32)).astype(BF16)
        far2[i] = send(4, i, c2.at[rows, cols], x2.at[rows, cols], across)
        started.append(far2[i])

    def down(g, after_first):
        for n in range(NCOL):
            cols = pl.ds(n * cols_n, cols_n)
            y = jnp.dot(abuf[...], wd[:, cols], preferred_element_type=F32).astype(BF16)
            pbuf[g, :, :, cols] = y.reshape(2, rows_g, cols_n)
            i = g * NCOL + n
            near2[i] = send(3, i, pbuf.at[g, other, :, cols], d2.at[pl.ds(g * rows_g, rows_g), cols], partner)
            started.append(near2[i])
            if n == 0 and after_first is not None:
                after_first()
            if n > 0:
                relay2(g, n - 1)
        relay2(g, NCOL - 1)

    gathers2 = {}

    def finish2(g):
        for n in range(NCOL):
            far2[g * NCOL + n].wait_recv()
        if not last:
            nweight = next_norm_ref[layer + 1:layer + 2, :].astype(F32)
        for s in range(SUB):
            for r in range(rows_s // 16):
                r0 = g * rows_g + s * rows_s + r * 16
                rows = pl.ds(r0, 16)
                total = (c2[rows, :].astype(F32) + x2[rows, :].astype(F32)).astype(BF16)
                xn = (x_own[rows, :].astype(F32) + total.astype(F32)).astype(BF16)
                if last:
                    obuf[g, core, pl.ds(s * rows_s + r * 16, 16), :] = xn
                else:
                    xo_ref[rows, :] = xn
                    obuf[g, core, pl.ds(s * rows_s + r * 16, 16), :] = rms(xn.astype(F32), nweight)
            part = obuf.at[g, core, pl.ds(s * rows_s, rows_s)]
            cp = send(5, g * SUB + s, part, part, partner)
            gathers2[g * SUB + s] = cp
            started.append(cp)

    def wait2(g):
        out = xo_ref if last else ho_ref
        for s in range(SUB):
            gathers2[g * SUB + s].wait_recv()
        for c in range(2):
            out[c * half + g * rows_g:c * half + (g + 1) * rows_g, :] = obuf[g, c]

    finish1(0)
    wait1(0)
    for cp in w_loads:
        cp.wait()
    gate_up(0)
    down(0, lambda: finish1(1))
    wait1(1)
    gate_up(1)
    down(1, None)
    finish2(0)
    wait2(0)
    finish2(1)
    wait2(1)
    for cp in c_loads:
        cp.wait()
    for cp in started:
        cp.wait_send()


def mlp_call(layer, last, x, part, norm, next_norm, wg, wu, wd, carry=()):
    batch, d = part.shape
    half = batch // 2
    rows_g = half // GROUPS
    ff = wg.shape[2]
    n_sem = max(GROUPS * NCOL, GROUPS * SUB)
    own = lambda: pltpu.VMEM((half, d), BF16)
    scratch = [
        pltpu.VMEM(wg.shape[1:], BF16), pltpu.VMEM(wu.shape[1:], BF16), pltpu.VMEM(wd.shape[1:], BF16),
        own(), own(), own(), own(), own(), own(), own(),
        pltpu.VMEM((GROUPS, 2, rows_g, d), BF16), pltpu.VMEM((2 * rows_g, ff), BF16),
        pltpu.VMEM((GROUPS, 2, rows_g, d), BF16), pltpu.VMEM((GROUPS, 2, rows_g, d), BF16),
        pltpu.SemaphoreType.DMA((3, 4)), pltpu.SemaphoreType.DMA((6, 4)), pltpu.SemaphoreType.DMA((6, n_sem)), pltpu.SemaphoreType.DMA((6, n_sem)),
    ]
    full = pltpu.VMEM((batch, d), BF16)
    mine = pltpu.VMEM((half, d), BF16)
    return pl.pallas_call(
        functools.partial(mlp_kernel, layer, last),
        out_shape=full if last else (full, mine) + tuple(pltpu.VMEM(a.shape[1:], BF16) for a in carry),
        in_specs=[VMEM] * 4 + [HBM] * (3 + len(carry)),
        out_specs=VMEM if last else (VMEM,) * (2 + len(carry)),
        scratch_shapes=scratch,
        compiler_params=pltpu.CompilerParams(collective_id=layer, has_side_effects=True, vmem_limit_bytes=(33 if last else 33) * 2**20),
        name=f"mlp{layer}",
    )(x, pltpu.with_memory_space_constraint(part, pltpu.VMEM), norm, next_norm, *in_hbm((wg, wu, wd) + tuple(carry)))


def solution(mesh):
    row_spec = P('dp', None)
    pos_spec = P('dp')
    cache_spec = P(None, 'dp', None, 'tp', None)
    norm_spec = P(None, None)
    col_spec = P(None, None, 'tp')
    split_rows = P(None, 'tp', None)

    def local_step(hidden, positions, k_cache, v_cache, attn_norm, w_query, w_key, w_value, w_out, mlp_norm, w_gate, w_up, w_down):
        tables = [jnp.asarray(t) for t in rope_by_position(k_cache.shape[2], k_cache.shape[4])]
        part, k_out, v_out = attention_call(0, True, positions, hidden, attn_norm, tables, w_query, w_key, w_value, w_out, k_cache, v_cache, None, None)
        h, x_own, *carried = mlp_call(0, False, hidden, part, mlp_norm, attn_norm, w_gate, w_up, w_down, (w_query, w_key, w_value, w_out, k_cache, v_cache))
        part, k_out, v_out = attention_call(1, False, positions, h, None, tables, *carried, k_out, v_out)[:3]
        hidden = mlp_call(1, True, x_own, part, mlp_norm, attn_norm, w_gate, w_up, w_down)
        return hidden, k_out, v_out

    return jax.shard_map(local_step, mesh=mesh, in_specs=(row_spec, pos_spec, cache_spec, cache_spec, norm_spec, col_spec, col_spec, col_spec, split_rows, norm_spec, col_spec, col_spec, split_rows), out_specs=(row_spec, cache_spec, cache_spec), check_vma=False)
```

```python
import functools
import math

import jax
import jax.numpy as jnp
import numpy as np
from jax import lax
from jax.experimental import pallas as pl
from jax.experimental.pallas import tpu as pltpu
from jax.sharding import PartitionSpec as P

MESH = pl.DeviceIdType.MESH
BF16 = jnp.bfloat16
F32 = jnp.float32
ANY = pl.BlockSpec(memory_space=pl.ANY)
HBM = pl.BlockSpec(memory_space=pltpu.HBM)
VMEM = pl.BlockSpec(memory_space=pltpu.VMEM)
SMEM = pl.BlockSpec(memory_space=pltpu.SMEM)


def rope_by_position(seq_len, head_dim):
    half = head_dim // 2
    inv_freq = np.power(np.float32(500000.0), -np.arange(half, dtype=np.float32) * np.float32(2.0 / head_dim)).astype(np.float32)
    wavelen = np.float32(2.0 * math.pi) / inv_freq
    smooth = (np.float32(8192.0) / wavelen - np.float32(1.0)) / np.float32(3.0)
    blended = (np.float32(1.0) - smooth) * inv_freq / np.float32(8.0) + smooth * inv_freq
    scaled = np.where(wavelen < 2048.0, inv_freq, np.where(wavelen > 8192.0, inv_freq / np.float32(8.0), blended)).astype(np.float32)
    angles = np.arange(seq_len, dtype=np.float32)[:, None] * scaled[None, :]
    cos = np.cos(angles.astype(np.float64)).astype(np.float32)
    sin = np.sin(angles.astype(np.float64)).astype(np.float32)
    return np.concatenate([cos, cos], axis=1), np.concatenate([-sin, sin], axis=1)


def rms(rows_f32, weight_f32):
    mean_sq = jnp.mean(rows_f32 * rows_f32, axis=-1, keepdims=True)
    return (rows_f32 * lax.rsqrt(mean_sq + 1e-5) * weight_f32).astype(BF16)


def in_hbm(arrays):
    return [pltpu.with_memory_space_constraint(a, pltpu.HBM) for a in arrays]


def attention_kernel(layer, first, chunk, *refs):
    refs = list(refs)
    pos_ref = refs.pop(0)
    x_in = refs.pop(0)
    norm_ref = refs.pop(0) if first else None
    cos_tab, sin_tab, wq_hbm, wk_hbm, wv_hbm, wo_hbm, kc_hbm, vc_hbm = refs[:8]
    refs = refs[8:]
    if first:
        part_ref, ko_hbm, vo_hbm = refs[:3]
        x_ref, wq, wk, wv, wo, kbuf, vbuf, h_scr = refs[3:11]
        refs = refs[11:]
    else:
        x_ref, wq, wk, wv, wo = x_in, wq_hbm, wk_hbm, wv_hbm, wo_hbm
        part_ref, ko_hbm, vo_hbm, kbuf, vbuf = refs[2:7]
        refs = refs[7:]
    (cos_scr, sin_scr, lim_scr, q_scr, k_scr, v_scr, p_scr, o_scr, w_sem, in_sem, out_sem) = refs
    batch = x_ref.shape[0]
    n_q = wq.shape[1] // 128
    n_kv = wk.shape[1] // 128
    group = n_q // n_kv
    rows_kv = kbuf.shape[1]
    n_chunks = batch // chunk

    if first:
        x_load = pltpu.make_async_copy(x_in, x_ref, w_sem.at[4])
        x_load.start()
        loads = []
        for i, (src, dst) in enumerate(((wq_hbm, wq), (wk_hbm, wk), (wv_hbm, wv))):
            loads.append(pltpu.make_async_copy(src.at[layer], dst, w_sem.at[i]))
        for c in loads:
            c.start()
        kv_loads = []
        for c in range(n_chunks):
            rows = pl.ds(c * chunk, chunk)
            a = pltpu.make_async_copy(kc_hbm.at[layer, rows], kbuf.at[rows], in_sem.at[0, c])
            b = pltpu.make_async_copy(vc_hbm.at[layer, rows], vbuf.at[rows], in_sem.at[1, c])
            a.start()
            b.start()
            kv_loads.append((a, b))
        wo_load = pltpu.make_async_copy(wo_hbm.at[layer], wo, w_sem.at[3])
        wo_load.start()

    per_row = 128 // n_q
    lane_request = lax.broadcasted_iota(jnp.int32, (1, 128), 1) // n_q

    def table_body(i, carry):
        limit = jnp.zeros((1, 128), jnp.int32)
        for u in range(per_row):
            b = i * per_row + u
            pos = pos_ref[b]
            cos_scr[pl.ds(b, 1), :] = cos_tab[pl.ds(pos, 1), :]
            sin_scr[pl.ds(b, 1), :] = sin_tab[pl.ds(pos, 1), :]
            limit = jnp.where(lane_request == u, pos * n_kv + n_kv - 1, limit)
        lim_scr[pl.ds(i, 1), :] = limit
        return carry

    lax.fori_loop(0, batch // per_row, table_body, 0)

    if first:
        x_load.wait()
        weight = norm_ref[layer:layer + 1, :].astype(F32)

        def norm_body(i, carry):
            rows = pl.ds(pl.multiple_of(i * 16, 16), 16)
            h_scr[rows, :] = rms(x_ref[rows, :].astype(F32), weight)
            return carry

        lax.fori_loop(0, batch // 16, norm_body, 0)
        h_src = h_scr
    else:
        h_src = x_ref

    def rope(v):
        v = v.astype(BF16).astype(F32)
        return v * cos_scr[...] + pltpu.roll(v, 64, 1) * sin_scr[...]

    h = h_src[...]
    if first:
        loads[0].wait()
    q = jnp.dot(h, wq[...], preferred_element_type=F32)
    for j in range(n_q):
        q_scr[pl.ds(j, batch, n_q), :] = rope(q[:, j * 128:(j + 1) * 128])
    if first:
        loads[1].wait()
    k = jnp.dot(h, wk[...], preferred_element_type=F32)
    for j in range(n_kv):
        k_scr[pl.ds(j, batch, n_kv), :] = rope(k[:, j * 128:(j + 1) * 128])
    if first:
        loads[2].wait()
    v = jnp.dot(h, wv[...], preferred_element_type=F32)
    for j in range(n_kv):
        v_scr[pl.ds(j, batch, n_kv), :] = v[:, j * 128:(j + 1) * 128]

    kmat = kbuf.reshape(batch * rows_kv, 128)
    vmat = vbuf.reshape(batch * rows_kv, 128)
    scale = 128 ** -0.5
    pair = 2 * n_q
    row_id = lax.broadcasted_iota(jnp.int32, (2 * pair, 128), 0)
    first_pair = row_id < pair
    first_in_pair = (row_id % pair) < n_q
    zero = jnp.zeros((2 * pair, 128), F32)
    quads = chunk // 4
    cols = chunk * n_q
    lane = lax.broadcasted_iota(jnp.int32, (rows_kv, cols), 1)
    row = lax.broadcasted_iota(jnp.int32, (rows_kv, cols), 0)
    same_head = (row % n_kv) == (lane % n_q) // group
    first_of_two = (lane // n_q) % 2 == 0
    lane_pair = lax.broadcasted_iota(jnp.int32, (128, 128), 1) // pair
    no_tile = jnp.zeros((128, 128), BF16)
    pairs_per_tile = 128 // pair
    tile_row = lax.broadcasted_iota(jnp.int32, (16, 128), 0)

    def square(mat, base):
        top = mat[pl.ds(base, 2 * rows_kv), :]
        bottom = mat[pl.ds(base + 2 * rows_kv, 2 * rows_kv), :]
        return jnp.concatenate([top, bottom], axis=1)

    stores = []
    for c in range(n_chunks):
        rows = pl.ds(c * chunk, chunk)
        stores.append((pltpu.make_async_copy(kbuf.at[rows], ko_hbm.at[layer, rows], out_sem.at[0, c]),
                       pltpu.make_async_copy(vbuf.at[rows], vo_hbm.at[layer, rows], out_sem.at[1, c])))

    for c in range(n_chunks):
        if first:
            kv_loads[c][0].wait()
            kv_loads[c][1].wait()

        def insert_body(i, carry):
            writes = []
            for u in range(16):
                b = c * chunk + i * 16 + u
                place = pos_ref[b] * n_kv
                block = pl.ds(pl.multiple_of((place // 16) * 16, 16), 16)
                here = tile_row // n_kv == (place % 16) // n_kv
                for buf, new in ((kbuf, k_scr), (vbuf, v_scr)):
                    rows_new = new[pl.ds(b * n_kv, 1), :]
                    for j in range(1, n_kv):
                        rows_new = jnp.where(tile_row % n_kv == j, new[pl.ds(b * n_kv + j, 1), :], rows_new)
                    writes.append((buf, b, block, jnp.where(here, rows_new, buf[b, block, :].astype(F32)).astype(BF16)))
            for buf, b, block, value in writes:
                buf[b, block, :] = value
            return carry

        lax.fori_loop(0, chunk // 16, insert_body, 0)

        q_t = q_scr[pl.ds(c * cols, cols), :].T
        acc = None
        for t in range(quads):
            halves = []
            for i in range(2):
                p = 2 * t + i
                tile = p // pairs_per_tile
                tiles = [no_tile] * (cols // 128)
                tiles[tile] = jnp.where(lane_pair == p % pairs_per_tile, q_t[:, tile * 128:(tile + 1) * 128], 0.0).astype(BF16)
                halves.append(jnp.concatenate(tiles, axis=1))
            d = jnp.dot(square(kmat, (c * chunk + t * 4) * rows_kv), jnp.concatenate(halves, axis=0), preferred_element_type=F32)
            acc = d if acc is None else acc + d
        stores[c][0].start()
        stores[c][1].start()
        s = jnp.where(first_of_two, acc[:rows_kv], acc[rows_kv:])
        limit = jnp.concatenate([lim_scr[pl.ds(c * (cols // 128) + j, 1), :] for j in range(cols // 128)], axis=1)
        s = jnp.where(same_head & (row <= limit), s * scale, -jnp.inf)
        e = jnp.exp(s - jnp.max(s, axis=0, keepdims=True))
        p_scr[...] = (e * (1.0 / jnp.sum(e, axis=0, keepdims=True))).T
        for t in range(quads):
            b = c * chunk + t * 4
            p4 = p_scr[pl.ds(t * 2 * pair, 2 * pair), :]
            wide = jnp.concatenate([jnp.where(first_in_pair, p4, zero), jnp.where(first_in_pair, zero, p4)], axis=1).astype(BF16)
            o = jnp.dot(wide, square(vmat, b * rows_kv), preferred_element_type=F32)
            o_scr[pl.ds(b * n_q, 2 * pair), :] = jnp.where(first_pair, o[:, :128], o[:, 128:])

    att = jnp.concatenate([o_scr[pl.ds(j, batch, n_q), :].astype(BF16) for j in range(n_q)], axis=1)
    if first:
        wo_load.wait()
    for n in range(wo.shape[1] // 512):
        cols_n = pl.ds(n * 512, 512)
        part_ref[:, cols_n] = jnp.dot(att, wo[:, cols_n], preferred_element_type=F32).astype(BF16)
    for a, b in stores:
        a.wait()
        b.wait()


def attention_call(layer, first, positions, x, norm, tables, wq, wk, wv, wo, kc, vc, k_out, v_out):
    batch, d = x.shape
    hd = kc.shape[-1]
    n_q, n_kv = wq.shape[-1] // hd, wk.shape[-1] // hd
    chunk = 64
    n_chunks = batch // chunk
    if first:
        ins = [positions] + in_hbm([x]) + [norm, tables[0], tables[1]] + in_hbm([wq, wk, wv, wo, kc, vc])
    else:
        ins = [positions, x, tables[0], tables[1], wq, wk, wv, wo, kc, vc]
    part = pltpu.VMEM((batch, d), BF16)
    if first:
        specs = [SMEM, HBM, VMEM, VMEM, VMEM] + [HBM] * 6
        outs = (part, pltpu.HBM(kc.shape, BF16), pltpu.HBM(vc.shape, BF16))
        out_specs = (VMEM, HBM, HBM)
        aliases = {}
        big = [(batch, d), wq.shape[1:], wk.shape[1:], wv.shape[1:], wo.shape[1:], kc.shape[1:], vc.shape[1:], (batch, d)]
    else:
        specs = [SMEM, VMEM, VMEM, VMEM] + [VMEM] * 6 + [HBM] * 2
        aliases = {len(ins): 1, len(ins) + 1: 2, len(ins) - 2: 3, len(ins) - 1: 4}
        outs = (part, pltpu.HBM(k_out.shape, BF16), pltpu.HBM(v_out.shape, BF16), pltpu.VMEM(kc.shape, BF16), pltpu.VMEM(vc.shape, BF16))
        ins += in_hbm([k_out, v_out])
        out_specs = (VMEM, HBM, HBM, VMEM, VMEM)
        big = []
    scratch = [pltpu.VMEM(shape, BF16) for shape in big] + [
        pltpu.VMEM((batch, hd), F32), pltpu.VMEM((batch, hd), F32), pltpu.VMEM((batch * n_q // hd, hd), jnp.int32),
        pltpu.VMEM((batch * n_q, hd), F32), pltpu.VMEM((batch * n_kv, hd), F32), pltpu.VMEM((batch * n_kv, hd), F32),
        pltpu.VMEM((chunk * n_q, hd), F32), pltpu.VMEM((batch * n_q, hd), F32),
        pltpu.SemaphoreType.DMA((5,)), pltpu.SemaphoreType.DMA((2, n_chunks)), pltpu.SemaphoreType.DMA((2, n_chunks)),
    ]
    return pl.pallas_call(
        functools.partial(attention_kernel, layer, first, chunk),
        out_shape=outs,
        in_specs=specs,
        out_specs=out_specs,
        scratch_shapes=scratch,
        input_output_aliases=aliases,
        compiler_params=pltpu.CompilerParams(vmem_limit_bytes=(62 if first else 8) * 2**20),
        name=f"attention{layer}",
    )(*ins)


GROUPS = 2
SUB = 2
NCOL = 4


def mlp_kernel(layer, last, x_ref, part_ref, norm_ref, next_norm_ref, wg_hbm, wu_hbm, wd_hbm, *refs):
    if last:
        carry_in, carry_out = (), ()
        (xo_ref,), refs = refs[:1], refs[1:]
    else:
        carry_in, (ho_ref, xo_ref), carry_out, refs = refs[:6], refs[6:8], refs[8:14], refs[14:]
    (wg, wu, wd, d1, c1, x1, d2, c2, x2, x_own, hbuf, abuf, pbuf, obuf, w_sem, c_sem, s_send, s_recv) = refs
    t = lax.axis_index("tp")
    core = lax.rem(t, 2)
    other = 1 - core
    partner = t + other - core
    across = lax.rem(t + 2, 4)
    d = x_ref.shape[1]
    half = d1.shape[0]
    rows_g = half // GROUPS
    rows_s = rows_g // SUB
    cols_n = d // NCOL

    barrier = pltpu.get_barrier_semaphore()
    for dev in (partner, across):
        pl.semaphore_signal(barrier, inc=1, device_id={"tp": dev}, device_id_type=MESH)
    w_loads = []
    for i, (src, dst) in enumerate(((wg_hbm, wg), (wu_hbm, wu), (wd_hbm, wd))):
        n = dst.shape[0] // 4
        for j in range(4):
            cp = pltpu.make_async_copy(src.at[layer, pl.ds(j * n, n)], dst.at[pl.ds(j * n, n)], w_sem.at[i, j])
            cp.start()
            w_loads.append(cp)
    pl.semaphore_wait(barrier, 2)

    def send(stage, idx, src, dst, dev):
        cp = pltpu.make_async_remote_copy(src_ref=src, dst_ref=dst, send_sem=s_send.at[stage, idx], recv_sem=s_recv.at[stage, idx],
                                          device_id={"tp": dev}, device_id_type=MESH)
        cp.start()
        return cp

    started = []

    subs = [(g, s, g * rows_g + s * rows_s) for g in range(GROUPS) for s in range(SUB)]
    near = []
    for i, (g, s, r0) in enumerate(subs):
        near.append(send(0, i, part_ref.at[pl.ds(other * half + r0, rows_s)], d1.at[pl.ds(r0, rows_s)], partner))
    far = []
    for i, (g, s, r0) in enumerate(subs):
        near[i].wait_recv()
        rows = pl.ds(r0, rows_s)
        c1[rows, :] = (part_ref[pl.ds(core * half + r0, rows_s), :].astype(F32) + d1[rows, :].astype(F32)).astype(BF16)
        far.append(send(1, i, c1.at[rows], x1.at[rows], across))
    started += near + far

    weight = norm_ref[layer:layer + 1, :].astype(F32)
    gathers1 = {}

    def finish1(g):
        for s in range(SUB):
            i = g * SUB + s
            far[i].wait_recv()
            for r in range(rows_s // 16):
                r0 = g * rows_g + s * rows_s + r * 16
                rows = pl.ds(r0, 16)
                total = (c1[rows, :].astype(F32) + x1[rows, :].astype(F32)).astype(BF16)
                res = x_ref[pl.ds(r0, 16), :] if last else x_ref[pl.ds(core * half + r0, 16), :]
                xn = (res.astype(F32) + total.astype(F32)).astype(BF16)
                x_own[rows, :] = xn
                hbuf[g, core, pl.ds(s * rows_s + r * 16, 16), :] = rms(xn.astype(F32), weight)
            part = hbuf.at[g, core, pl.ds(s * rows_s, rows_s)]
            cp = send(2, i, part, part, partner)
            gathers1[i] = cp
            started.append(cp)

    def wait1(g):
        for s in range(SUB):
            gathers1[g * SUB + s].wait_recv()

    def gate_up(g):
        hid = hbuf.at[g].reshape(2 * rows_g, d)

        def body(n, carry):
            cols = pl.ds(pl.multiple_of(n * 512, 512), 512)
            gate = jnp.dot(hid[...], wg[:, cols], preferred_element_type=F32).astype(BF16).astype(F32)
            up = jnp.dot(hid[...], wu[:, cols], preferred_element_type=F32).astype(BF16).astype(F32)
            abuf[:, cols] = (gate * (1.0 / (1.0 + jnp.exp(-gate))) * up).astype(BF16)
            return carry

        lax.fori_loop(0, wg.shape[1] // 512, body, 0)

    near2, far2 = {}, {}

    def relay2(g, n):
        i = g * NCOL + n
        near2[i].wait_recv()
        cols = pl.ds(n * cols_n, cols_n)
        rows = pl.ds(g * rows_g, rows_g)
        c2[rows, cols] = (pbuf[g, core, :, cols].astype(F32) + d2[rows, cols].astype(F32)).astype(BF16)
        far2[i] = send(4, i, c2.at[rows, cols], x2.at[rows, cols], across)
        started.append(far2[i])

    def down(g, after_first):
        for n in range(NCOL):
            cols = pl.ds(n * cols_n, cols_n)
            y = jnp.dot(abuf[...], wd[:, cols], preferred_element_type=F32).astype(BF16)
            pbuf[g, :, :, cols] = y.reshape(2, rows_g, cols_n)
            i = g * NCOL + n
            near2[i] = send(3, i, pbuf.at[g, other, :, cols], d2.at[pl.ds(g * rows_g, rows_g), cols], partner)
            started.append(near2[i])
            if n == 0 and after_first is not None:
                after_first()
            if n > 0:
                relay2(g, n - 1)
        relay2(g, NCOL - 1)

    gathers2 = {}

    def finish2(g):
        for n in range(NCOL):
            far2[g * NCOL + n].wait_recv()
        if not last:
            nweight = next_norm_ref[layer + 1:layer + 2, :].astype(F32)
        for s in range(SUB):
            for r in range(rows_s // 16):
                r0 = g * rows_g + s * rows_s + r * 16
                rows = pl.ds(r0, 16)
                total = (c2[rows, :].astype(F32) + x2[rows, :].astype(F32)).astype(BF16)
                xn = (x_own[rows, :].astype(F32) + total.astype(F32)).astype(BF16)
                if last:
                    obuf[g, core, pl.ds(s * rows_s + r * 16, 16), :] = xn
                else:
                    xo_ref[rows, :] = xn
                    obuf[g, core, pl.ds(s * rows_s + r * 16, 16), :] = rms(xn.astype(F32), nweight)
            part = obuf.at[g, core, pl.ds(s * rows_s, rows_s)]
            cp = send(5, g * SUB + s, part, part, partner)
            gathers2[g * SUB + s] = cp
            started.append(cp)

    def wait2(g):
        out = xo_ref if last else ho_ref
        for s in range(SUB):
            gathers2[g * SUB + s].wait_recv()
        for c in range(2):
            out[c * half + g * rows_g:c * half + (g + 1) * rows_g, :] = obuf[g, c]

    finish1(0)
    wait1(0)
    for cp in w_loads:
        cp.wait()
    c_loads = []
    for i, (src, dst) in enumerate(zip(carry_in, carry_out)):
        n = dst.shape[0] // 4
        for j in range(4):
            cp = pltpu.make_async_copy(src.at[layer + 1, pl.ds(j * n, n)], dst.at[pl.ds(j * n, n)], c_sem.at[i, j])
            cp.start()
            c_loads.append(cp)
    gate_up(0)
    down(0, lambda: finish1(1))
    wait1(1)
    gate_up(1)
    down(1, None)
    finish2(0)
    wait2(0)
    finish2(1)
    wait2(1)
    for cp in c_loads:
        cp.wait()
    for cp in started:
        cp.wait_send()


def mlp_call(layer, last, x, part, norm, next_norm, wg, wu, wd, carry=()):
    batch, d = part.shape
    half = batch // 2
    rows_g = half // GROUPS
    ff = wg.shape[2]
    n_sem = max(GROUPS * NCOL, GROUPS * SUB)
    own = lambda: pltpu.VMEM((half, d), BF16)
    scratch = [
        pltpu.VMEM(wg.shape[1:], BF16), pltpu.VMEM(wu.shape[1:], BF16), pltpu.VMEM(wd.shape[1:], BF16),
        own(), own(), own(), own(), own(), own(), own(),
        pltpu.VMEM((GROUPS, 2, rows_g, d), BF16), pltpu.VMEM((2 * rows_g, ff), BF16),
        pltpu.VMEM((GROUPS, 2, rows_g, d), BF16), pltpu.VMEM((GROUPS, 2, rows_g, d), BF16),
        pltpu.SemaphoreType.DMA((3, 4)), pltpu.SemaphoreType.DMA((6, 4)), pltpu.SemaphoreType.DMA((6, n_sem)), pltpu.SemaphoreType.DMA((6, n_sem)),
    ]
    full = pltpu.VMEM((batch, d), BF16)
    mine = pltpu.VMEM((half, d), BF16)
    return pl.pallas_call(
        functools.partial(mlp_kernel, layer, last),
        out_shape=full if last else (full, mine) + tuple(pltpu.VMEM(a.shape[1:], BF16) for a in carry),
        in_specs=[VMEM] * 4 + [HBM] * (3 + len(carry)),
        out_specs=VMEM if last else (VMEM,) * (2 + len(carry)),
        scratch_shapes=scratch,
        compiler_params=pltpu.CompilerParams(collective_id=layer, has_side_effects=True, vmem_limit_bytes=(33 if last else 33) * 2**20),
        name=f"mlp{layer}",
    )(x, pltpu.with_memory_space_constraint(part, pltpu.VMEM), norm, next_norm, *in_hbm((wg, wu, wd) + tuple(carry)))


def solution(mesh):
    row_spec = P('dp', None)
    pos_spec = P('dp')
    cache_spec = P(None, 'dp', None, 'tp', None)
    norm_spec = P(None, None)
    col_spec = P(None, None, 'tp')
    split_rows = P(None, 'tp', None)

    def local_step(hidden, positions, k_cache, v_cache, attn_norm, w_query, w_key, w_value, w_out, mlp_norm, w_gate, w_up, w_down):
        shape = k_cache.shape
        flat = shape[:2] + (shape[2] * shape[3], shape[4])
        k_cache, v_cache = k_cache.reshape(flat), v_cache.reshape(flat)
        tables = [jnp.asarray(t) for t in rope_by_position(shape[2], shape[4])]
        part, k_out, v_out = attention_call(0, True, positions, hidden, attn_norm, tables, w_query, w_key, w_value, w_out, k_cache, v_cache, None, None)
        h, x_own, *carried = mlp_call(0, False, hidden, part, mlp_norm, attn_norm, w_gate, w_up, w_down, (w_query, w_key, w_value, w_out, k_cache, v_cache))
        part, k_out, v_out = attention_call(1, False, positions, h, None, tables, *carried, k_out, v_out)[:3]
        hidden = mlp_call(1, True, x_own, part, mlp_norm, attn_norm, w_gate, w_up, w_down)
        return hidden, k_out.reshape(shape), v_out.reshape(shape)

    return jax.shard_map(local_step, mesh=mesh, in_specs=(row_spec, pos_spec, cache_spec, cache_spec, norm_spec, col_spec, col_spec, col_spec, split_rows, norm_spec, col_spec, col_spec, split_rows), out_specs=(row_spec, cache_spec, cache_spec), check_vma=False)
```

```python
import functools
import math

import jax
import jax.numpy as jnp
import numpy as np
from jax import lax
from jax.experimental import pallas as pl
from jax.experimental.pallas import tpu as pltpu
from jax.sharding import PartitionSpec as P

MESH = pl.DeviceIdType.MESH
BF16 = jnp.bfloat16
F32 = jnp.float32
ANY = pl.BlockSpec(memory_space=pl.ANY)
HBM = pl.BlockSpec(memory_space=pltpu.HBM)
VMEM = pl.BlockSpec(memory_space=pltpu.VMEM)
SMEM = pl.BlockSpec(memory_space=pltpu.SMEM)


def rope_by_position(seq_len, head_dim):
    half = head_dim // 2
    inv_freq = np.power(np.float32(500000.0), -np.arange(half, dtype=np.float32) * np.float32(2.0 / head_dim)).astype(np.float32)
    wavelen = np.float32(2.0 * math.pi) / inv_freq
    smooth = (np.float32(8192.0) / wavelen - np.float32(1.0)) / np.float32(3.0)
    blended = (np.float32(1.0) - smooth) * inv_freq / np.float32(8.0) + smooth * inv_freq
    scaled = np.where(wavelen < 2048.0, inv_freq, np.where(wavelen > 8192.0, inv_freq / np.float32(8.0), blended)).astype(np.float32)
    angles = np.arange(seq_len, dtype=np.float32)[:, None] * scaled[None, :]
    cos = np.cos(angles.astype(np.float64)).astype(np.float32)
    sin = np.sin(angles.astype(np.float64)).astype(np.float32)
    return np.concatenate([cos, cos], axis=1), np.concatenate([-sin, sin], axis=1)


def norm_block(read, weight, write, width):
    step = 256
    acc = None
    for j in range(width // step):
        v = read(j * step, step)
        sq = v * v
        acc = sq if acc is None else acc + sq
    scale = lax.rsqrt(jnp.sum(acc, axis=-1, keepdims=True) * (1.0 / width) + 1e-5)
    for j in range(width // step):
        write(j * step, step, (read(j * step, step) * scale * weight(j * step, step)).astype(BF16))


def in_hbm(arrays):
    return [pltpu.with_memory_space_constraint(a, pltpu.HBM) for a in arrays]


def attention_kernel(layer, first, chunk, *refs):
    refs = list(refs)
    pos_ref = refs.pop(0)
    x_in = refs.pop(0)
    norm_ref = refs.pop(0) if first else None
    cos_tab, sin_tab, wq_hbm, wk_hbm, wv_hbm, wo_hbm, kc_hbm, vc_hbm = refs[:8]
    refs = refs[8:]
    if first:
        part_ref, ko_hbm, vo_hbm = refs[:3]
        x_ref, wq, wk, wv, wo, kbuf, vbuf, h_scr = refs[3:11]
        refs = refs[11:]
    else:
        x_ref, wq, wk, wv, wo = x_in, wq_hbm, wk_hbm, wv_hbm, wo_hbm
        part_ref, ko_hbm, vo_hbm, kbuf, vbuf = refs[2:7]
        refs = refs[7:]
    (cos_scr, sin_scr, lim_scr, q_scr, k_scr, v_scr, p_scr, o_scr, w_sem, in_sem, out_sem) = refs
    batch = x_ref.shape[0]
    n_q = wq.shape[1] // 128
    n_kv = wk.shape[1] // 128
    group = n_q // n_kv
    rows_kv = kbuf.shape[1]
    n_chunks = batch // chunk

    if first:
        x_load = pltpu.make_async_copy(x_in, x_ref, w_sem.at[4])
        x_load.start()
        loads = []
        for i, (src, dst) in enumerate(((wq_hbm, wq), (wk_hbm, wk), (wv_hbm, wv))):
            loads.append(pltpu.make_async_copy(src.at[layer], dst, w_sem.at[i]))
        for c in loads:
            c.start()
        kv_loads = []
        for c in range(n_chunks):
            rows = pl.ds(c * chunk, chunk)
            a = pltpu.make_async_copy(kc_hbm.at[layer, rows], kbuf.at[rows], in_sem.at[0, c])
            b = pltpu.make_async_copy(vc_hbm.at[layer, rows], vbuf.at[rows], in_sem.at[1, c])
            a.start()
            b.start()
            kv_loads.append((a, b))
        wo_load = pltpu.make_async_copy(wo_hbm.at[layer], wo, w_sem.at[3])
        wo_load.start()

    per_row = 128 // n_q
    lane_request = lax.broadcasted_iota(jnp.int32, (1, 128), 1) // n_q

    def table_body(i, carry):
        limit = jnp.zeros((1, 128), jnp.int32)
        for u in range(per_row):
            b = i * per_row + u
            pos = pos_ref[b]
            cos_scr[pl.ds(b, 1), :] = cos_tab[pl.ds(pos, 1), :]
            sin_scr[pl.ds(b, 1), :] = sin_tab[pl.ds(pos, 1), :]
            limit = jnp.where(lane_request == u, pos * n_kv + n_kv - 1, limit)
        lim_scr[pl.ds(i, 1), :] = limit
        return carry

    lax.fori_loop(0, batch // per_row, table_body, 0)

    if first:
        x_load.wait()
        def norm_body(i, carry):
            rows = pl.ds(pl.multiple_of(i * 16, 16), 16)

            def write(j, n, v):
                h_scr[rows, j:j + n] = v

            norm_block(lambda j, n: x_ref[rows, j:j + n].astype(F32), lambda j, n: norm_ref[layer:layer + 1, j:j + n].astype(F32), write, h_scr.shape[1])
            return carry

        lax.fori_loop(0, batch // 16, norm_body, 0)
        h_src = h_scr
    else:
        h_src = x_ref

    def rope(v):
        v = v.astype(BF16).astype(F32)
        return v * cos_scr[...] + pltpu.roll(v, 64, 1) * sin_scr[...]

    h = h_src[...]
    if first:
        loads[0].wait()
    q = jnp.dot(h, wq[...], preferred_element_type=F32)
    for j in range(n_q):
        q_scr[pl.ds(j, batch, n_q), :] = rope(q[:, j * 128:(j + 1) * 128])
    if first:
        loads[1].wait()
    k = jnp.dot(h, wk[...], preferred_element_type=F32)
    for j in range(n_kv):
        k_scr[pl.ds(j, batch, n_kv), :] = rope(k[:, j * 128:(j + 1) * 128])
    if first:
        loads[2].wait()
    v = jnp.dot(h, wv[...], preferred_element_type=F32)
    for j in range(n_kv):
        v_scr[pl.ds(j, batch, n_kv), :] = v[:, j * 128:(j + 1) * 128]

    kmat = kbuf.reshape(batch * rows_kv, 128)
    vmat = vbuf.reshape(batch * rows_kv, 128)
    scale = 128 ** -0.5
    pair = 2 * n_q
    row_id = lax.broadcasted_iota(jnp.int32, (2 * pair, 128), 0)
    first_pair = row_id < pair
    first_in_pair = (row_id % pair) < n_q
    zero = jnp.zeros((2 * pair, 128), F32)
    quads = chunk // 4
    cols = chunk * n_q
    lane = lax.broadcasted_iota(jnp.int32, (rows_kv, cols), 1)
    row = lax.broadcasted_iota(jnp.int32, (rows_kv, cols), 0)
    same_head = (row % n_kv) == (lane % n_q) // group
    first_of_two = (lane // n_q) % 2 == 0
    lane_pair = lax.broadcasted_iota(jnp.int32, (128, 128), 1) // pair
    no_tile = jnp.zeros((128, 128), BF16)
    pairs_per_tile = 128 // pair
    per_tile = 16 // n_kv
    shift = per_tile.bit_length() - 1
    tile_row = lax.broadcasted_iota(jnp.int32, (16, 128), 0) // n_kv
    tile_head = lax.broadcasted_iota(jnp.int32, (8, 128), 0) % n_kv

    def square(mat, base):
        top = mat[pl.ds(base, 2 * rows_kv), :]
        bottom = mat[pl.ds(base + 2 * rows_kv, 2 * rows_kv), :]
        return jnp.concatenate([top, bottom], axis=1)

    stores = []
    for c in range(n_chunks):
        rows = pl.ds(c * chunk, chunk)
        stores.append((pltpu.make_async_copy(kbuf.at[rows], ko_hbm.at[layer, rows], out_sem.at[0, c]),
                       pltpu.make_async_copy(vbuf.at[rows], vo_hbm.at[layer, rows], out_sem.at[1, c])))

    for c in range(n_chunks):
        if first:
            kv_loads[c][0].wait()
            kv_loads[c][1].wait()

        for i in range(c * chunk, (c + 1) * chunk, 8):
            writes = []
            for b in range(i, i + 8):
                pos = pos_ref[b]
                block = pl.ds(pl.multiple_of(lax.shift_left(lax.shift_right_logical(pos, shift), 4), 16), 16)
                here = tile_row == lax.bitwise_and(pos, per_tile - 1)
                for buf, new in ((kbuf, k_scr), (vbuf, v_scr)):
                    fresh = jnp.broadcast_to(new[b * n_kv:b * n_kv + 1, :], (8, 128))
                    for j in range(1, n_kv):
                        fresh = jnp.where(tile_head == j, new[b * n_kv + j:b * n_kv + j + 1, :], fresh)
                    value = jnp.where(here, jnp.concatenate([fresh, fresh], axis=0), buf[b, block, :].astype(F32))
                    writes.append((buf, b, block, value.astype(BF16)))
            for buf, b, block, value in writes:
                buf[b, block, :] = value

        q_t = q_scr[pl.ds(c * cols, cols), :].T
        acc = None
        for t in range(quads):
            halves = []
            for i in range(2):
                p = 2 * t + i
                tile = p // pairs_per_tile
                tiles = [no_tile] * (cols // 128)
                tiles[tile] = jnp.where(lane_pair == p % pairs_per_tile, q_t[:, tile * 128:(tile + 1) * 128], 0.0).astype(BF16)
                halves.append(jnp.concatenate(tiles, axis=1))
            d = jnp.dot(square(kmat, (c * chunk + t * 4) * rows_kv), jnp.concatenate(halves, axis=0), preferred_element_type=F32)
            acc = d if acc is None else acc + d
        stores[c][0].start()
        stores[c][1].start()
        s = jnp.where(first_of_two, acc[:rows_kv], acc[rows_kv:])
        limit = jnp.concatenate([lim_scr[pl.ds(c * (cols // 128) + j, 1), :] for j in range(cols // 128)], axis=1)
        s = jnp.where(same_head & (row <= limit), s * scale, -jnp.inf)
        e = jnp.exp(s - jnp.max(s, axis=0, keepdims=True))
        p_scr[...] = (e * (1.0 / jnp.sum(e, axis=0, keepdims=True))).T
        for t in range(quads):
            b = c * chunk + t * 4
            p4 = p_scr[pl.ds(t * 2 * pair, 2 * pair), :]
            wide = jnp.concatenate([jnp.where(first_in_pair, p4, zero), jnp.where(first_in_pair, zero, p4)], axis=1).astype(BF16)
            o = jnp.dot(wide, square(vmat, b * rows_kv), preferred_element_type=F32)
            o_scr[pl.ds(b * n_q, 2 * pair), :] = jnp.where(first_pair, o[:, :128], o[:, 128:])

    att = jnp.concatenate([o_scr[pl.ds(j, batch, n_q), :].astype(BF16) for j in range(n_q)], axis=1)
    if first:
        wo_load.wait()
    for n in range(wo.shape[1] // 512):
        cols_n = pl.ds(n * 512, 512)
        part_ref[:, cols_n] = jnp.dot(att, wo[:, cols_n], preferred_element_type=F32).astype(BF16)
    for a, b in stores:
        a.wait()
        b.wait()


def attention_call(layer, first, positions, x, norm, tables, wq, wk, wv, wo, kc, vc, k_out, v_out):
    batch, d = x.shape
    hd = kc.shape[-1]
    n_q, n_kv = wq.shape[-1] // hd, wk.shape[-1] // hd
    chunk = 64
    n_chunks = batch // chunk
    if first:
        ins = [positions] + in_hbm([x]) + [norm, tables[0], tables[1]] + in_hbm([wq, wk, wv, wo, kc, vc])
    else:
        ins = [positions, x, tables[0], tables[1], wq, wk, wv, wo, kc, vc]
    part = pltpu.VMEM((batch, d), BF16)
    if first:
        specs = [SMEM, HBM, VMEM, VMEM, VMEM] + [HBM] * 6
        outs = (part, pltpu.HBM(kc.shape, BF16), pltpu.HBM(vc.shape, BF16))
        out_specs = (VMEM, HBM, HBM)
        aliases = {}
        big = [(batch, d), wq.shape[1:], wk.shape[1:], wv.shape[1:], wo.shape[1:], kc.shape[1:], vc.shape[1:], (batch, d)]
    else:
        specs = [SMEM, VMEM, VMEM, VMEM] + [VMEM] * 6 + [HBM] * 2
        aliases = {len(ins): 1, len(ins) + 1: 2, len(ins) - 2: 3, len(ins) - 1: 4}
        outs = (part, pltpu.HBM(k_out.shape, BF16), pltpu.HBM(v_out.shape, BF16), pltpu.VMEM(kc.shape, BF16), pltpu.VMEM(vc.shape, BF16))
        ins += in_hbm([k_out, v_out])
        out_specs = (VMEM, HBM, HBM, VMEM, VMEM)
        big = []
    scratch = [pltpu.VMEM(shape, BF16) for shape in big] + [
        pltpu.VMEM((batch, hd), F32), pltpu.VMEM((batch, hd), F32), pltpu.VMEM((batch * n_q // hd, hd), jnp.int32),
        pltpu.VMEM((batch * n_q, hd), F32), pltpu.VMEM((batch * n_kv, hd), F32), pltpu.VMEM((batch * n_kv, hd), F32),
        pltpu.VMEM((chunk * n_q, hd), F32), pltpu.VMEM((batch * n_q, hd), F32),
        pltpu.SemaphoreType.DMA((5,)), pltpu.SemaphoreType.DMA((2, n_chunks)), pltpu.SemaphoreType.DMA((2, n_chunks)),
    ]
    return pl.pallas_call(
        functools.partial(attention_kernel, layer, first, chunk),
        out_shape=outs,
        in_specs=specs,
        out_specs=out_specs,
        scratch_shapes=scratch,
        input_output_aliases=aliases,
        compiler_params=pltpu.CompilerParams(vmem_limit_bytes=(62 if first else 8) * 2**20),
        name=f"attention{layer}",
    )(*ins)


GROUPS = 2
SUB = 2
NCOL = 4


def mlp_kernel(layer, last, x_ref, part_ref, norm_ref, next_norm_ref, wg_hbm, wu_hbm, wd_hbm, *refs):
    if last:
        carry_in, carry_out = (), ()
        (xo_ref,), refs = refs[:1], refs[1:]
    else:
        carry_in, (ho_ref, xo_ref), carry_out, refs = refs[:6], refs[6:8], refs[8:14], refs[14:]
    (wg, wu, wd, d1, c1, x1, d2, c2, x2, x_own, hbuf, abuf, pbuf, obuf, w_sem, c_sem, s_send, s_recv) = refs
    t = lax.axis_index("tp")
    core = lax.rem(t, 2)
    other = 1 - core
    partner = t + other - core
    across = lax.rem(t + 2, 4)
    d = x_ref.shape[1]
    half = d1.shape[0]
    rows_g = half // GROUPS
    rows_s = rows_g // SUB
    cols_n = d // NCOL

    barrier = pltpu.get_barrier_semaphore()
    for dev in (partner, across):
        pl.semaphore_signal(barrier, inc=1, device_id={"tp": dev}, device_id_type=MESH)
    w_loads = []
    for i, (src, dst) in enumerate(((wg_hbm, wg), (wu_hbm, wu), (wd_hbm, wd))):
        n = dst.shape[0] // 4
        for j in range(4):
            cp = pltpu.make_async_copy(src.at[layer, pl.ds(j * n, n)], dst.at[pl.ds(j * n, n)], w_sem.at[i, j])
            cp.start()
            w_loads.append(cp)
    pl.semaphore_wait(barrier, 2)

    def send(stage, idx, src, dst, dev):
        cp = pltpu.make_async_remote_copy(src_ref=src, dst_ref=dst, send_sem=s_send.at[stage, idx], recv_sem=s_recv.at[stage, idx],
                                          device_id={"tp": dev}, device_id_type=MESH)
        cp.start()
        return cp

    started = []

    def add_norm(mine, theirs, res, res_row, row, x_to, w_ref, w_row, dst, dst_row):
        rows = pl.ds(row, 16)
        to = pl.ds(dst_row, 16)

        def total(j, n):
            t = (mine[rows, j:j + n].astype(F32) + theirs[rows, j:j + n].astype(F32)).astype(BF16).astype(F32)
            return (res[pl.ds(res_row, 16), j:j + n].astype(F32) + t).astype(BF16)

        if w_ref is None:
            for j in range(0, d, 256):
                dst[to, j:j + 256] = total(j, 256)
            return

        def keep(j, n):
            v = total(j, n)
            x_to[rows, j:j + n] = v
            return v.astype(F32)

        first_pass = [True] * (d // 256)

        def read(j, n):
            if first_pass[j // 256]:
                first_pass[j // 256] = False
                return keep(j, n)
            return x_to[rows, j:j + n].astype(F32)

        def write(j, n, v):
            dst[to, j:j + n] = v

        norm_block(read, lambda j, n: w_ref[w_row:w_row + 1, j:j + n].astype(F32), write, d)

    subs = [(g, s, g * rows_g + s * rows_s) for g in range(GROUPS) for s in range(SUB)]
    near = []
    for i, (g, s, r0) in enumerate(subs):
        near.append(send(0, i, part_ref.at[pl.ds(other * half + r0, rows_s)], d1.at[pl.ds(r0, rows_s)], partner))
    far = []
    for i, (g, s, r0) in enumerate(subs):
        near[i].wait_recv()
        rows = pl.ds(r0, rows_s)
        c1[rows, :] = (part_ref[pl.ds(core * half + r0, rows_s), :].astype(F32) + d1[rows, :].astype(F32)).astype(BF16)
        far.append(send(1, i, c1.at[rows], x1.at[rows], across))
    started += near + far

    gathers1 = {}

    def finish1(g):
        for s in range(SUB):
            i = g * SUB + s
            far[i].wait_recv()
            for r in range(rows_s // 16):
                r0 = g * rows_g + s * rows_s + r * 16
                rows = pl.ds(r0, 16)
                add_norm(c1, x1, x_ref, r0 if last else core * half + r0, r0, x_own, norm_ref, layer, hbuf.at[g, core], s * rows_s + r * 16)
            part = hbuf.at[g, core, pl.ds(s * rows_s, rows_s)]
            cp = send(2, i, part, part, partner)
            gathers1[i] = cp
            started.append(cp)

    def wait1(g):
        for s in range(SUB):
            gathers1[g * SUB + s].wait_recv()

    def gate_up(g):
        hid = hbuf.at[g].reshape(2 * rows_g, d)

        def body(n, carry):
            cols = pl.ds(pl.multiple_of(n * 512, 512), 512)
            gate = jnp.dot(hid[...], wg[:, cols], preferred_element_type=F32).astype(BF16).astype(F32)
            up = jnp.dot(hid[...], wu[:, cols], preferred_element_type=F32).astype(BF16).astype(F32)
            abuf[:, cols] = (gate * (1.0 / (1.0 + jnp.exp(-gate))) * up).astype(BF16)
            return carry

        lax.fori_loop(0, wg.shape[1] // 512, body, 0)

    near2, far2 = {}, {}

    def relay2(g, n):
        i = g * NCOL + n
        near2[i].wait_recv()
        cols = pl.ds(n * cols_n, cols_n)
        rows = pl.ds(g * rows_g, rows_g)
        c2[rows, cols] = (pbuf[g, core, :, cols].astype(F32) + d2[rows, cols].astype(F32)).astype(BF16)
        far2[i] = send(4, i, c2.at[rows, cols], x2.at[rows, cols], across)
        started.append(far2[i])

    def down(g, after_first):
        for n in range(NCOL):
            cols = pl.ds(n * cols_n, cols_n)
            y = jnp.dot(abuf[...], wd[:, cols], preferred_element_type=F32).astype(BF16)
            pbuf[g, :, :, cols] = y.reshape(2, rows_g, cols_n)
            i = g * NCOL + n
            near2[i] = send(3, i, pbuf.at[g, other, :, cols], d2.at[pl.ds(g * rows_g, rows_g), cols], partner)
            started.append(near2[i])
            if n == 0 and after_first is not None:
                after_first()
            if n > 0:
                relay2(g, n - 1)
        relay2(g, NCOL - 1)

    gathers2 = {}

    def finish2(g):
        for n in range(NCOL):
            far2[g * NCOL + n].wait_recv()
        for s in range(SUB):
            for r in range(rows_s // 16):
                r0 = g * rows_g + s * rows_s + r * 16
                if last:
                    add_norm(c2, x2, x_own, r0, r0, None, None, 0, obuf.at[g, core], s * rows_s + r * 16)
                else:
                    add_norm(c2, x2, x_own, r0, r0, xo_ref, next_norm_ref, layer + 1, obuf.at[g, core], s * rows_s + r * 16)
            part = obuf.at[g, core, pl.ds(s * rows_s, rows_s)]
            cp = send(5, g * SUB + s, part, part, partner)
            gathers2[g * SUB + s] = cp
            started.append(cp)

    def wait2(g):
        out = xo_ref if last else ho_ref
        for s in range(SUB):
            gathers2[g * SUB + s].wait_recv()
        for c in range(2):
            out[c * half + g * rows_g:c * half + (g + 1) * rows_g, :] = obuf[g, c]

    finish1(0)
    wait1(0)
    for cp in w_loads:
        cp.wait()
    c_loads = []
    for i, (src, dst) in enumerate(zip(carry_in, carry_out)):
        n = dst.shape[0] // 4
        for j in range(4):
            cp = pltpu.make_async_copy(src.at[layer + 1, pl.ds(j * n, n)], dst.at[pl.ds(j * n, n)], c_sem.at[i, j])
            cp.start()
            c_loads.append(cp)
    gate_up(0)
    down(0, lambda: finish1(1))
    wait1(1)
    gate_up(1)
    down(1, None)
    finish2(0)
    wait2(0)
    finish2(1)
    wait2(1)
    for cp in c_loads:
        cp.wait()
    for cp in started:
        cp.wait_send()


def mlp_call(layer, last, x, part, norm, next_norm, wg, wu, wd, carry=()):
    batch, d = part.shape
    half = batch // 2
    rows_g = half // GROUPS
    ff = wg.shape[2]
    n_sem = max(GROUPS * NCOL, GROUPS * SUB)
    own = lambda: pltpu.VMEM((half, d), BF16)
    scratch = [
        pltpu.VMEM(wg.shape[1:], BF16), pltpu.VMEM(wu.shape[1:], BF16), pltpu.VMEM(wd.shape[1:], BF16),
        own(), own(), own(), own(), own(), own(), own(),
        pltpu.VMEM((GROUPS, 2, rows_g, d), BF16), pltpu.VMEM((2 * rows_g, ff), BF16),
        pltpu.VMEM((GROUPS, 2, rows_g, d), BF16), pltpu.VMEM((GROUPS, 2, rows_g, d), BF16),
        pltpu.SemaphoreType.DMA((3, 4)), pltpu.SemaphoreType.DMA((6, 4)), pltpu.SemaphoreType.DMA((6, n_sem)), pltpu.SemaphoreType.DMA((6, n_sem)),
    ]
    full = pltpu.VMEM((batch, d), BF16)
    mine = pltpu.VMEM((half, d), BF16)
    return pl.pallas_call(
        functools.partial(mlp_kernel, layer, last),
        out_shape=full if last else (full, mine) + tuple(pltpu.VMEM(a.shape[1:], BF16) for a in carry),
        in_specs=[VMEM] * 4 + [HBM] * (3 + len(carry)),
        out_specs=VMEM if last else (VMEM,) * (2 + len(carry)),
        scratch_shapes=scratch,
        compiler_params=pltpu.CompilerParams(collective_id=layer, has_side_effects=True, vmem_limit_bytes=(33 if last else 33) * 2**20),
        name=f"mlp{layer}",
    )(x, pltpu.with_memory_space_constraint(part, pltpu.VMEM), norm, next_norm, *in_hbm((wg, wu, wd) + tuple(carry)))


def solution(mesh):
    row_spec = P('dp', None)
    pos_spec = P('dp')
    cache_spec = P(None, 'dp', None, 'tp', None)
    norm_spec = P(None, None)
    col_spec = P(None, None, 'tp')
    split_rows = P(None, 'tp', None)

    def local_step(hidden, positions, k_cache, v_cache, attn_norm, w_query, w_key, w_value, w_out, mlp_norm, w_gate, w_up, w_down):
        shape = k_cache.shape
        flat = shape[:2] + (shape[2] * shape[3], shape[4])
        k_cache, v_cache = k_cache.reshape(flat), v_cache.reshape(flat)
        tables = [jnp.asarray(t) for t in rope_by_position(shape[2], shape[4])]
        part, k_out, v_out = attention_call(0, True, positions, hidden, attn_norm, tables, w_query, w_key, w_value, w_out, k_cache, v_cache, None, None)
        h, x_own, *carried = mlp_call(0, False, hidden, part, mlp_norm, attn_norm, w_gate, w_up, w_down, (w_query, w_key, w_value, w_out, k_cache, v_cache))
        part, k_out, v_out = attention_call(1, False, positions, h, None, tables, *carried, k_out, v_out)[:3]
        hidden = mlp_call(1, True, x_own, part, mlp_norm, attn_norm, w_gate, w_up, w_down)
        return hidden, k_out.reshape(shape), v_out.reshape(shape)

    return jax.shard_map(local_step, mesh=mesh, in_specs=(row_spec, pos_spec, cache_spec, cache_spec, norm_spec, col_spec, col_spec, col_spec, split_rows, norm_spec, col_spec, col_spec, split_rows), out_specs=(row_spec, cache_spec, cache_spec), check_vma=False)
```

```python
import functools
import math

import jax
import jax.numpy as jnp
import numpy as np
from jax import lax
from jax.experimental import pallas as pl
from jax.experimental.pallas import tpu as pltpu
from jax.sharding import PartitionSpec as P

MESH = pl.DeviceIdType.MESH
BF16 = jnp.bfloat16
F32 = jnp.float32
ANY = pl.BlockSpec(memory_space=pl.ANY)
HBM = pl.BlockSpec(memory_space=pltpu.HBM)
VMEM = pl.BlockSpec(memory_space=pltpu.VMEM)
SMEM = pl.BlockSpec(memory_space=pltpu.SMEM)


def rope_by_position(seq_len, head_dim):
    half = head_dim // 2
    inv_freq = np.power(np.float32(500000.0), -np.arange(half, dtype=np.float32) * np.float32(2.0 / head_dim)).astype(np.float32)
    wavelen = np.float32(2.0 * math.pi) / inv_freq
    smooth = (np.float32(8192.0) / wavelen - np.float32(1.0)) / np.float32(3.0)
    blended = (np.float32(1.0) - smooth) * inv_freq / np.float32(8.0) + smooth * inv_freq
    scaled = np.where(wavelen < 2048.0, inv_freq, np.where(wavelen > 8192.0, inv_freq / np.float32(8.0), blended)).astype(np.float32)
    angles = np.arange(seq_len, dtype=np.float32)[:, None] * scaled[None, :]
    cos = np.cos(angles.astype(np.float64)).astype(np.float32)
    sin = np.sin(angles.astype(np.float64)).astype(np.float32)
    return np.concatenate([cos, cos], axis=1), np.concatenate([-sin, sin], axis=1)


def norm_block(read, weight, write, width):
    step = 256
    acc = None
    for j in range(width // step):
        v = read(j * step, step)
        sq = v * v
        acc = sq if acc is None else acc + sq
    scale = lax.rsqrt(jnp.sum(acc, axis=-1, keepdims=True) * (1.0 / width) + 1e-5)
    for j in range(width // step):
        write(j * step, step, (read(j * step, step) * scale * weight(j * step, step)).astype(BF16))


def in_hbm(arrays):
    return [pltpu.with_memory_space_constraint(a, pltpu.HBM) for a in arrays]


def attention_kernel(layer, first, chunk, *refs):
    refs = list(refs)
    pos_ref = refs.pop(0)
    x_in = refs.pop(0)
    norm_ref = refs.pop(0) if first else None
    cos_tab, sin_tab, wq_hbm, wk_hbm, wv_hbm, wo_hbm, kc_hbm, vc_hbm = refs[:8]
    refs = refs[8:]
    if first:
        part_ref, ko_hbm, vo_hbm = refs[:3]
        x_ref, wq, wk, wv, wo, kbuf, vbuf, h_scr = refs[3:11]
        refs = refs[11:]
    else:
        x_ref, wq, wk, wv, wo = x_in, wq_hbm, wk_hbm, wv_hbm, wo_hbm
        part_ref, ko_hbm, vo_hbm, kbuf, vbuf = refs[2:7]
        refs = refs[7:]
    (cos_scr, sin_scr, lim_scr, q_scr, k_scr, v_scr, p_scr, o_scr, w_sem, in_sem, out_sem) = refs
    batch = x_ref.shape[0]
    n_q = wq.shape[1] // 128
    n_kv = wk.shape[1] // 128
    group = n_q // n_kv
    rows_kv = kbuf.shape[1]
    n_chunks = batch // chunk

    if first:
        x_load = pltpu.make_async_copy(x_in, x_ref, w_sem.at[4])
        x_load.start()
        loads = []
        for i, (src, dst) in enumerate(((wq_hbm, wq), (wk_hbm, wk), (wv_hbm, wv))):
            loads.append(pltpu.make_async_copy(src.at[layer], dst, w_sem.at[i]))
        for c in loads:
            c.start()
        kv_loads = []
        for c in range(n_chunks):
            rows = pl.ds(c * chunk, chunk)
            a = pltpu.make_async_copy(kc_hbm.at[layer, rows], kbuf.at[rows], in_sem.at[0, c])
            b = pltpu.make_async_copy(vc_hbm.at[layer, rows], vbuf.at[rows], in_sem.at[1, c])
            a.start()
            b.start()
            kv_loads.append((a, b))
        wo_load = pltpu.make_async_copy(wo_hbm.at[layer], wo, w_sem.at[3])
        wo_load.start()

    per_row = 128 // n_q
    lane_request = lax.broadcasted_iota(jnp.int32, (1, 128), 1) // n_q

    def table_body(i, carry):
        limit = jnp.zeros((1, 128), jnp.int32)
        for u in range(per_row):
            b = i * per_row + u
            pos = pos_ref[b]
            cos_scr[pl.ds(b, 1), :] = cos_tab[pl.ds(pos, 1), :]
            sin_scr[pl.ds(b, 1), :] = sin_tab[pl.ds(pos, 1), :]
            limit = jnp.where(lane_request == u, pos * n_kv + n_kv - 1, limit)
        lim_scr[pl.ds(i, 1), :] = limit
        return carry

    lax.fori_loop(0, batch // per_row, table_body, 0)

    if first:
        x_load.wait()
        def norm_body(i, carry):
            rows = pl.ds(pl.multiple_of(i * 16, 16), 16)

            def write(j, n, v):
                h_scr[rows, j:j + n] = v

            norm_block(lambda j, n: x_ref[rows, j:j + n].astype(F32), lambda j, n: norm_ref[layer:layer + 1, j:j + n].astype(F32), write, h_scr.shape[1])
            return carry

        lax.fori_loop(0, batch // 16, norm_body, 0)
        h_src = h_scr
    else:
        h_src = x_ref

    def rope(v):
        v = v.astype(BF16).astype(F32)
        return v * cos_scr[...] + pltpu.roll(v, 64, 1) * sin_scr[...]

    h = h_src[...]
    if first:
        loads[0].wait()
    q = jnp.dot(h, wq[...], preferred_element_type=F32)
    for j in range(n_q):
        q_scr[pl.ds(j, batch, n_q), :] = rope(q[:, j * 128:(j + 1) * 128])
    if first:
        loads[1].wait()
    k = jnp.dot(h, wk[...], preferred_element_type=F32)
    for j in range(n_kv):
        k_scr[pl.ds(j, batch, n_kv), :] = rope(k[:, j * 128:(j + 1) * 128])
    if first:
        loads[2].wait()
    v = jnp.dot(h, wv[...], preferred_element_type=F32)
    for j in range(n_kv):
        v_scr[pl.ds(j, batch, n_kv), :] = v[:, j * 128:(j + 1) * 128]

    kmat = kbuf.reshape(batch * rows_kv, 128)
    vmat = vbuf.reshape(batch * rows_kv, 128)
    scale = 128 ** -0.5
    pair = 2 * n_q
    row_id = lax.broadcasted_iota(jnp.int32, (2 * pair, 128), 0)
    first_pair = row_id < pair
    first_in_pair = (row_id % pair) < n_q
    zero = jnp.zeros((2 * pair, 128), F32)
    quads = chunk // 4
    cols = chunk * n_q
    lane = lax.broadcasted_iota(jnp.int32, (rows_kv, cols), 1)
    row = lax.broadcasted_iota(jnp.int32, (rows_kv, cols), 0)
    same_head = (row % n_kv) == (lane % n_q) // group
    first_of_two = (lane // n_q) % 2 == 0
    lane_pair = lax.broadcasted_iota(jnp.int32, (128, 128), 1) // pair
    no_tile = jnp.zeros((128, 128), BF16)
    pairs_per_tile = 128 // pair
    per_tile = 16 // n_kv
    shift = per_tile.bit_length() - 1
    tile_row = lax.broadcasted_iota(jnp.int32, (16, 128), 0) // n_kv
    tile_head = lax.broadcasted_iota(jnp.int32, (8, 128), 0) % n_kv

    def square(mat, base):
        top = mat[pl.ds(base, 2 * rows_kv), :]
        bottom = mat[pl.ds(base + 2 * rows_kv, 2 * rows_kv), :]
        return jnp.concatenate([top, bottom], axis=1)

    stores = []
    for c in range(n_chunks):
        rows = pl.ds(c * chunk, chunk)
        stores.append((pltpu.make_async_copy(kbuf.at[rows], ko_hbm.at[layer, rows], out_sem.at[0, c]),
                       pltpu.make_async_copy(vbuf.at[rows], vo_hbm.at[layer, rows], out_sem.at[1, c])))

    def values(c):
        for t in range(quads):
            b = c * chunk + t * 4
            p4 = p_scr[c % 2, pl.ds(t * 2 * pair, 2 * pair), :]
            wide = jnp.concatenate([jnp.where(first_in_pair, p4, zero), jnp.where(first_in_pair, zero, p4)], axis=1).astype(BF16)
            o = jnp.dot(wide, square(vmat, b * rows_kv), preferred_element_type=F32)
            o_scr[pl.ds(b * n_q, 2 * pair), :] = jnp.where(first_pair, o[:, :128], o[:, 128:])

    for c in range(n_chunks):
        if first:
            kv_loads[c][0].wait()
            kv_loads[c][1].wait()

        for i in range(c * chunk, (c + 1) * chunk, 8):
            writes = []
            for b in range(i, i + 8):
                pos = pos_ref[b]
                block = pl.ds(pl.multiple_of(lax.shift_left(lax.shift_right_logical(pos, shift), 4), 16), 16)
                here = tile_row == lax.bitwise_and(pos, per_tile - 1)
                for buf, new in ((kbuf, k_scr), (vbuf, v_scr)):
                    fresh = jnp.broadcast_to(new[b * n_kv:b * n_kv + 1, :], (8, 128))
                    for j in range(1, n_kv):
                        fresh = jnp.where(tile_head == j, new[b * n_kv + j:b * n_kv + j + 1, :], fresh)
                    value = jnp.where(here, jnp.concatenate([fresh, fresh], axis=0), buf[b, block, :].astype(F32))
                    writes.append((buf, b, block, value.astype(BF16)))
            for buf, b, block, value in writes:
                buf[b, block, :] = value

        q_t = q_scr[pl.ds(c * cols, cols), :].T
        acc = None
        for t in range(quads):
            halves = []
            for i in range(2):
                p = 2 * t + i
                tile = p // pairs_per_tile
                tiles = [no_tile] * (cols // 128)
                tiles[tile] = jnp.where(lane_pair == p % pairs_per_tile, q_t[:, tile * 128:(tile + 1) * 128], 0.0).astype(BF16)
                halves.append(jnp.concatenate(tiles, axis=1))
            d = jnp.dot(square(kmat, (c * chunk + t * 4) * rows_kv), jnp.concatenate(halves, axis=0), preferred_element_type=F32)
            acc = d if acc is None else acc + d
        if c > 0:
            values(c - 1)
        stores[c][0].start()
        stores[c][1].start()
        s = jnp.where(first_of_two, acc[:rows_kv], acc[rows_kv:])
        limit = jnp.concatenate([lim_scr[pl.ds(c * (cols // 128) + j, 1), :] for j in range(cols // 128)], axis=1)
        s = jnp.where(same_head & (row <= limit), s * scale, -jnp.inf)
        e = jnp.exp(s - jnp.max(s, axis=0, keepdims=True))
        p_scr[c % 2] = (e * (1.0 / jnp.sum(e, axis=0, keepdims=True))).T
    values(n_chunks - 1)

    att = jnp.concatenate([o_scr[pl.ds(j, batch, n_q), :].astype(BF16) for j in range(n_q)], axis=1)
    if first:
        wo_load.wait()
    for n in range(wo.shape[1] // 512):
        cols_n = pl.ds(n * 512, 512)
        part_ref[:, cols_n] = jnp.dot(att, wo[:, cols_n], preferred_element_type=F32).astype(BF16)
    for a, b in stores:
        a.wait()
        b.wait()


def attention_call(layer, first, positions, x, norm, tables, wq, wk, wv, wo, kc, vc, k_out, v_out):
    batch, d = x.shape
    hd = kc.shape[-1]
    n_q, n_kv = wq.shape[-1] // hd, wk.shape[-1] // hd
    chunk = 64
    n_chunks = batch // chunk
    if first:
        ins = [positions] + in_hbm([x]) + [norm, tables[0], tables[1]] + in_hbm([wq, wk, wv, wo, kc, vc])
    else:
        ins = [positions, x, tables[0], tables[1], wq, wk, wv, wo, kc, vc]
    part = pltpu.VMEM((batch, d), BF16)
    if first:
        specs = [SMEM, HBM, VMEM, VMEM, VMEM] + [HBM] * 6
        outs = (part, pltpu.HBM(kc.shape, BF16), pltpu.HBM(vc.shape, BF16))
        out_specs = (VMEM, HBM, HBM)
        aliases = {}
        big = [(batch, d), wq.shape[1:], wk.shape[1:], wv.shape[1:], wo.shape[1:], kc.shape[1:], vc.shape[1:], (batch, d)]
    else:
        specs = [SMEM, VMEM, VMEM, VMEM] + [VMEM] * 6 + [HBM] * 2
        aliases = {len(ins): 1, len(ins) + 1: 2, len(ins) - 2: 3, len(ins) - 1: 4}
        outs = (part, pltpu.HBM(k_out.shape, BF16), pltpu.HBM(v_out.shape, BF16), pltpu.VMEM(kc.shape, BF16), pltpu.VMEM(vc.shape, BF16))
        ins += in_hbm([k_out, v_out])
        out_specs = (VMEM, HBM, HBM, VMEM, VMEM)
        big = []
    scratch = [pltpu.VMEM(shape, BF16) for shape in big] + [
        pltpu.VMEM((batch, hd), F32), pltpu.VMEM((batch, hd), F32), pltpu.VMEM((batch * n_q // hd, hd), jnp.int32),
        pltpu.VMEM((batch * n_q, hd), F32), pltpu.VMEM((batch * n_kv, hd), F32), pltpu.VMEM((batch * n_kv, hd), F32),
        pltpu.VMEM((2, chunk * n_q, hd), F32), pltpu.VMEM((batch * n_q, hd), F32),
        pltpu.SemaphoreType.DMA((5,)), pltpu.SemaphoreType.DMA((2, n_chunks)), pltpu.SemaphoreType.DMA((2, n_chunks)),
    ]
    return pl.pallas_call(
        functools.partial(attention_kernel, layer, first, chunk),
        out_shape=outs,
        in_specs=specs,
        out_specs=out_specs,
        scratch_shapes=scratch,
        input_output_aliases=aliases,
        compiler_params=pltpu.CompilerParams(vmem_limit_bytes=(62 if first else 8) * 2**20),
        name=f"attention{layer}",
    )(*ins)


GROUPS = 2
SUB = 2
NCOL = 4


def mlp_kernel(layer, last, x_ref, part_ref, norm_ref, next_norm_ref, wg_hbm, wu_hbm, wd_hbm, *refs):
    if last:
        carry_in, carry_out = (), ()
        (xo_ref,), refs = refs[:1], refs[1:]
    else:
        carry_in, (ho_ref, xo_ref), carry_out, refs = refs[:6], refs[6:8], refs[8:14], refs[14:]
    (wg, wu, wd, d1, c1, x1, d2, c2, x2, x_own, hbuf, abuf, pbuf, obuf, w_sem, c_sem, s_send, s_recv) = refs
    t = lax.axis_index("tp")
    core = lax.rem(t, 2)
    other = 1 - core
    partner = t + other - core
    across = lax.rem(t + 2, 4)
    d = x_ref.shape[1]
    half = d1.shape[0]
    rows_g = half // GROUPS
    rows_s = rows_g // SUB
    cols_n = d // NCOL

    barrier = pltpu.get_barrier_semaphore()
    for dev in (partner, across):
        pl.semaphore_signal(barrier, inc=1, device_id={"tp": dev}, device_id_type=MESH)
    w_loads = []
    for i, (src, dst) in enumerate(((wg_hbm, wg), (wu_hbm, wu), (wd_hbm, wd))):
        n = dst.shape[0] // 4
        for j in range(4):
            cp = pltpu.make_async_copy(src.at[layer, pl.ds(j * n, n)], dst.at[pl.ds(j * n, n)], w_sem.at[i, j])
            cp.start()
            w_loads.append(cp)
    pl.semaphore_wait(barrier, 2)

    def send(stage, idx, src, dst, dev):
        cp = pltpu.make_async_remote_copy(src_ref=src, dst_ref=dst, send_sem=s_send.at[stage, idx], recv_sem=s_recv.at[stage, idx],
                                          device_id={"tp": dev}, device_id_type=MESH)
        cp.start()
        return cp

    started = []

    def add_norm(mine, theirs, res, res_row, row, x_to, w_ref, w_row, dst, dst_row):
        rows = pl.ds(row, 16)
        to = pl.ds(dst_row, 16)

        def total(j, n):
            t = (mine[rows, j:j + n].astype(F32) + theirs[rows, j:j + n].astype(F32)).astype(BF16).astype(F32)
            return (res[pl.ds(res_row, 16), j:j + n].astype(F32) + t).astype(BF16)

        if w_ref is None:
            for j in range(0, d, 256):
                dst[to, j:j + 256] = total(j, 256)
            return

        def keep(j, n):
            v = total(j, n)
            x_to[rows, j:j + n] = v
            return v.astype(F32)

        first_pass = [True] * (d // 256)

        def read(j, n):
            if first_pass[j // 256]:
                first_pass[j // 256] = False
                return keep(j, n)
            return x_to[rows, j:j + n].astype(F32)

        def write(j, n, v):
            dst[to, j:j + n] = v

        norm_block(read, lambda j, n: w_ref[w_row:w_row + 1, j:j + n].astype(F32), write, d)

    subs = [(g, s, g * rows_g + s * rows_s) for g in range(GROUPS) for s in range(SUB)]
    near = []
    for i, (g, s, r0) in enumerate(subs):
        near.append(send(0, i, part_ref.at[pl.ds(other * half + r0, rows_s)], d1.at[pl.ds(r0, rows_s)], partner))
    far = []
    for i, (g, s, r0) in enumerate(subs):
        near[i].wait_recv()
        rows = pl.ds(r0, rows_s)
        c1[rows, :] = (part_ref[pl.ds(core * half + r0, rows_s), :].astype(F32) + d1[rows, :].astype(F32)).astype(BF16)
        far.append(send(1, i, c1.at[rows], x1.at[rows], across))
    started += near + far

    gathers1 = {}

    def finish1(g):
        for s in range(SUB):
            i = g * SUB + s
            far[i].wait_recv()
            for r in range(rows_s // 16):
                r0 = g * rows_g + s * rows_s + r * 16
                rows = pl.ds(r0, 16)
                add_norm(c1, x1, x_ref, r0 if last else core * half + r0, r0, x_own, norm_ref, layer, hbuf.at[g, core], s * rows_s + r * 16)
            part = hbuf.at[g, core, pl.ds(s * rows_s, rows_s)]
            cp = send(2, i, part, part, partner)
            gathers1[i] = cp
            started.append(cp)

    def wait1(g):
        for s in range(SUB):
            gathers1[g * SUB + s].wait_recv()

    def gate_up(g):
        hid = hbuf.at[g].reshape(2 * rows_g, d)

        def body(n, carry):
            cols = pl.ds(pl.multiple_of(n * 512, 512), 512)
            gate = jnp.dot(hid[...], wg[:, cols], preferred_element_type=F32).astype(BF16).astype(F32)
            up = jnp.dot(hid[...], wu[:, cols], preferred_element_type=F32).astype(BF16).astype(F32)
            abuf[:, cols] = (gate * (1.0 / (1.0 + jnp.exp(-gate))) * up).astype(BF16)
            return carry

        lax.fori_loop(0, wg.shape[1] // 512, body, 0)

    near2, far2 = {}, {}

    def relay2(g, n):
        i = g * NCOL + n
        near2[i].wait_recv()
        cols = pl.ds(n * cols_n, cols_n)
        rows = pl.ds(g * rows_g, rows_g)
        c2[rows, cols] = (pbuf[g, core, :, cols].astype(F32) + d2[rows, cols].astype(F32)).astype(BF16)
        far2[i] = send(4, i, c2.at[rows, cols], x2.at[rows, cols], across)
        started.append(far2[i])

    def down(g, after_first):
        for n in range(NCOL):
            cols = pl.ds(n * cols_n, cols_n)
            y = jnp.dot(abuf[...], wd[:, cols], preferred_element_type=F32).astype(BF16)
            pbuf[g, :, :, cols] = y.reshape(2, rows_g, cols_n)
            i = g * NCOL + n
            near2[i] = send(3, i, pbuf.at[g, other, :, cols], d2.at[pl.ds(g * rows_g, rows_g), cols], partner)
            started.append(near2[i])
            if n == 0 and after_first is not None:
                after_first()
            if n > 0:
                relay2(g, n - 1)
        relay2(g, NCOL - 1)

    gathers2 = {}

    def finish2(g):
        for n in range(NCOL):
            far2[g * NCOL + n].wait_recv()
        for s in range(SUB):
            for r in range(rows_s // 16):
                r0 = g * rows_g + s * rows_s + r * 16
                if last:
                    add_norm(c2, x2, x_own, r0, r0, None, None, 0, obuf.at[g, core], s * rows_s + r * 16)
                else:
                    add_norm(c2, x2, x_own, r0, r0, xo_ref, next_norm_ref, layer + 1, obuf.at[g, core], s * rows_s + r * 16)
            part = obuf.at[g, core, pl.ds(s * rows_s, rows_s)]
            cp = send(5, g * SUB + s, part, part, partner)
            gathers2[g * SUB + s] = cp
            started.append(cp)

    def wait2(g):
        out = xo_ref if last else ho_ref
        for s in range(SUB):
            gathers2[g * SUB + s].wait_recv()
        for c in range(2):
            out[c * half + g * rows_g:c * half + (g + 1) * rows_g, :] = obuf[g, c]

    finish1(0)
    wait1(0)
    for cp in w_loads:
        cp.wait()
    c_loads = []
    for i, (src, dst) in enumerate(zip(carry_in, carry_out)):
        n = dst.shape[0] // 4
        for j in range(4):
            cp = pltpu.make_async_copy(src.at[layer + 1, pl.ds(j * n, n)], dst.at[pl.ds(j * n, n)], c_sem.at[i, j])
            cp.start()
            c_loads.append(cp)
    gate_up(0)
    down(0, lambda: finish1(1))
    wait1(1)
    gate_up(1)
    down(1, None)
    finish2(0)
    wait2(0)
    finish2(1)
    wait2(1)
    for cp in c_loads:
        cp.wait()
    for cp in started:
        cp.wait_send()


def mlp_call(layer, last, x, part, norm, next_norm, wg, wu, wd, carry=()):
    batch, d = part.shape
    half = batch // 2
    rows_g = half // GROUPS
    ff = wg.shape[2]
    n_sem = max(GROUPS * NCOL, GROUPS * SUB)
    own = lambda: pltpu.VMEM((half, d), BF16)
    scratch = [
        pltpu.VMEM(wg.shape[1:], BF16), pltpu.VMEM(wu.shape[1:], BF16), pltpu.VMEM(wd.shape[1:], BF16),
        own(), own(), own(), own(), own(), own(), own(),
        pltpu.VMEM((GROUPS, 2, rows_g, d), BF16), pltpu.VMEM((2 * rows_g, ff), BF16),
        pltpu.VMEM((GROUPS, 2, rows_g, d), BF16), pltpu.VMEM((GROUPS, 2, rows_g, d), BF16),
        pltpu.SemaphoreType.DMA((3, 4)), pltpu.SemaphoreType.DMA((6, 4)), pltpu.SemaphoreType.DMA((6, n_sem)), pltpu.SemaphoreType.DMA((6, n_sem)),
    ]
    full = pltpu.VMEM((batch, d), BF16)
    mine = pltpu.VMEM((half, d), BF16)
    return pl.pallas_call(
        functools.partial(mlp_kernel, layer, last),
        out_shape=full if last else (full, mine) + tuple(pltpu.VMEM(a.shape[1:], BF16) for a in carry),
        in_specs=[VMEM] * 4 + [HBM] * (3 + len(carry)),
        out_specs=VMEM if last else (VMEM,) * (2 + len(carry)),
        scratch_shapes=scratch,
        compiler_params=pltpu.CompilerParams(collective_id=layer, has_side_effects=True, vmem_limit_bytes=(33 if last else 33) * 2**20),
        name=f"mlp{layer}",
    )(x, pltpu.with_memory_space_constraint(part, pltpu.VMEM), norm, next_norm, *in_hbm((wg, wu, wd) + tuple(carry)))


def solution(mesh):
    row_spec = P('dp', None)
    pos_spec = P('dp')
    cache_spec = P(None, 'dp', None, 'tp', None)
    norm_spec = P(None, None)
    col_spec = P(None, None, 'tp')
    split_rows = P(None, 'tp', None)

    def local_step(hidden, positions, k_cache, v_cache, attn_norm, w_query, w_key, w_value, w_out, mlp_norm, w_gate, w_up, w_down):
        shape = k_cache.shape
        flat = shape[:2] + (shape[2] * shape[3], shape[4])
        k_cache, v_cache = k_cache.reshape(flat), v_cache.reshape(flat)
        tables = [jnp.asarray(t) for t in rope_by_position(shape[2], shape[4])]
        part, k_out, v_out = attention_call(0, True, positions, hidden, attn_norm, tables, w_query, w_key, w_value, w_out, k_cache, v_cache, None, None)
        h, x_own, *carried = mlp_call(0, False, hidden, part, mlp_norm, attn_norm, w_gate, w_up, w_down, (w_query, w_key, w_value, w_out, k_cache, v_cache))
        part, k_out, v_out = attention_call(1, False, positions, h, None, tables, *carried, k_out, v_out)[:3]
        hidden = mlp_call(1, True, x_own, part, mlp_norm, attn_norm, w_gate, w_up, w_down)
        return hidden, k_out.reshape(shape), v_out.reshape(shape)

    return jax.shard_map(local_step, mesh=mesh, in_specs=(row_spec, pos_spec, cache_spec, cache_spec, norm_spec, col_spec, col_spec, col_spec, split_rows, norm_spec, col_spec, col_spec, split_rows), out_specs=(row_spec, cache_spec, cache_spec), check_vma=False)
```

```python
import functools
import math

import jax
import jax.numpy as jnp
import numpy as np
from jax import lax
from jax.experimental import pallas as pl
from jax.experimental.pallas import tpu as pltpu
from jax.sharding import PartitionSpec as P

MESH = pl.DeviceIdType.MESH
BF16 = jnp.bfloat16
F32 = jnp.float32
ANY = pl.BlockSpec(memory_space=pl.ANY)
HBM = pl.BlockSpec(memory_space=pltpu.HBM)
VMEM = pl.BlockSpec(memory_space=pltpu.VMEM)
SMEM = pl.BlockSpec(memory_space=pltpu.SMEM)


def rope_by_position(seq_len, head_dim):
    half = head_dim // 2
    inv_freq = np.power(np.float32(500000.0), -np.arange(half, dtype=np.float32) * np.float32(2.0 / head_dim)).astype(np.float32)
    wavelen = np.float32(2.0 * math.pi) / inv_freq
    smooth = (np.float32(8192.0) / wavelen - np.float32(1.0)) / np.float32(3.0)
    blended = (np.float32(1.0) - smooth) * inv_freq / np.float32(8.0) + smooth * inv_freq
    scaled = np.where(wavelen < 2048.0, inv_freq, np.where(wavelen > 8192.0, inv_freq / np.float32(8.0), blended)).astype(np.float32)
    angles = np.arange(seq_len, dtype=np.float32)[:, None] * scaled[None, :]
    cos = np.cos(angles.astype(np.float64)).astype(np.float32)
    sin = np.sin(angles.astype(np.float64)).astype(np.float32)
    return np.concatenate([cos, cos], axis=1), np.concatenate([-sin, sin], axis=1)


def norm_block(read, weight, write, width):
    step = 256
    acc = None
    for j in range(width // step):
        v = read(j * step, step)
        sq = v * v
        acc = sq if acc is None else acc + sq
    scale = lax.rsqrt(jnp.sum(acc, axis=-1, keepdims=True) * (1.0 / width) + 1e-5)
    for j in range(width // step):
        write(j * step, step, (read(j * step, step) * scale * weight(j * step, step)).astype(BF16))


def in_hbm(arrays):
    return [pltpu.with_memory_space_constraint(a, pltpu.HBM) for a in arrays]


def attention_kernel(layer, first, chunk, *refs):
    refs = list(refs)
    pos_ref = refs.pop(0)
    x_in = refs.pop(0)
    norm_in = refs.pop(0) if first else None
    cos_tab, sin_tab, wq_hbm, wk_hbm, wv_hbm, wo_hbm, kc_hbm, vc_hbm = refs[:8]
    refs = refs[8:]
    if first:
        part_ref, ko_hbm, vo_hbm = refs[:3]
        x_ref, wq, wk, wv, wo, kbuf, vbuf, h_scr, norm_ref, cos_ref, sin_ref, pos_smem, small_sem = refs[3:16]
        refs = refs[16:]
        small = []
        for i, (src, dst) in enumerate(((pos_ref, pos_smem), (cos_tab, cos_ref), (sin_tab, sin_ref), (norm_in, norm_ref))):
            small.append(pltpu.make_async_copy(src, dst, small_sem.at[i]))
            small[i].start()
        pos_ref, cos_tab, sin_tab = pos_smem, cos_ref, sin_ref
    else:
        x_ref, wq, wk, wv, wo = x_in, wq_hbm, wk_hbm, wv_hbm, wo_hbm
        part_ref, ko_hbm, vo_hbm, kbuf, vbuf = refs[2:7]
        refs = refs[7:]
    (cos_scr, sin_scr, lim_scr, q_scr, k_scr, v_scr, p_scr, o_scr, w_sem, in_sem, out_sem) = refs
    batch = x_ref.shape[0]
    n_q = wq.shape[1] // 128
    n_kv = wk.shape[1] // 128
    group = n_q // n_kv
    rows_kv = kbuf.shape[1]
    n_chunks = batch // chunk

    if first:
        x_load = pltpu.make_async_copy(x_in, x_ref, w_sem.at[4])
        x_load.start()
        loads = []
        for i, (src, dst) in enumerate(((wq_hbm, wq), (wk_hbm, wk), (wv_hbm, wv))):
            loads.append(pltpu.make_async_copy(src.at[layer], dst, w_sem.at[i]))
        for c in loads:
            c.start()
        kv_loads = []
        for c in range(n_chunks):
            rows = pl.ds(c * chunk, chunk)
            a = pltpu.make_async_copy(kc_hbm.at[layer, rows], kbuf.at[rows], in_sem.at[0, c])
            b = pltpu.make_async_copy(vc_hbm.at[layer, rows], vbuf.at[rows], in_sem.at[1, c])
            a.start()
            b.start()
            kv_loads.append((a, b))
        wo_load = pltpu.make_async_copy(wo_hbm.at[layer], wo, w_sem.at[3])
        wo_load.start()

    if first:
        for cp in small:
            cp.wait()

    per_row = 128 // n_q
    lane_request = lax.broadcasted_iota(jnp.int32, (1, 128), 1) // n_q

    def table_body(i, carry):
        limit = jnp.zeros((1, 128), jnp.int32)
        for u in range(per_row):
            b = i * per_row + u
            pos = pos_ref[b]
            cos_scr[pl.ds(b, 1), :] = cos_tab[pl.ds(pos, 1), :]
            sin_scr[pl.ds(b, 1), :] = sin_tab[pl.ds(pos, 1), :]
            limit = jnp.where(lane_request == u, pos * n_kv + n_kv - 1, limit)
        lim_scr[pl.ds(i, 1), :] = limit
        return carry

    lax.fori_loop(0, batch // per_row, table_body, 0)

    if first:
        x_load.wait()
        def norm_body(i, carry):
            rows = pl.ds(pl.multiple_of(i * 16, 16), 16)

            def write(j, n, v):
                h_scr[rows, j:j + n] = v

            norm_block(lambda j, n: x_ref[rows, j:j + n].astype(F32), lambda j, n: norm_ref[layer:layer + 1, j:j + n].astype(F32), write, h_scr.shape[1])
            return carry

        lax.fori_loop(0, batch // 16, norm_body, 0)
        h_src = h_scr
    else:
        h_src = x_ref

    def rope(v):
        v = v.astype(BF16).astype(F32)
        return v * cos_scr[...] + pltpu.roll(v, 64, 1) * sin_scr[...]

    h = h_src[...]
    if first:
        loads[0].wait()
    q = jnp.dot(h, wq[...], preferred_element_type=F32)
    for j in range(n_q):
        q_scr[pl.ds(j, batch, n_q), :] = rope(q[:, j * 128:(j + 1) * 128])
    if first:
        loads[1].wait()
    k = jnp.dot(h, wk[...], preferred_element_type=F32)
    for j in range(n_kv):
        k_scr[pl.ds(j, batch, n_kv), :] = rope(k[:, j * 128:(j + 1) * 128])
    if first:
        loads[2].wait()
    v = jnp.dot(h, wv[...], preferred_element_type=F32)
    for j in range(n_kv):
        v_scr[pl.ds(j, batch, n_kv), :] = v[:, j * 128:(j + 1) * 128]

    kmat = kbuf.reshape(batch * rows_kv, 128)
    vmat = vbuf.reshape(batch * rows_kv, 128)
    scale = 128 ** -0.5
    pair = 2 * n_q
    row_id = lax.broadcasted_iota(jnp.int32, (2 * pair, 128), 0)
    first_pair = row_id < pair
    first_in_pair = (row_id % pair) < n_q
    zero = jnp.zeros((2 * pair, 128), F32)
    quads = chunk // 4
    cols = chunk * n_q
    lane = lax.broadcasted_iota(jnp.int32, (rows_kv, cols), 1)
    row = lax.broadcasted_iota(jnp.int32, (rows_kv, cols), 0)
    same_head = (row % n_kv) == (lane % n_q) // group
    first_of_two = (lane // n_q) % 2 == 0
    lane_pair = lax.broadcasted_iota(jnp.int32, (128, 128), 1) // pair
    no_tile = jnp.zeros((128, 128), BF16)
    pairs_per_tile = 128 // pair
    per_tile = 16 // n_kv
    shift = per_tile.bit_length() - 1
    tile_row = lax.broadcasted_iota(jnp.int32, (16, 128), 0) // n_kv
    tile_head = lax.broadcasted_iota(jnp.int32, (8, 128), 0) % n_kv

    def square(mat, base):
        top = mat[pl.ds(base, 2 * rows_kv), :]
        bottom = mat[pl.ds(base + 2 * rows_kv, 2 * rows_kv), :]
        return jnp.concatenate([top, bottom], axis=1)

    stores = []
    for c in range(n_chunks):
        rows = pl.ds(c * chunk, chunk)
        stores.append((pltpu.make_async_copy(kbuf.at[rows], ko_hbm.at[layer, rows], out_sem.at[0, c]),
                       pltpu.make_async_copy(vbuf.at[rows], vo_hbm.at[layer, rows], out_sem.at[1, c])))

    def values(c):
        for t in range(quads):
            b = c * chunk + t * 4
            p4 = p_scr[c % 2, pl.ds(t * 2 * pair, 2 * pair), :]
            wide = jnp.concatenate([jnp.where(first_in_pair, p4, zero), jnp.where(first_in_pair, zero, p4)], axis=1).astype(BF16)
            o = jnp.dot(wide, square(vmat, b * rows_kv), preferred_element_type=F32)
            o_scr[pl.ds(b * n_q, 2 * pair), :] = jnp.where(first_pair, o[:, :128], o[:, 128:])

    for c in range(n_chunks):
        if first:
            kv_loads[c][0].wait()
            kv_loads[c][1].wait()

        for i in range(c * chunk, (c + 1) * chunk, 8):
            writes = []
            for b in range(i, i + 8):
                pos = pos_ref[b]
                block = pl.ds(pl.multiple_of(lax.shift_left(lax.shift_right_logical(pos, shift), 4), 16), 16)
                here = tile_row == lax.bitwise_and(pos, per_tile - 1)
                for buf, new in ((kbuf, k_scr), (vbuf, v_scr)):
                    fresh = jnp.broadcast_to(new[b * n_kv:b * n_kv + 1, :], (8, 128))
                    for j in range(1, n_kv):
                        fresh = jnp.where(tile_head == j, new[b * n_kv + j:b * n_kv + j + 1, :], fresh)
                    value = jnp.where(here, jnp.concatenate([fresh, fresh], axis=0), buf[b, block, :].astype(F32))
                    writes.append((buf, b, block, value.astype(BF16)))
            for buf, b, block, value in writes:
                buf[b, block, :] = value

        q_t = q_scr[pl.ds(c * cols, cols), :].T
        acc = None
        for t in range(quads):
            halves = []
            for i in range(2):
                p = 2 * t + i
                tile = p // pairs_per_tile
                tiles = [no_tile] * (cols // 128)
                tiles[tile] = jnp.where(lane_pair == p % pairs_per_tile, q_t[:, tile * 128:(tile + 1) * 128], 0.0).astype(BF16)
                halves.append(jnp.concatenate(tiles, axis=1))
            d = jnp.dot(square(kmat, (c * chunk + t * 4) * rows_kv), jnp.concatenate(halves, axis=0), preferred_element_type=F32)
            acc = d if acc is None else acc + d
        if c > 0:
            values(c - 1)
        stores[c][0].start()
        stores[c][1].start()
        s = jnp.where(first_of_two, acc[:rows_kv], acc[rows_kv:])
        limit = jnp.concatenate([lim_scr[pl.ds(c * (cols // 128) + j, 1), :] for j in range(cols // 128)], axis=1)
        s = jnp.where(same_head & (row <= limit), s * scale, -jnp.inf)
        e = jnp.exp(s - jnp.max(s, axis=0, keepdims=True))
        p_scr[c % 2] = (e * (1.0 / jnp.sum(e, axis=0, keepdims=True))).T
    values(n_chunks - 1)

    att = jnp.concatenate([o_scr[pl.ds(j, batch, n_q), :].astype(BF16) for j in range(n_q)], axis=1)
    if first:
        wo_load.wait()
    for n in range(wo.shape[1] // 512):
        cols_n = pl.ds(n * 512, 512)
        part_ref[:, cols_n] = jnp.dot(att, wo[:, cols_n], preferred_element_type=F32).astype(BF16)
    for a, b in stores:
        a.wait()
        b.wait()


def attention_call(layer, first, positions, x, norm, tables, wq, wk, wv, wo, kc, vc, k_out, v_out):
    batch, d = x.shape
    hd = kc.shape[-1]
    n_q, n_kv = wq.shape[-1] // hd, wk.shape[-1] // hd
    chunk = 64
    n_chunks = batch // chunk
    if first:
        ins = in_hbm([positions, x, norm, tables[0], tables[1], wq, wk, wv, wo, kc, vc])
    else:
        ins = [positions, x, tables[0], tables[1], wq, wk, wv, wo, kc, vc]
    part = pltpu.VMEM((batch, d), BF16)
    if first:
        specs = [HBM] * 11
        outs = (part, pltpu.HBM(kc.shape, BF16), pltpu.HBM(vc.shape, BF16))
        out_specs = (VMEM, HBM, HBM)
        aliases = {}
        big = [(batch, d), wq.shape[1:], wk.shape[1:], wv.shape[1:], wo.shape[1:], kc.shape[1:], vc.shape[1:], (batch, d)]
    else:
        specs = [SMEM, VMEM, VMEM, VMEM] + [VMEM] * 6 + [HBM] * 2
        aliases = {len(ins): 1, len(ins) + 1: 2, len(ins) - 2: 3, len(ins) - 1: 4}
        outs = (part, pltpu.HBM(k_out.shape, BF16), pltpu.HBM(v_out.shape, BF16), pltpu.VMEM(kc.shape, BF16), pltpu.VMEM(vc.shape, BF16))
        ins += in_hbm([k_out, v_out])
        out_specs = (VMEM, HBM, HBM, VMEM, VMEM)
        big = []
    scratch = [pltpu.VMEM(shape, BF16) for shape in big]
    if first:
        scratch += [pltpu.VMEM(norm.shape, BF16), pltpu.VMEM(tables[0].shape, F32), pltpu.VMEM(tables[1].shape, F32),
                    pltpu.SMEM((batch,), jnp.int32), pltpu.SemaphoreType.DMA((4,))]
    scratch += [
        pltpu.VMEM((batch, hd), F32), pltpu.VMEM((batch, hd), F32), pltpu.VMEM((batch * n_q // hd, hd), jnp.int32),
        pltpu.VMEM((batch * n_q, hd), F32), pltpu.VMEM((batch * n_kv, hd), F32), pltpu.VMEM((batch * n_kv, hd), F32),
        pltpu.VMEM((2, chunk * n_q, hd), F32), pltpu.VMEM((batch * n_q, hd), F32),
        pltpu.SemaphoreType.DMA((5,)), pltpu.SemaphoreType.DMA((2, n_chunks)), pltpu.SemaphoreType.DMA((2, n_chunks)),
    ]
    return pl.pallas_call(
        functools.partial(attention_kernel, layer, first, chunk),
        out_shape=outs,
        in_specs=specs,
        out_specs=out_specs,
        scratch_shapes=scratch,
        input_output_aliases=aliases,
        compiler_params=pltpu.CompilerParams(vmem_limit_bytes=(62 if first else 8) * 2**20),
        name=f"attention{layer}",
    )(*ins)


GROUPS = 2
SUB = 2
NCOL = 4


def mlp_kernel(layer, last, x_in, part_ref, norm_in, next_norm_in, wg_hbm, wu_hbm, wd_hbm, *refs):
    if last:
        carry_in, carry_out = (), ()
        (xo_ref,), refs = refs[:1], refs[1:]
    else:
        carry_in, (ho_ref, xo_ref), carry_out, refs = refs[:6], refs[6:8], refs[8:14], refs[14:]
    (wg, wu, wd, d1, c1, x1, d2, c2, x2, x_own, hbuf, abuf, pbuf, norm_ref, next_norm_ref, n_sem, w_sem, c_sem, s_send, s_recv) = refs
    t = lax.axis_index("tp")
    core = lax.rem(t, 2)
    other = 1 - core
    partner = t + other - core
    across = lax.rem(t + 2, 4)
    out = xo_ref if last else ho_ref
    d = part_ref.shape[1]
    half = d1.shape[0]
    rows_g = half // GROUPS
    rows_s = rows_g // SUB
    cols_n = d // NCOL

    barrier = pltpu.get_barrier_semaphore()
    for dev in (partner, across):
        pl.semaphore_signal(barrier, inc=1, device_id={"tp": dev}, device_id_type=MESH)
    small = [pltpu.make_async_copy(norm_in, norm_ref, n_sem.at[0]), pltpu.make_async_copy(next_norm_in, next_norm_ref, n_sem.at[1])]
    if not last:
        small.append(pltpu.make_async_copy(x_in.at[pl.ds(pl.multiple_of(core * half, half), half)], x_own, n_sem.at[2]))
    for cp in small:
        cp.start()
    w_loads = []
    for i, (src, dst) in enumerate(((wg_hbm, wg), (wu_hbm, wu), (wd_hbm, wd))):
        n = dst.shape[0] // 4
        for j in range(4):
            cp = pltpu.make_async_copy(src.at[layer, pl.ds(j * n, n)], dst.at[pl.ds(j * n, n)], w_sem.at[i, j])
            cp.start()
            w_loads.append(cp)
    pl.semaphore_wait(barrier, 2)

    def send(stage, idx, src, dst, dev):
        cp = pltpu.make_async_remote_copy(src_ref=src, dst_ref=dst, send_sem=s_send.at[stage, idx], recv_sem=s_recv.at[stage, idx],
                                          device_id={"tp": dev}, device_id_type=MESH)
        cp.start()
        return cp

    started = []

    def add_norm(mine, theirs, res, res_row, row, x_to, w_ref, w_row, dst, dst_row):
        rows = pl.ds(row, 16)
        to = pl.ds(dst_row, 16)

        def total(j, n):
            t = (mine[rows, j:j + n].astype(F32) + theirs[rows, j:j + n].astype(F32)).astype(BF16).astype(F32)
            return (res[pl.ds(res_row, 16), j:j + n].astype(F32) + t).astype(BF16)

        if w_ref is None:
            for j in range(0, d, 256):
                dst[to, j:j + 256] = total(j, 256)
            return

        def keep(j, n):
            v = total(j, n)
            x_to[rows, j:j + n] = v
            return v.astype(F32)

        first_pass = [True] * (d // 256)

        def read(j, n):
            if first_pass[j // 256]:
                first_pass[j // 256] = False
                return keep(j, n)
            return x_to[rows, j:j + n].astype(F32)

        def write(j, n, v):
            dst[to, j:j + n] = v

        norm_block(read, lambda j, n: w_ref[w_row:w_row + 1, j:j + n].astype(F32), write, d)

    subs = [(g, s, g * rows_g + s * rows_s) for g in range(GROUPS) for s in range(SUB)]
    near = []
    for i, (g, s, r0) in enumerate(subs):
        near.append(send(0, i, part_ref.at[pl.ds(other * half + r0, rows_s)], d1.at[pl.ds(r0, rows_s)], partner))
    far = []
    for i, (g, s, r0) in enumerate(subs):
        near[i].wait_recv()
        rows = pl.ds(r0, rows_s)
        c1[rows, :] = (part_ref[pl.ds(core * half + r0, rows_s), :].astype(F32) + d1[rows, :].astype(F32)).astype(BF16)
        far.append(send(1, i, c1.at[rows], x1.at[rows], across))
    started += near + far

    gathers1 = {}

    def finish1(g):
        for s in range(SUB):
            i = g * SUB + s
            far[i].wait_recv()
            for r in range(rows_s // 16):
                r0 = g * rows_g + s * rows_s + r * 16
                rows = pl.ds(r0, 16)
                add_norm(c1, x1, x_in if last else x_own, r0, r0, x_own, norm_ref, layer, hbuf.at[g, core], s * rows_s + r * 16)
            part = hbuf.at[g, core, pl.ds(s * rows_s, rows_s)]
            cp = send(2, i, part, part, partner)
            gathers1[i] = cp
            started.append(cp)

    def wait1(g):
        for s in range(SUB):
            gathers1[g * SUB + s].wait_recv()

    def gate_up(g):
        hid = hbuf.at[g].reshape(2 * rows_g, d)

        def body(n, carry):
            cols = pl.ds(n * 512, 512)
            gate = jnp.dot(hid[...], wg[:, cols], preferred_element_type=F32).astype(BF16).astype(F32)
            up = jnp.dot(hid[...], wu[:, cols], preferred_element_type=F32).astype(BF16).astype(F32)
            abuf[:, cols] = (gate * (1.0 / (1.0 + jnp.exp(-gate))) * up).astype(BF16)
            return carry

        for n in range(wg.shape[1] // 512):
            body(n, 0)

    near2, far2 = {}, {}

    def relay2(g, n):
        i = g * NCOL + n
        near2[i].wait_recv()
        cols = pl.ds(n * cols_n, cols_n)
        rows = pl.ds(g * rows_g, rows_g)
        c2[rows, cols] = (pbuf[g, core, :, cols].astype(F32) + d2[rows, cols].astype(F32)).astype(BF16)
        far2[i] = send(4, i, c2.at[rows, cols], x2.at[rows, cols], across)
        started.append(far2[i])

    def down(g, after_first):
        for n in range(NCOL):
            cols = pl.ds(n * cols_n, cols_n)
            y = jnp.dot(abuf[...], wd[:, cols], preferred_element_type=F32).astype(BF16)
            pbuf[g, :, :, cols] = y.reshape(2, rows_g, cols_n)
            i = g * NCOL + n
            near2[i] = send(3, i, pbuf.at[g, other, :, cols], d2.at[pl.ds(g * rows_g, rows_g), cols], partner)
            started.append(near2[i])
            if n == 0 and after_first is not None:
                after_first()
            if n > 0:
                relay2(g, n - 1)
        relay2(g, NCOL - 1)

    gathers2 = {}

    def finish2(g):
        for n in range(NCOL):
            far2[g * NCOL + n].wait_recv()
        for s in range(SUB):
            for r in range(rows_s // 16):
                r0 = g * rows_g + s * rows_s + r * 16
                to = pl.multiple_of(core * half + r0, 16)
                if last:
                    add_norm(c2, x2, x_own, r0, r0, None, None, 0, out, to)
                else:
                    add_norm(c2, x2, x_own, r0, r0, xo_ref, next_norm_ref, layer + 1, out, to)
            part = out.at[pl.ds(pl.multiple_of(core * half + g * rows_g + s * rows_s, rows_s), rows_s)]
            cp = send(5, g * SUB + s, part, part, partner)
            gathers2[g * SUB + s] = cp
            started.append(cp)

    def wait2(g):
        for s in range(SUB):
            gathers2[g * SUB + s].wait_recv()

    for cp in small:
        cp.wait()
    finish1(0)
    wait1(0)
    for cp in w_loads:
        cp.wait()
    c_loads = []
    for i, (src, dst) in enumerate(zip(carry_in, carry_out)):
        n = dst.shape[0] // 4
        for j in range(4):
            cp = pltpu.make_async_copy(src.at[layer + 1, pl.ds(j * n, n)], dst.at[pl.ds(j * n, n)], c_sem.at[i, j])
            cp.start()
            c_loads.append(cp)
    gate_up(0)
    down(0, lambda: finish1(1))
    wait1(1)
    gate_up(1)
    down(1, None)
    finish2(0)
    wait2(0)
    finish2(1)
    wait2(1)
    for cp in c_loads:
        cp.wait()
    for cp in started:
        cp.wait_send()


def mlp_call(layer, last, x, part, norm, next_norm, wg, wu, wd, carry=()):
    batch, d = part.shape
    half = batch // 2
    rows_g = half // GROUPS
    ff = wg.shape[2]
    n_sem = max(GROUPS * NCOL, GROUPS * SUB)
    own = lambda: pltpu.VMEM((half, d), BF16)
    scratch = [
        pltpu.VMEM(wg.shape[1:], BF16), pltpu.VMEM(wu.shape[1:], BF16), pltpu.VMEM(wd.shape[1:], BF16),
        own(), own(), own(), own(), own(), own(), own(),
        pltpu.VMEM((GROUPS, 2, rows_g, d), BF16), pltpu.VMEM((2 * rows_g, ff), BF16),
        pltpu.VMEM((GROUPS, 2, rows_g, d), BF16), pltpu.VMEM(norm.shape, BF16), pltpu.VMEM(norm.shape, BF16),
        pltpu.SemaphoreType.DMA((3,)), pltpu.SemaphoreType.DMA((3, 4)), pltpu.SemaphoreType.DMA((6, 4)), pltpu.SemaphoreType.DMA((6, n_sem)), pltpu.SemaphoreType.DMA((6, n_sem)),
    ]
    full = pltpu.VMEM((batch, d), BF16)
    mine = pltpu.VMEM((half, d), BF16)
    return pl.pallas_call(
        functools.partial(mlp_kernel, layer, last),
        out_shape=full if last else (full, mine) + tuple(pltpu.VMEM(a.shape[1:], BF16) for a in carry),
        in_specs=[VMEM if last else HBM, VMEM] + [HBM] * (5 + len(carry)),
        out_specs=VMEM if last else (VMEM,) * (2 + len(carry)),
        scratch_shapes=scratch,
        compiler_params=pltpu.CompilerParams(collective_id=layer, has_side_effects=True, vmem_limit_bytes=(33 if last else 33) * 2**20),
        name=f"mlp{layer}",
    )(pltpu.with_memory_space_constraint(x, pltpu.VMEM if last else pltpu.HBM), pltpu.with_memory_space_constraint(part, pltpu.VMEM),
      *in_hbm((norm, next_norm, wg, wu, wd) + tuple(carry)))


def solution(mesh):
    row_spec = P('dp', None)
    pos_spec = P('dp')
    cache_spec = P(None, 'dp', None, 'tp', None)
    norm_spec = P(None, None)
    col_spec = P(None, None, 'tp')
    split_rows = P(None, 'tp', None)

    def local_step(hidden, positions, k_cache, v_cache, attn_norm, w_query, w_key, w_value, w_out, mlp_norm, w_gate, w_up, w_down):
        shape = k_cache.shape
        flat = shape[:2] + (shape[2] * shape[3], shape[4])
        k_cache, v_cache = k_cache.reshape(flat), v_cache.reshape(flat)
        tables = [jnp.asarray(t) for t in rope_by_position(shape[2], shape[4])]
        part, k_out, v_out = attention_call(0, True, positions, hidden, attn_norm, tables, w_query, w_key, w_value, w_out, k_cache, v_cache, None, None)
        h, x_own, *carried = mlp_call(0, False, hidden, part, mlp_norm, attn_norm, w_gate, w_up, w_down, (w_query, w_key, w_value, w_out, k_cache, v_cache))
        part, k_out, v_out = attention_call(1, False, positions, h, None, tables, *carried, k_out, v_out)[:3]
        hidden = mlp_call(1, True, x_own, part, mlp_norm, attn_norm, w_gate, w_up, w_down)
        return hidden, k_out.reshape(shape), v_out.reshape(shape)

    return jax.shard_map(local_step, mesh=mesh, in_specs=(row_spec, pos_spec, cache_spec, cache_spec, norm_spec, col_spec, col_spec, col_spec, split_rows, norm_spec, col_spec, col_spec, split_rows), out_specs=(row_spec, cache_spec, cache_spec), check_vma=False)
```

```python
import functools
import math

import jax
import jax.numpy as jnp
import numpy as np
from jax import lax
from jax.experimental import pallas as pl
from jax.experimental.pallas import tpu as pltpu
from jax.sharding import PartitionSpec as P

MESH = pl.DeviceIdType.MESH
BF16 = jnp.bfloat16
F32 = jnp.float32
ANY = pl.BlockSpec(memory_space=pl.ANY)
HBM = pl.BlockSpec(memory_space=pltpu.HBM)
VMEM = pl.BlockSpec(memory_space=pltpu.VMEM)
SMEM = pl.BlockSpec(memory_space=pltpu.SMEM)


def rope_by_position(seq_len, head_dim):
    half = head_dim // 2
    inv_freq = np.power(np.float32(500000.0), -np.arange(half, dtype=np.float32) * np.float32(2.0 / head_dim)).astype(np.float32)
    wavelen = np.float32(2.0 * math.pi) / inv_freq
    smooth = (np.float32(8192.0) / wavelen - np.float32(1.0)) / np.float32(3.0)
    blended = (np.float32(1.0) - smooth) * inv_freq / np.float32(8.0) + smooth * inv_freq
    scaled = np.where(wavelen < 2048.0, inv_freq, np.where(wavelen > 8192.0, inv_freq / np.float32(8.0), blended)).astype(np.float32)
    angles = np.arange(seq_len, dtype=np.float32)[:, None] * scaled[None, :]
    cos = np.cos(angles.astype(np.float64)).astype(np.float32)
    sin = np.sin(angles.astype(np.float64)).astype(np.float32)
    return np.concatenate([cos, cos], axis=1), np.concatenate([-sin, sin], axis=1)


def norm_block(read, weight, write, width):
    step = 256
    acc = None
    for j in range(width // step):
        v = read(j * step, step)
        sq = v * v
        acc = sq if acc is None else acc + sq
    scale = lax.rsqrt(jnp.sum(acc, axis=-1, keepdims=True) * (1.0 / width) + 1e-5)
    for j in range(width // step):
        write(j * step, step, (read(j * step, step) * scale * weight(j * step, step)).astype(BF16))


def in_hbm(arrays):
    return [pltpu.with_memory_space_constraint(a, pltpu.HBM) for a in arrays]


def attention_kernel(layer, first, chunk, *refs):
    refs = list(refs)
    pos_ref = refs.pop(0)
    x_in = refs.pop(0)
    norm_ref = refs.pop(0) if first else None
    cos_tab, sin_tab, wq_hbm, wk_hbm, wv_hbm, wo_hbm, kc_hbm, vc_hbm = refs[:8]
    refs = refs[8:]
    if first:
        part_ref, ko_hbm, vo_hbm = refs[:3]
        x_ref, wq, wk, wv, wo, kbuf, vbuf, h_scr = refs[3:11]
        refs = refs[11:]
    else:
        x_ref, wq, wk, wv, wo = x_in, wq_hbm, wk_hbm, wv_hbm, wo_hbm
        part_ref, ko_hbm, vo_hbm, kbuf, vbuf = refs[2:7]
        refs = refs[7:]
    (cos_scr, sin_scr, lim_scr, q_scr, k_scr, v_scr, p_scr, o_scr, w_sem, in_sem, out_sem) = refs
    batch = x_ref.shape[0]
    n_q = wq.shape[1] // 128
    n_kv = wk.shape[1] // 128
    group = n_q // n_kv
    rows_kv = kbuf.shape[1]
    n_chunks = batch // chunk

    if first:
        x_load = pltpu.make_async_copy(x_in, x_ref, w_sem.at[4])
        x_load.start()
        loads = []
        for i, (src, dst) in enumerate(((wq_hbm, wq), (wk_hbm, wk), (wv_hbm, wv))):
            loads.append(pltpu.make_async_copy(src.at[layer], dst, w_sem.at[i]))
        for c in loads:
            c.start()
        kv_loads = []
        for c in range(n_chunks):
            rows = pl.ds(c * chunk, chunk)
            a = pltpu.make_async_copy(kc_hbm.at[layer, rows], kbuf.at[rows], in_sem.at[0, c])
            b = pltpu.make_async_copy(vc_hbm.at[layer, rows], vbuf.at[rows], in_sem.at[1, c])
            kv_loads.append((a, b))
        wo_load = pltpu.make_async_copy(wo_hbm.at[layer], wo, w_sem.at[3])
        kv_loads[0][0].start()
        kv_loads[0][1].start()

    per_row = 128 // n_q
    lane_request = lax.broadcasted_iota(jnp.int32, (1, 128), 1) // n_q

    def table_body(i, carry):
        limit = jnp.zeros((1, 128), jnp.int32)
        for u in range(per_row):
            b = i * per_row + u
            pos = pos_ref[b]
            cos_scr[pl.ds(b, 1), :] = cos_tab[pl.ds(pos, 1), :]
            sin_scr[pl.ds(b, 1), :] = sin_tab[pl.ds(pos, 1), :]
            limit = jnp.where(lane_request == u, pos * n_kv + n_kv - 1, limit)
        lim_scr[pl.ds(i, 1), :] = limit
        return carry

    lax.fori_loop(0, batch // per_row, table_body, 0)

    if first:
        x_load.wait()
        def norm_body(i, carry):
            rows = pl.ds(pl.multiple_of(i * 16, 16), 16)

            def write(j, n, v):
                h_scr[rows, j:j + n] = v

            norm_block(lambda j, n: x_ref[rows, j:j + n].astype(F32), lambda j, n: norm_ref[layer:layer + 1, j:j + n].astype(F32), write, h_scr.shape[1])
            return carry

        lax.fori_loop(0, batch // 16, norm_body, 0)
        h_src = h_scr
    else:
        h_src = x_ref

    def rope(v):
        v = v.astype(BF16).astype(F32)
        return v * cos_scr[...] + pltpu.roll(v, 64, 1) * sin_scr[...]

    h = h_src[...]
    if first:
        loads[0].wait()
        kv_loads[1][0].start()
        kv_loads[1][1].start()
    q = jnp.dot(h, wq[...], preferred_element_type=F32)
    for j in range(n_q):
        q_scr[pl.ds(j, batch, n_q), :] = rope(q[:, j * 128:(j + 1) * 128])
    if first:
        loads[1].wait()
        kv_loads[2][0].start()
        kv_loads[2][1].start()
    k = jnp.dot(h, wk[...], preferred_element_type=F32)
    for j in range(n_kv):
        k_scr[pl.ds(j, batch, n_kv), :] = rope(k[:, j * 128:(j + 1) * 128])
    if first:
        loads[2].wait()
        kv_loads[3][0].start()
        kv_loads[3][1].start()
        wo_load.start()
    v = jnp.dot(h, wv[...], preferred_element_type=F32)
    for j in range(n_kv):
        v_scr[pl.ds(j, batch, n_kv), :] = v[:, j * 128:(j + 1) * 128]

    kmat = kbuf.reshape(batch * rows_kv, 128)
    vmat = vbuf.reshape(batch * rows_kv, 128)
    scale = 128 ** -0.5
    pair = 2 * n_q
    row_id = lax.broadcasted_iota(jnp.int32, (2 * pair, 128), 0)
    first_pair = row_id < pair
    first_in_pair = (row_id % pair) < n_q
    zero = jnp.zeros((2 * pair, 128), F32)
    quads = chunk // 4
    cols = chunk * n_q
    lane = lax.broadcasted_iota(jnp.int32, (rows_kv, cols), 1)
    row = lax.broadcasted_iota(jnp.int32, (rows_kv, cols), 0)
    same_head = (row % n_kv) == (lane % n_q) // group
    first_of_two = (lane // n_q) % 2 == 0
    lane_pair = lax.broadcasted_iota(jnp.int32, (128, 128), 1) // pair
    no_tile = jnp.zeros((128, 128), BF16)
    pairs_per_tile = 128 // pair
    per_tile = 16 // n_kv
    shift = per_tile.bit_length() - 1
    tile_row = lax.broadcasted_iota(jnp.int32, (16, 128), 0) // n_kv
    tile_head = lax.broadcasted_iota(jnp.int32, (8, 128), 0) % n_kv

    def square(mat, base):
        top = mat[pl.ds(base, 2 * rows_kv), :]
        bottom = mat[pl.ds(base + 2 * rows_kv, 2 * rows_kv), :]
        return jnp.concatenate([top, bottom], axis=1)

    stores = []
    for c in range(n_chunks):
        rows = pl.ds(c * chunk, chunk)
        stores.append((pltpu.make_async_copy(kbuf.at[rows], ko_hbm.at[layer, rows], out_sem.at[0, c]),
                       pltpu.make_async_copy(vbuf.at[rows], vo_hbm.at[layer, rows], out_sem.at[1, c])))

    def values(c):
        for t in range(quads):
            b = c * chunk + t * 4
            p4 = p_scr[c % 2, pl.ds(t * 2 * pair, 2 * pair), :]
            wide = jnp.concatenate([jnp.where(first_in_pair, p4, zero), jnp.where(first_in_pair, zero, p4)], axis=1).astype(BF16)
            o = jnp.dot(wide, square(vmat, b * rows_kv), preferred_element_type=F32)
            o_scr[pl.ds(b * n_q, 2 * pair), :] = jnp.where(first_pair, o[:, :128], o[:, 128:])

    for c in range(n_chunks):
        if first:
            kv_loads[c][0].wait()
            kv_loads[c][1].wait()

        for i in range(c * chunk, (c + 1) * chunk, 8):
            writes = []
            for b in range(i, i + 8):
                pos = pos_ref[b]
                block = pl.ds(pl.multiple_of(lax.shift_left(lax.shift_right_logical(pos, shift), 4), 16), 16)
                here = tile_row == lax.bitwise_and(pos, per_tile - 1)
                for buf, new in ((kbuf, k_scr), (vbuf, v_scr)):
                    fresh = jnp.broadcast_to(new[b * n_kv:b * n_kv + 1, :], (8, 128))
                    for j in range(1, n_kv):
                        fresh = jnp.where(tile_head == j, new[b * n_kv + j:b * n_kv + j + 1, :], fresh)
                    value = jnp.where(here, jnp.concatenate([fresh, fresh], axis=0), buf[b, block, :].astype(F32))
                    writes.append((buf, b, block, value.astype(BF16)))
            for buf, b, block, value in writes:
                buf[b, block, :] = value

        q_t = q_scr[pl.ds(c * cols, cols), :].T
        acc = None
        for t in range(quads):
            halves = []
            for i in range(2):
                p = 2 * t + i
                tile = p // pairs_per_tile
                tiles = [no_tile] * (cols // 128)
                tiles[tile] = jnp.where(lane_pair == p % pairs_per_tile, q_t[:, tile * 128:(tile + 1) * 128], 0.0).astype(BF16)
                halves.append(jnp.concatenate(tiles, axis=1))
            d = jnp.dot(square(kmat, (c * chunk + t * 4) * rows_kv), jnp.concatenate(halves, axis=0), preferred_element_type=F32)
            acc = d if acc is None else acc + d
        if c > 0:
            values(c - 1)
        stores[c][0].start()
        stores[c][1].start()
        s = jnp.where(first_of_two, acc[:rows_kv], acc[rows_kv:])
        limit = jnp.concatenate([lim_scr[pl.ds(c * (cols // 128) + j, 1), :] for j in range(cols // 128)], axis=1)
        s = jnp.where(same_head & (row <= limit), s * scale, -jnp.inf)
        e = jnp.exp(s - jnp.max(s, axis=0, keepdims=True))
        p_scr[c % 2] = (e * (1.0 / jnp.sum(e, axis=0, keepdims=True))).T
    values(n_chunks - 1)

    att = jnp.concatenate([o_scr[pl.ds(j, batch, n_q), :].astype(BF16) for j in range(n_q)], axis=1)
    if first:
        wo_load.wait()
    for n in range(wo.shape[1] // 512):
        cols_n = pl.ds(n * 512, 512)
        part_ref[:, cols_n] = jnp.dot(att, wo[:, cols_n], preferred_element_type=F32).astype(BF16)
    for a, b in stores:
        a.wait()
        b.wait()


def attention_call(layer, first, positions, x, norm, tables, wq, wk, wv, wo, kc, vc, k_out, v_out):
    batch, d = x.shape
    hd = kc.shape[-1]
    n_q, n_kv = wq.shape[-1] // hd, wk.shape[-1] // hd
    chunk = 64
    n_chunks = batch // chunk
    if first:
        ins = [positions] + in_hbm([x]) + [norm, tables[0], tables[1]] + in_hbm([wq, wk, wv, wo, kc, vc])
    else:
        ins = [positions, x, tables[0], tables[1], wq, wk, wv, wo, kc, vc]
    part = pltpu.VMEM((batch, d), BF16)
    if first:
        specs = [SMEM, HBM, VMEM, VMEM, VMEM] + [HBM] * 6
        outs = (part, pltpu.HBM(kc.shape, BF16), pltpu.HBM(vc.shape, BF16))
        out_specs = (VMEM, HBM, HBM)
        aliases = {}
        big = [(batch, d), wq.shape[1:], wk.shape[1:], wv.shape[1:], wo.shape[1:], kc.shape[1:], vc.shape[1:], (batch, d)]
    else:
        specs = [SMEM, VMEM, VMEM, VMEM] + [VMEM] * 6 + [HBM] * 2
        aliases = {len(ins): 1, len(ins) + 1: 2, len(ins) - 2: 3, len(ins) - 1: 4}
        outs = (part, pltpu.HBM(k_out.shape, BF16), pltpu.HBM(v_out.shape, BF16), pltpu.VMEM(kc.shape, BF16), pltpu.VMEM(vc.shape, BF16))
        ins += in_hbm([k_out, v_out])
        out_specs = (VMEM, HBM, HBM, VMEM, VMEM)
        big = []
    scratch = [pltpu.VMEM(shape, BF16) for shape in big]
    scratch += [
        pltpu.VMEM((batch, hd), F32), pltpu.VMEM((batch, hd), F32), pltpu.VMEM((batch * n_q // hd, hd), jnp.int32),
        pltpu.VMEM((batch * n_q, hd), F32), pltpu.VMEM((batch * n_kv, hd), F32), pltpu.VMEM((batch * n_kv, hd), F32),
        pltpu.VMEM((2, chunk * n_q, hd), F32), pltpu.VMEM((batch * n_q, hd), F32),
        pltpu.SemaphoreType.DMA((5,)), pltpu.SemaphoreType.DMA((2, n_chunks)), pltpu.SemaphoreType.DMA((2, n_chunks)),
    ]
    return pl.pallas_call(
        functools.partial(attention_kernel, layer, first, chunk),
        out_shape=outs,
        in_specs=specs,
        out_specs=out_specs,
        scratch_shapes=scratch,
        input_output_aliases=aliases,
        compiler_params=pltpu.CompilerParams(vmem_limit_bytes=(62 if first else 8) * 2**20),
        name=f"attention{layer}",
    )(*ins)


GROUPS = 2
SUB = 4
NCOL = 2


def mlp_kernel(layer, last, x_in, part_ref, norm_in, next_norm_in, wg_hbm, wu_hbm, wd_hbm, *refs):
    if last:
        carry_in, carry_out = (), ()
        (xo_ref,), refs = refs[:1], refs[1:]
    else:
        carry_in, (ho_ref, xo_ref), carry_out, refs = refs[:6], refs[6:8], refs[8:14], refs[14:]
    (wg, wu, wd, d1, c1, x1, d2, c2, x2, x_own, hbuf, abuf, pbuf, norm_ref, next_norm_ref, n_sem, w_sem, c_sem, s_send, s_recv) = refs
    t = lax.axis_index("tp")
    core = lax.rem(t, 2)
    other = 1 - core
    partner = t + other - core
    across = lax.rem(t + 2, 4)
    out = xo_ref if last else ho_ref
    d = part_ref.shape[1]
    half = d1.shape[0]
    rows_g = half // GROUPS
    rows_s = rows_g // SUB
    cols_n = d // NCOL

    barrier = pltpu.get_barrier_semaphore()
    for dev in (partner, across):
        pl.semaphore_signal(barrier, inc=1, device_id={"tp": dev}, device_id_type=MESH)
    small = [pltpu.make_async_copy(norm_in, norm_ref, n_sem.at[0]), pltpu.make_async_copy(next_norm_in, next_norm_ref, n_sem.at[1])]
    if not last:
        small.append(pltpu.make_async_copy(x_in.at[pl.ds(pl.multiple_of(core * half, half), half)], x_own, n_sem.at[2]))
    for cp in small:
        cp.start()
    w_loads = []
    for i, (src, dst) in enumerate(((wg_hbm, wg), (wu_hbm, wu), (wd_hbm, wd))):
        n = dst.shape[0] // 4
        for j in range(4):
            cp = pltpu.make_async_copy(src.at[layer, pl.ds(j * n, n)], dst.at[pl.ds(j * n, n)], w_sem.at[i, j])
            cp.start()
            w_loads.append(cp)
    pl.semaphore_wait(barrier, 2)

    def send(stage, idx, src, dst, dev):
        cp = pltpu.make_async_remote_copy(src_ref=src, dst_ref=dst, send_sem=s_send.at[stage, idx], recv_sem=s_recv.at[stage, idx],
                                          device_id={"tp": dev}, device_id_type=MESH)
        cp.start()
        return cp

    started = []

    def add_norm(mine, theirs, res, res_row, row, x_to, w_ref, w_row, dst, dst_row):
        rows = pl.ds(row, 16)
        to = pl.ds(dst_row, 16)

        def total(j, n):
            t = (mine[rows, j:j + n].astype(F32) + theirs[rows, j:j + n].astype(F32)).astype(BF16).astype(F32)
            return (res[pl.ds(res_row, 16), j:j + n].astype(F32) + t).astype(BF16)

        if w_ref is None:
            for j in range(0, d, 256):
                dst[to, j:j + 256] = total(j, 256)
            return

        def keep(j, n):
            v = total(j, n)
            x_to[rows, j:j + n] = v
            return v.astype(F32)

        first_pass = [True] * (d // 256)

        def read(j, n):
            if first_pass[j // 256]:
                first_pass[j // 256] = False
                return keep(j, n)
            return x_to[rows, j:j + n].astype(F32)

        def write(j, n, v):
            dst[to, j:j + n] = v

        norm_block(read, lambda j, n: w_ref[w_row:w_row + 1, j:j + n].astype(F32), write, d)

    subs = [(g, s, g * rows_g + s * rows_s) for g in range(GROUPS) for s in range(SUB)]
    near = []
    for i, (g, s, r0) in enumerate(subs):
        near.append(send(0, i, part_ref.at[pl.ds(other * half + r0, rows_s)], d1.at[pl.ds(r0, rows_s)], partner))
    far = []
    for i, (g, s, r0) in enumerate(subs):
        near[i].wait_recv()
        rows = pl.ds(r0, rows_s)
        c1[rows, :] = (part_ref[pl.ds(core * half + r0, rows_s), :].astype(F32) + d1[rows, :].astype(F32)).astype(BF16)
        far.append(send(1, i, c1.at[rows], x1.at[rows], across))
    started += near + far

    gathers1 = {}

    def finish1(g):
        for s in range(SUB):
            i = g * SUB + s
            far[i].wait_recv()
            for r in range(rows_s // 16):
                r0 = g * rows_g + s * rows_s + r * 16
                rows = pl.ds(r0, 16)
                add_norm(c1, x1, x_in if last else x_own, r0, r0, x_own, norm_ref, layer, hbuf.at[g, core], s * rows_s + r * 16)
            part = hbuf.at[g, core, pl.ds(s * rows_s, rows_s)]
            cp = send(2, i, part, part, partner)
            gathers1[i] = cp
            started.append(cp)

    def wait1(g):
        for s in range(SUB):
            gathers1[g * SUB + s].wait_recv()

    def gate_up(g):
        hid = hbuf.at[g].reshape(2 * rows_g, d)

        def body(n, carry):
            cols = pl.ds(n * 512, 512)
            gate = jnp.dot(hid[...], wg[:, cols], preferred_element_type=F32).astype(BF16).astype(F32)
            up = jnp.dot(hid[...], wu[:, cols], preferred_element_type=F32).astype(BF16).astype(F32)
            abuf[:, cols] = (gate * (1.0 / (1.0 + jnp.exp(-gate))) * up).astype(BF16)
            return carry

        for n in range(wg.shape[1] // 512):
            body(n, 0)

    near2, far2 = {}, {}

    def relay2(g, n):
        i = g * NCOL + n
        near2[i].wait_recv()
        cols = pl.ds(n * cols_n, cols_n)
        rows = pl.ds(g * rows_g, rows_g)
        c2[rows, cols] = (pbuf[g, core, :, cols].astype(F32) + d2[rows, cols].astype(F32)).astype(BF16)
        far2[i] = send(4, i, c2.at[rows, cols], x2.at[rows, cols], across)
        started.append(far2[i])

    def down(g, after_first):
        for n in range(NCOL):
            cols = pl.ds(n * cols_n, cols_n)
            y = jnp.dot(abuf[...], wd[:, cols], preferred_element_type=F32).astype(BF16)
            pbuf[g, :, :, cols] = y.reshape(2, rows_g, cols_n)
            i = g * NCOL + n
            near2[i] = send(3, i, pbuf.at[g, other, :, cols], d2.at[pl.ds(g * rows_g, rows_g), cols], partner)
            started.append(near2[i])
            if n == 0 and after_first is not None:
                after_first()
            if n > 0:
                relay2(g, n - 1)
        relay2(g, NCOL - 1)

    gathers2 = {}

    def finish2(g):
        for n in range(NCOL):
            far2[g * NCOL + n].wait_recv()
        for s in range(SUB):
            for r in range(rows_s // 16):
                r0 = g * rows_g + s * rows_s + r * 16
                to = pl.multiple_of(core * half + r0, 16)
                if last:
                    add_norm(c2, x2, x_own, r0, r0, None, None, 0, out, to)
                else:
                    add_norm(c2, x2, x_own, r0, r0, xo_ref, next_norm_ref, layer + 1, out, to)
            part = out.at[pl.ds(pl.multiple_of(core * half + g * rows_g + s * rows_s, rows_s), rows_s)]
            cp = send(5, g * SUB + s, part, part, partner)
            gathers2[g * SUB + s] = cp
            started.append(cp)

    def wait2(g):
        for s in range(SUB):
            gathers2[g * SUB + s].wait_recv()

    for cp in small:
        cp.wait()
    finish1(0)
    wait1(0)
    for cp in w_loads:
        cp.wait()
    c_loads = []
    for i, (src, dst) in enumerate(zip(carry_in, carry_out)):
        n = dst.shape[0] // 4
        for j in range(4):
            cp = pltpu.make_async_copy(src.at[layer + 1, pl.ds(j * n, n)], dst.at[pl.ds(j * n, n)], c_sem.at[i, j])
            cp.start()
            c_loads.append(cp)
    gate_up(0)
    down(0, lambda: finish1(1))
    wait1(1)
    gate_up(1)
    down(1, None)
    finish2(0)
    wait2(0)
    finish2(1)
    wait2(1)
    for cp in c_loads:
        cp.wait()
    for cp in started:
        cp.wait_send()


def mlp_call(layer, last, x, part, norm, next_norm, wg, wu, wd, carry=()):
    batch, d = part.shape
    half = batch // 2
    rows_g = half // GROUPS
    ff = wg.shape[2]
    n_sem = max(GROUPS * NCOL, GROUPS * SUB)
    own = lambda: pltpu.VMEM((half, d), BF16)
    scratch = [
        pltpu.VMEM(wg.shape[1:], BF16), pltpu.VMEM(wu.shape[1:], BF16), pltpu.VMEM(wd.shape[1:], BF16),
        own(), own(), own(), own(), own(), own(), own(),
        pltpu.VMEM((GROUPS, 2, rows_g, d), BF16), pltpu.VMEM((2 * rows_g, ff), BF16),
        pltpu.VMEM((GROUPS, 2, rows_g, d), BF16), pltpu.VMEM(norm.shape, BF16), pltpu.VMEM(norm.shape, BF16),
        pltpu.SemaphoreType.DMA((3,)), pltpu.SemaphoreType.DMA((3, 4)), pltpu.SemaphoreType.DMA((6, 4)), pltpu.SemaphoreType.DMA((6, n_sem)), pltpu.SemaphoreType.DMA((6, n_sem)),
    ]
    full = pltpu.VMEM((batch, d), BF16)
    mine = pltpu.VMEM((half, d), BF16)
    return pl.pallas_call(
        functools.partial(mlp_kernel, layer, last),
        out_shape=full if last else (full, mine) + tuple(pltpu.VMEM(a.shape[1:], BF16) for a in carry),
        in_specs=[VMEM if last else HBM, VMEM] + [HBM] * (5 + len(carry)),
        out_specs=VMEM if last else (VMEM,) * (2 + len(carry)),
        scratch_shapes=scratch,
        compiler_params=pltpu.CompilerParams(collective_id=layer, has_side_effects=True, vmem_limit_bytes=(33 if last else 33) * 2**20),
        name=f"mlp{layer}",
    )(pltpu.with_memory_space_constraint(x, pltpu.VMEM if last else pltpu.HBM), pltpu.with_memory_space_constraint(part, pltpu.VMEM),
      *in_hbm((norm, next_norm, wg, wu, wd) + tuple(carry)))


def solution(mesh):
    row_spec = P('dp', None)
    pos_spec = P('dp')
    cache_spec = P(None, 'dp', None, 'tp', None)
    norm_spec = P(None, None)
    col_spec = P(None, None, 'tp')
    split_rows = P(None, 'tp', None)

    def local_step(hidden, positions, k_cache, v_cache, attn_norm, w_query, w_key, w_value, w_out, mlp_norm, w_gate, w_up, w_down):
        shape = k_cache.shape
        flat = shape[:2] + (shape[2] * shape[3], shape[4])
        k_cache, v_cache = k_cache.reshape(flat), v_cache.reshape(flat)
        tables = [jnp.asarray(t) for t in rope_by_position(shape[2], shape[4])]
        part, k_out, v_out = attention_call(0, True, positions, hidden, attn_norm, tables, w_query, w_key, w_value, w_out, k_cache, v_cache, None, None)
        h, x_own, *carried = mlp_call(0, False, hidden, part, mlp_norm, attn_norm, w_gate, w_up, w_down, (w_query, w_key, w_value, w_out, k_cache, v_cache))
        part, k_out, v_out = attention_call(1, False, positions, h, None, tables, *carried, k_out, v_out)[:3]
        hidden = mlp_call(1, True, x_own, part, mlp_norm, attn_norm, w_gate, w_up, w_down)
        return hidden, k_out.reshape(shape), v_out.reshape(shape)

    return jax.shard_map(local_step, mesh=mesh, in_specs=(row_spec, pos_spec, cache_spec, cache_spec, norm_spec, col_spec, col_spec, col_spec, split_rows, norm_spec, col_spec, col_spec, split_rows), out_specs=(row_spec, cache_spec, cache_spec), check_vma=False)
```

```python
import functools
import math

import jax
import jax.numpy as jnp
import numpy as np
from jax import lax
from jax.experimental import pallas as pl
from jax.experimental.pallas import tpu as pltpu
from jax.sharding import PartitionSpec as P

MESH = pl.DeviceIdType.MESH
BF16 = jnp.bfloat16
F32 = jnp.float32
ANY = pl.BlockSpec(memory_space=pl.ANY)
HBM = pl.BlockSpec(memory_space=pltpu.HBM)
VMEM = pl.BlockSpec(memory_space=pltpu.VMEM)
SMEM = pl.BlockSpec(memory_space=pltpu.SMEM)


def rope_by_position(seq_len, head_dim):
    half = head_dim // 2
    inv_freq = np.power(np.float32(500000.0), -np.arange(half, dtype=np.float32) * np.float32(2.0 / head_dim)).astype(np.float32)
    wavelen = np.float32(2.0 * math.pi) / inv_freq
    smooth = (np.float32(8192.0) / wavelen - np.float32(1.0)) / np.float32(3.0)
    blended = (np.float32(1.0) - smooth) * inv_freq / np.float32(8.0) + smooth * inv_freq
    scaled = np.where(wavelen < 2048.0, inv_freq, np.where(wavelen > 8192.0, inv_freq / np.float32(8.0), blended)).astype(np.float32)
    angles = np.arange(seq_len, dtype=np.float32)[:, None] * scaled[None, :]
    cos = np.cos(angles.astype(np.float64)).astype(np.float32)
    sin = np.sin(angles.astype(np.float64)).astype(np.float32)
    return np.concatenate([cos, cos], axis=1), np.concatenate([-sin, sin], axis=1)


def norm_block(read, weight, write, width):
    step = 256
    acc = None
    for j in range(width // step):
        v = read(j * step, step)
        sq = v * v
        acc = sq if acc is None else acc + sq
    scale = lax.rsqrt(jnp.sum(acc, axis=-1, keepdims=True) * (1.0 / width) + 1e-5)
    for j in range(width // step):
        write(j * step, step, (read(j * step, step) * scale * weight(j * step, step)).astype(BF16))


def in_hbm(arrays):
    return [pltpu.with_memory_space_constraint(a, pltpu.HBM) for a in arrays]


def attention_kernel(layer, first, chunk, *refs):
    refs = list(refs)
    pos_ref = refs.pop(0)
    x_in = refs.pop(0)
    norm_ref = refs.pop(0) if first else None
    cos_tab, sin_tab, wq_hbm, wk_hbm, wv_hbm, wo_hbm, kc_hbm, vc_hbm = refs[:8]
    refs = refs[8:]
    if first:
        part_ref, ko_hbm, vo_hbm = refs[:3]
        x_ref, wq, wk, wv, wo, kbuf, vbuf, h_scr = refs[3:11]
        refs = refs[11:]
    else:
        x_ref, wq, wk, wv, wo = x_in, wq_hbm, wk_hbm, wv_hbm, wo_hbm
        part_ref, ko_hbm, vo_hbm, kbuf, vbuf = refs[2:7]
        refs = refs[7:]
    (cos_scr, sin_scr, lim_scr, q_scr, k_scr, v_scr, p_scr, o_scr, w_sem, in_sem, out_sem) = refs
    batch = x_ref.shape[0]
    n_q = wq.shape[1] // 128
    n_kv = wk.shape[1] // 128
    group = n_q // n_kv
    rows_kv = kbuf.shape[1]
    n_chunks = batch // chunk

    if first:
        x_load = pltpu.make_async_copy(x_in, x_ref, w_sem.at[4])
        x_load.start()
        loads = []
        for i, (src, dst) in enumerate(((wq_hbm, wq), (wk_hbm, wk), (wv_hbm, wv))):
            loads.append(pltpu.make_async_copy(src.at[layer], dst, w_sem.at[i]))
        for c in loads:
            c.start()
        kv_loads = []
        for c in range(n_chunks):
            rows = pl.ds(c * chunk, chunk)
            a = pltpu.make_async_copy(kc_hbm.at[layer, rows], kbuf.at[rows], in_sem.at[0, c])
            b = pltpu.make_async_copy(vc_hbm.at[layer, rows], vbuf.at[rows], in_sem.at[1, c])
            kv_loads.append((a, b))
        wo_load = pltpu.make_async_copy(wo_hbm.at[layer], wo, w_sem.at[3])
        kv_loads[0][0].start()
        kv_loads[0][1].start()

    per_row = 128 // n_q
    lane_request = lax.broadcasted_iota(jnp.int32, (1, 128), 1) // n_q

    def table_body(i, carry):
        limit = jnp.zeros((1, 128), jnp.int32)
        for u in range(per_row):
            b = i * per_row + u
            pos = pos_ref[b]
            cos_scr[pl.ds(b, 1), :] = cos_tab[pl.ds(pos, 1), :]
            sin_scr[pl.ds(b, 1), :] = sin_tab[pl.ds(pos, 1), :]
            limit = jnp.where(lane_request == u, pos * n_kv + n_kv - 1, limit)
        lim_scr[pl.ds(i, 1), :] = limit
        return carry

    lax.fori_loop(0, batch // per_row, table_body, 0)

    if first:
        x_load.wait()
        def norm_body(i, carry):
            rows = pl.ds(pl.multiple_of(i * 16, 16), 16)

            def write(j, n, v):
                h_scr[rows, j:j + n] = v

            norm_block(lambda j, n: x_ref[rows, j:j + n].astype(F32), lambda j, n: norm_ref[layer:layer + 1, j:j + n].astype(F32), write, h_scr.shape[1])
            return carry

        lax.fori_loop(0, batch // 16, norm_body, 0)
        h_src = h_scr
    else:
        h_src = x_ref

    def rope(v):
        v = v.astype(BF16).astype(F32)
        return v * cos_scr[...] + pltpu.roll(v, 64, 1) * sin_scr[...]

    h = h_src[...]
    if first:
        loads[0].wait()
        kv_loads[1][0].start()
        kv_loads[1][1].start()
    q = jnp.dot(h, wq[...], preferred_element_type=F32)
    for j in range(n_q):
        q_scr[pl.ds(j, batch, n_q), :] = rope(q[:, j * 128:(j + 1) * 128])
    if first:
        loads[1].wait()
        kv_loads[2][0].start()
        kv_loads[2][1].start()
    k = jnp.dot(h, wk[...], preferred_element_type=F32)
    for j in range(n_kv):
        k_scr[pl.ds(j, batch, n_kv), :] = rope(k[:, j * 128:(j + 1) * 128])
    if first:
        loads[2].wait()
        kv_loads[3][0].start()
        kv_loads[3][1].start()
        wo_load.start()
    v = jnp.dot(h, wv[...], preferred_element_type=F32)
    for j in range(n_kv):
        v_scr[pl.ds(j, batch, n_kv), :] = v[:, j * 128:(j + 1) * 128]

    kmat = kbuf.reshape(batch * rows_kv, 128)
    vmat = vbuf.reshape(batch * rows_kv, 128)
    scale = 128 ** -0.5
    pair = 2 * n_q
    row_id = lax.broadcasted_iota(jnp.int32, (2 * pair, 128), 0)
    first_pair = row_id < pair
    first_in_pair = (row_id % pair) < n_q
    zero = jnp.zeros((2 * pair, 128), F32)
    quads = chunk // 4
    cols = chunk * n_q
    lane = lax.broadcasted_iota(jnp.int32, (rows_kv, cols), 1)
    row = lax.broadcasted_iota(jnp.int32, (rows_kv, cols), 0)
    same_head = (row % n_kv) == (lane % n_q) // group
    first_of_two = (lane // n_q) % 2 == 0
    lane_pair = lax.broadcasted_iota(jnp.int32, (128, 128), 1) // pair
    no_tile = jnp.zeros((128, 128), BF16)
    pairs_per_tile = 128 // pair
    per_tile = 16 // n_kv
    shift = per_tile.bit_length() - 1
    tile_row = lax.broadcasted_iota(jnp.int32, (16, 128), 0) // n_kv
    tile_head = lax.broadcasted_iota(jnp.int32, (8, 128), 0) % n_kv

    def square(mat, base):
        top = mat[pl.ds(base, 2 * rows_kv), :]
        bottom = mat[pl.ds(base + 2 * rows_kv, 2 * rows_kv), :]
        return jnp.concatenate([top, bottom], axis=1)

    stores = []
    for c in range(n_chunks):
        rows = pl.ds(c * chunk, chunk)
        stores.append((pltpu.make_async_copy(kbuf.at[rows], ko_hbm.at[layer, rows], out_sem.at[0, c]),
                       pltpu.make_async_copy(vbuf.at[rows], vo_hbm.at[layer, rows], out_sem.at[1, c])))

    def insert(c):
        for i in range(c * chunk, (c + 1) * chunk, 8):
            writes = []
            for b in range(i, i + 8):
                pos = pos_ref[b]
                block = pl.ds(pl.multiple_of(lax.shift_left(lax.shift_right_logical(pos, shift), 4), 16), 16)
                here = tile_row == lax.bitwise_and(pos, per_tile - 1)
                for buf, new in ((kbuf, k_scr), (vbuf, v_scr)):
                    fresh = jnp.broadcast_to(new[b * n_kv:b * n_kv + 1, :], (8, 128))
                    for j in range(1, n_kv):
                        fresh = jnp.where(tile_head == j, new[b * n_kv + j:b * n_kv + j + 1, :], fresh)
                    value = jnp.where(here, jnp.concatenate([fresh, fresh], axis=0), buf[b, block, :].astype(F32))
                    writes.append((buf, b, block, value.astype(BF16)))
            for buf, b, block, value in writes:
                buf[b, block, :] = value

    def values(c):
        for t in range(quads):
            b = c * chunk + t * 4
            p4 = p_scr[c % 2, pl.ds(t * 2 * pair, 2 * pair), :]
            wide = jnp.concatenate([jnp.where(first_in_pair, p4, zero), jnp.where(first_in_pair, zero, p4)], axis=1).astype(BF16)
            o = jnp.dot(wide, square(vmat, b * rows_kv), preferred_element_type=F32)
            o_scr[pl.ds(b * n_q, 2 * pair), :] = jnp.where(first_pair, o[:, :128], o[:, 128:])

    for c in range(n_chunks):
        if first:
            kv_loads[c][0].wait()
            kv_loads[c][1].wait()

        if first:
            insert(c)
        elif c == 0:
            for other in range(n_chunks):
                insert(other)

        q_t = q_scr[pl.ds(c * cols, cols), :].T
        acc = None
        for t in range(quads):
            halves = []
            for i in range(2):
                p = 2 * t + i
                tile = p // pairs_per_tile
                tiles = [no_tile] * (cols // 128)
                tiles[tile] = jnp.where(lane_pair == p % pairs_per_tile, q_t[:, tile * 128:(tile + 1) * 128], 0.0).astype(BF16)
                halves.append(jnp.concatenate(tiles, axis=1))
            d = jnp.dot(square(kmat, (c * chunk + t * 4) * rows_kv), jnp.concatenate(halves, axis=0), preferred_element_type=F32)
            acc = d if acc is None else acc + d
        if c > 0:
            values(c - 1)
        for ready in ([c] if first or c > 1 else [2 * c, 2 * c + 1] if c < 2 else []):
            if first or c < 2:
                stores[ready][0].start()
                stores[ready][1].start()
        s = jnp.where(first_of_two, acc[:rows_kv], acc[rows_kv:])
        limit = jnp.concatenate([lim_scr[pl.ds(c * (cols // 128) + j, 1), :] for j in range(cols // 128)], axis=1)
        s = jnp.where(same_head & (row <= limit), s * scale, -jnp.inf)
        e = jnp.exp(s - jnp.max(s, axis=0, keepdims=True))
        p_scr[c % 2] = (e * (1.0 / jnp.sum(e, axis=0, keepdims=True))).T
    values(n_chunks - 1)

    att = jnp.concatenate([o_scr[pl.ds(j, batch, n_q), :].astype(BF16) for j in range(n_q)], axis=1)
    if first:
        wo_load.wait()
    for n in range(wo.shape[1] // 512):
        cols_n = pl.ds(n * 512, 512)
        part_ref[:, cols_n] = jnp.dot(att, wo[:, cols_n], preferred_element_type=F32).astype(BF16)
    for a, b in stores:
        a.wait()
        b.wait()


def attention_call(layer, first, positions, x, norm, tables, wq, wk, wv, wo, kc, vc, k_out, v_out):
    batch, d = x.shape
    hd = kc.shape[-1]
    n_q, n_kv = wq.shape[-1] // hd, wk.shape[-1] // hd
    chunk = 64
    n_chunks = batch // chunk
    if first:
        ins = [positions] + in_hbm([x]) + [norm, tables[0], tables[1]] + in_hbm([wq, wk, wv, wo, kc, vc])
    else:
        ins = [positions, x, tables[0], tables[1], wq, wk, wv, wo, kc, vc]
    part = pltpu.VMEM((batch, d), BF16)
    if first:
        specs = [SMEM, HBM, VMEM, VMEM, VMEM] + [HBM] * 6
        outs = (part, pltpu.HBM(kc.shape, BF16), pltpu.HBM(vc.shape, BF16))
        out_specs = (VMEM, HBM, HBM)
        aliases = {}
        big = [(batch, d), wq.shape[1:], wk.shape[1:], wv.shape[1:], wo.shape[1:], kc.shape[1:], vc.shape[1:], (batch, d)]
    else:
        specs = [SMEM, VMEM, VMEM, VMEM] + [VMEM] * 6 + [HBM] * 2
        aliases = {len(ins): 1, len(ins) + 1: 2, len(ins) - 2: 3, len(ins) - 1: 4}
        outs = (part, pltpu.HBM(k_out.shape, BF16), pltpu.HBM(v_out.shape, BF16), pltpu.VMEM(kc.shape, BF16), pltpu.VMEM(vc.shape, BF16))
        ins += in_hbm([k_out, v_out])
        out_specs = (VMEM, HBM, HBM, VMEM, VMEM)
        big = []
    scratch = [pltpu.VMEM(shape, BF16) for shape in big]
    scratch += [
        pltpu.VMEM((batch, hd), F32), pltpu.VMEM((batch, hd), F32), pltpu.VMEM((batch * n_q // hd, hd), jnp.int32),
        pltpu.VMEM((batch * n_q, hd), F32), pltpu.VMEM((batch * n_kv, hd), F32), pltpu.VMEM((batch * n_kv, hd), F32),
        pltpu.VMEM((2, chunk * n_q, hd), F32), pltpu.VMEM((batch * n_q, hd), F32),
        pltpu.SemaphoreType.DMA((5,)), pltpu.SemaphoreType.DMA((2, n_chunks)), pltpu.SemaphoreType.DMA((2, n_chunks)),
    ]
    return pl.pallas_call(
        functools.partial(attention_kernel, layer, first, chunk),
        out_shape=outs,
        in_specs=specs,
        out_specs=out_specs,
        scratch_shapes=scratch,
        input_output_aliases=aliases,
        compiler_params=pltpu.CompilerParams(vmem_limit_bytes=(62 if first else 8) * 2**20),
        name=f"attention{layer}",
    )(*ins)


GROUPS = 2
SUB = 4
NCOL = 2


def mlp_kernel(layer, last, x_in, part_ref, norm_in, next_norm_in, wg_hbm, wu_hbm, wd_hbm, *refs):
    if last:
        carry_in, carry_out = (), ()
        (xo_ref,), refs = refs[:1], refs[1:]
    else:
        carry_in, (ho_ref, xo_ref), carry_out, refs = refs[:6], refs[6:8], refs[8:14], refs[14:]
    (wg, wu, wd, d1, c1, x1, d2, c2, x2, x_own, hbuf, abuf, pbuf, norm_ref, next_norm_ref, n_sem, w_sem, c_sem, s_send, s_recv) = refs
    t = lax.axis_index("tp")
    core = lax.rem(t, 2)
    other = 1 - core
    partner = t + other - core
    across = lax.rem(t + 2, 4)
    out = xo_ref if last else ho_ref
    d = part_ref.shape[1]
    half = d1.shape[0]
    rows_g = half // GROUPS
    rows_s = rows_g // SUB
    cols_n = d // NCOL

    barrier = pltpu.get_barrier_semaphore()
    for dev in (partner, across):
        pl.semaphore_signal(barrier, inc=1, device_id={"tp": dev}, device_id_type=MESH)
    small = [pltpu.make_async_copy(norm_in, norm_ref, n_sem.at[0]), pltpu.make_async_copy(next_norm_in, next_norm_ref, n_sem.at[1])]
    if not last:
        small.append(pltpu.make_async_copy(x_in.at[pl.ds(pl.multiple_of(core * half, half), half)], x_own, n_sem.at[2]))
    for cp in small:
        cp.start()
    w_loads = []
    for i, (src, dst) in enumerate(((wg_hbm, wg), (wu_hbm, wu), (wd_hbm, wd))):
        n = dst.shape[0] // 4
        for j in range(4):
            cp = pltpu.make_async_copy(src.at[layer, pl.ds(j * n, n)], dst.at[pl.ds(j * n, n)], w_sem.at[i, j])
            cp.start()
            w_loads.append(cp)
    pl.semaphore_wait(barrier, 2)

    def send(stage, idx, src, dst, dev):
        cp = pltpu.make_async_remote_copy(src_ref=src, dst_ref=dst, send_sem=s_send.at[stage, idx], recv_sem=s_recv.at[stage, idx],
                                          device_id={"tp": dev}, device_id_type=MESH)
        cp.start()
        return cp

    started = []

    def add_norm(mine, theirs, res, res_row, row, x_to, w_ref, w_row, dst, dst_row):
        rows = pl.ds(row, 16)
        to = pl.ds(dst_row, 16)

        def total(j, n):
            t = (mine[rows, j:j + n].astype(F32) + theirs[rows, j:j + n].astype(F32)).astype(BF16).astype(F32)
            return (res[pl.ds(res_row, 16), j:j + n].astype(F32) + t).astype(BF16)

        if w_ref is None:
            for j in range(0, d, 256):
                dst[to, j:j + 256] = total(j, 256)
            return

        def keep(j, n):
            v = total(j, n)
            x_to[rows, j:j + n] = v
            return v.astype(F32)

        first_pass = [True] * (d // 256)

        def read(j, n):
            if first_pass[j // 256]:
                first_pass[j // 256] = False
                return keep(j, n)
            return x_to[rows, j:j + n].astype(F32)

        def write(j, n, v):
            dst[to, j:j + n] = v

        norm_block(read, lambda j, n: w_ref[w_row:w_row + 1, j:j + n].astype(F32), write, d)

    subs = [(g, s, g * rows_g + s * rows_s) for g in range(GROUPS) for s in range(SUB)]
    near = []
    for i, (g, s, r0) in enumerate(subs):
        near.append(send(0, i, part_ref.at[pl.ds(other * half + r0, rows_s)], d1.at[pl.ds(r0, rows_s)], partner))
    far = []
    for i, (g, s, r0) in enumerate(subs):
        near[i].wait_recv()
        rows = pl.ds(r0, rows_s)
        c1[rows, :] = (part_ref[pl.ds(core * half + r0, rows_s), :].astype(F32) + d1[rows, :].astype(F32)).astype(BF16)
        far.append(send(1, i, c1.at[rows], x1.at[rows], across))
    started += near + far

    gathers1 = {}

    def finish1(g):
        for s in range(SUB):
            i = g * SUB + s
            far[i].wait_recv()
            for r in range(rows_s // 16):
                r0 = g * rows_g + s * rows_s + r * 16
                rows = pl.ds(r0, 16)
                add_norm(c1, x1, x_in if last else x_own, r0, r0, x_own, norm_ref, layer, hbuf.at[g, core], s * rows_s + r * 16)
            part = hbuf.at[g, core, pl.ds(s * rows_s, rows_s)]
            cp = send(2, i, part, part, partner)
            gathers1[i] = cp
            started.append(cp)

    def wait1(g):
        for s in range(SUB):
            gathers1[g * SUB + s].wait_recv()

    def gate_up(g):
        hid = hbuf.at[g].reshape(2 * rows_g, d)

        def body(n, carry):
            cols = pl.ds(n * 512, 512)
            gate = jnp.dot(hid[...], wg[:, cols], preferred_element_type=F32).astype(BF16).astype(F32)
            up = jnp.dot(hid[...], wu[:, cols], preferred_element_type=F32).astype(BF16).astype(F32)
            abuf[:, cols] = (gate * (1.0 / (1.0 + jnp.exp(-gate))) * up).astype(BF16)
            return carry

        for n in range(wg.shape[1] // 512):
            body(n, 0)

    near2, far2 = {}, {}

    def relay2(g, n):
        i = g * NCOL + n
        near2[i].wait_recv()
        cols = pl.ds(n * cols_n, cols_n)
        rows = pl.ds(g * rows_g, rows_g)
        c2[rows, cols] = (pbuf[g, core, :, cols].astype(F32) + d2[rows, cols].astype(F32)).astype(BF16)
        far2[i] = send(4, i, c2.at[rows, cols], x2.at[rows, cols], across)
        started.append(far2[i])

    def down(g, after_first):
        for n in range(NCOL):
            cols = pl.ds(n * cols_n, cols_n)
            y = jnp.dot(abuf[...], wd[:, cols], preferred_element_type=F32).astype(BF16)
            pbuf[g, :, :, cols] = y.reshape(2, rows_g, cols_n)
            i = g * NCOL + n
            near2[i] = send(3, i, pbuf.at[g, other, :, cols], d2.at[pl.ds(g * rows_g, rows_g), cols], partner)
            started.append(near2[i])
            if n == 0 and after_first is not None:
                after_first()
            if n > 0:
                relay2(g, n - 1)
        relay2(g, NCOL - 1)

    gathers2 = {}

    def finish2(g):
        for n in range(NCOL):
            far2[g * NCOL + n].wait_recv()
        for s in range(SUB):
            for r in range(rows_s // 16):
                r0 = g * rows_g + s * rows_s + r * 16
                to = pl.multiple_of(core * half + r0, 16)
                if last:
                    add_norm(c2, x2, x_own, r0, r0, None, None, 0, out, to)
                else:
                    add_norm(c2, x2, x_own, r0, r0, xo_ref, next_norm_ref, layer + 1, out, to)
            part = out.at[pl.ds(pl.multiple_of(core * half + g * rows_g + s * rows_s, rows_s), rows_s)]
            cp = send(5, g * SUB + s, part, part, partner)
            gathers2[g * SUB + s] = cp
            started.append(cp)

    def wait2(g):
        for s in range(SUB):
            gathers2[g * SUB + s].wait_recv()

    for cp in small:
        cp.wait()
    finish1(0)
    wait1(0)
    for cp in w_loads:
        cp.wait()
    c_loads = []
    for i, (src, dst) in enumerate(zip(carry_in, carry_out)):
        n = dst.shape[0] // 4
        for j in range(4):
            cp = pltpu.make_async_copy(src.at[layer + 1, pl.ds(j * n, n)], dst.at[pl.ds(j * n, n)], c_sem.at[i, j])
            cp.start()
            c_loads.append(cp)
    gate_up(0)
    down(0, lambda: finish1(1))
    wait1(1)
    gate_up(1)
    down(1, None)
    finish2(0)
    wait2(0)
    finish2(1)
    wait2(1)
    for cp in c_loads:
        cp.wait()
    for cp in started:
        cp.wait_send()


def mlp_call(layer, last, x, part, norm, next_norm, wg, wu, wd, carry=()):
    batch, d = part.shape
    half = batch // 2
    rows_g = half // GROUPS
    ff = wg.shape[2]
    n_sem = max(GROUPS * NCOL, GROUPS * SUB)
    own = lambda: pltpu.VMEM((half, d), BF16)
    scratch = [
        pltpu.VMEM(wg.shape[1:], BF16), pltpu.VMEM(wu.shape[1:], BF16), pltpu.VMEM(wd.shape[1:], BF16),
        own(), own(), own(), own(), own(), own(), own(),
        pltpu.VMEM((GROUPS, 2, rows_g, d), BF16), pltpu.VMEM((2 * rows_g, ff), BF16),
        pltpu.VMEM((GROUPS, 2, rows_g, d), BF16), pltpu.VMEM(norm.shape, BF16), pltpu.VMEM(norm.shape, BF16),
        pltpu.SemaphoreType.DMA((3,)), pltpu.SemaphoreType.DMA((3, 4)), pltpu.SemaphoreType.DMA((6, 4)), pltpu.SemaphoreType.DMA((6, n_sem)), pltpu.SemaphoreType.DMA((6, n_sem)),
    ]
    full = pltpu.VMEM((batch, d), BF16)
    mine = pltpu.VMEM((half, d), BF16)
    return pl.pallas_call(
        functools.partial(mlp_kernel, layer, last),
        out_shape=full if last else (full, mine) + tuple(pltpu.VMEM(a.shape[1:], BF16) for a in carry),
        in_specs=[VMEM if last else HBM, VMEM] + [HBM] * (5 + len(carry)),
        out_specs=VMEM if last else (VMEM,) * (2 + len(carry)),
        scratch_shapes=scratch,
        compiler_params=pltpu.CompilerParams(collective_id=layer, has_side_effects=True, vmem_limit_bytes=(33 if last else 33) * 2**20),
        name=f"mlp{layer}",
    )(pltpu.with_memory_space_constraint(x, pltpu.VMEM if last else pltpu.HBM), pltpu.with_memory_space_constraint(part, pltpu.VMEM),
      *in_hbm((norm, next_norm, wg, wu, wd) + tuple(carry)))


def solution(mesh):
    row_spec = P('dp', None)
    pos_spec = P('dp')
    cache_spec = P(None, 'dp', None, 'tp', None)
    norm_spec = P(None, None)
    col_spec = P(None, None, 'tp')
    split_rows = P(None, 'tp', None)

    def local_step(hidden, positions, k_cache, v_cache, attn_norm, w_query, w_key, w_value, w_out, mlp_norm, w_gate, w_up, w_down):
        shape = k_cache.shape
        flat = shape[:2] + (shape[2] * shape[3], shape[4])
        k_cache, v_cache = k_cache.reshape(flat), v_cache.reshape(flat)
        tables = [jnp.asarray(t) for t in rope_by_position(shape[2], shape[4])]
        part, k_out, v_out = attention_call(0, True, positions, hidden, attn_norm, tables, w_query, w_key, w_value, w_out, k_cache, v_cache, None, None)
        h, x_own, *carried = mlp_call(0, False, hidden, part, mlp_norm, attn_norm, w_gate, w_up, w_down, (w_query, w_key, w_value, w_out, k_cache, v_cache))
        part, k_out, v_out = attention_call(1, False, positions, h, None, tables, *carried, k_out, v_out)[:3]
        hidden = mlp_call(1, True, x_own, part, mlp_norm, attn_norm, w_gate, w_up, w_down)
        return hidden, k_out.reshape(shape), v_out.reshape(shape)

    return jax.shard_map(local_step, mesh=mesh, in_specs=(row_spec, pos_spec, cache_spec, cache_spec, norm_spec, col_spec, col_spec, col_spec, split_rows, norm_spec, col_spec, col_spec, split_rows), out_specs=(row_spec, cache_spec, cache_spec), check_vma=False)
```
